128 devices in a mesh: gx: 4 (over x_hi, core), gy: 4 (over y), gz: 8 (over z, x_lo).
Axes of the slice: x: 4 (x_hi: 2, x_lo: 2; x = x_hi * 2 + x_lo), y: 4, z: 4, core: 2. Of those that a mesh axis runs over, the one named last changes fastest.
Arguments:
- field: float32 [64, 1024, 1024], P('gx', 'gy', 'gz'), may hold values from -6 to 6
- source: float32 [64, 1024, 1024], P('gx', 'gy', 'gz'), may hold values from -6 to 6
Outputs:
- smoothed: float32 [64, 1024, 1024], P('gx', 'gy', 'gz')
The draws below stay inside these ranges and needn't reach their ends.
All inputs are finite; a program needn't handle non-finite values.
Results may differ from the reference program's by a relative error of at most 0.00002.
Values sent between devices are 32-bit elements; how exact they have to be, the bound alone decides.
A program may use at most 64 MiB of HBM per device.

```python
import jax
import jax.numpy as jnp

SWEEPS = 3
NX = 64
NY = 1024
NZ = 1024


def block_levels(key, shape, split, least, top_value):
    def one(position, parts):
        draws = jax.random.uniform(jax.random.fold_in(jax.random.fold_in(key, 6), position), (parts,), jnp.float32, least / len(split), top_value / len(split))
        return jnp.repeat(jnp.exp(draws), shape[position] // parts).reshape((-1,) + (1,) * (len(shape) - position - 1))

    loudness = one(*split[0])
    for cut in split[1:]:
        loudness = loudness * one(*cut)
    return loudness


def bell_draw(own_key, shape, spread, most, shards=(), held_as=jnp.bfloat16):
    entries = jax.random.normal(own_key, shape, jnp.float32) * spread
    if len(shards) > 0:
        entries = block_levels(own_key, shape, shards, -0.22, 0.18) * entries
    return jnp.clip(entries, min=-most, max=most).astype(held_as)


def setup_inputs(seed: int = 0) -> dict:
    key_of = jax.random.split(jax.random.key(seed), 3)
    field = bell_draw(key_of[0], (NX, NY, NZ), 1.0, 6.0, ((0, 4), (1, 4), (2, 8)), jnp.float32)
    source = bell_draw(key_of[1], (NX, NY, NZ), 1.0, 6.0, ((0, 4), (1, 4), (2, 8)), jnp.float32)
    return dict(field=field, source=source)


def relax(values, source, parity, colour):
    padded = jnp.pad(values, ((1, 1), (0, 0), (0, 0)))
    beside = padded[2:] + padded[:-2]
    beside = beside + jnp.roll(values, -1, 1) + jnp.roll(values, 1, 1)
    beside = beside + jnp.roll(values, -1, 2) + jnp.roll(values, 1, 2)
    return jnp.where(parity == colour, (source + beside) / 6.0, values)


def reference(field, source):
    nx, ny, nz = field.shape
    parity = (jnp.arange(nx, dtype=jnp.int32)[:, None, None] + jnp.arange(ny, dtype=jnp.int32)[None, :, None] + jnp.arange(nz, dtype=jnp.int32)[None, None, :]) % 2
    values = field
    for sweep in range(SWEEPS):
        values = relax(values, source, parity, 0)
        values = relax(values, source, parity, 1)
    return values
```

```python
import functools

import jax
import jax.numpy as jnp
from jax import lax
from jax.experimental import pallas as pl
from jax.experimental.pallas import tpu as pltpu
from jax.sharding import PartitionSpec as P

SWEEPS = 3
MESH = pl.DeviceIdType.MESH
PAD = 16
OFF = 2
GROUP = 8
THIRD = 1.0 / 6.0


def kernel(sizes, f_hbm, s_hbm, ov, fv, sv, xb, rb, sr, sb, fb, mh, ml, lz, hz, dg, cn, g, rd, sg, cu, cd, ystage, yland, xystage, xyland,
           send, recv, fsem, ssem):
    ngx, ngy, ngz = sizes
    planes, rows, cols = f_hbm.shape
    nm = planes // 2
    blocks = rows // 8
    gx, gy, gz = (lax.axis_index(a) for a in ("gx", "gy", "gz"))
    has_lo, has_hi = gx > 0, gx < ngx - 1
    y_lo, y_hi = lax.rem(gy + ngy - 1, ngy), lax.rem(gy + 1, ngy)
    z_lo, z_hi = lax.rem(gz + ngz - 1, ngz), lax.rem(gz + 1, ngz)
    x_to = (gx - 1, gx + 1)
    y_to = (y_lo, y_hi)
    z_to = (z_lo, z_hi)
    has = (has_lo, has_hi)
    flip = gx >= ngx // 2
    order = [m for a in range(nm // 2) for m in (a, nm - 1 - a)]

    def load(ref, to, sem, m):
        return pltpu.make_async_copy(ref.at[pl.ds(2 * m, 2)], to.at[pl.ds(2 * m, 2)], sem.at[m])

    for m in order:
        load(f_hbm, fv, fsem, m).start()
    for m in order:
        load(s_hbm, sv, ssem, m).start()

    barrier = pltpu.get_barrier_semaphore()

    def greet(device):
        pl.semaphore_signal(barrier, inc=1, device_id=device, device_id_type=MESH)

    for e in range(2):
        greet({"gy": y_to[e]})
        greet({"gz": z_to[e]})
        for d in range(2):
            greet({"gy": y_to[e], "gz": z_to[d]})

        @pl.when(has[e])
        def _():
            greet({"gx": x_to[e]})
            for d in range(2):
                greet({"gx": x_to[e], "gy": y_to[d]})
                greet({"gx": x_to[e], "gz": z_to[d]})

    row8 = lax.broadcasted_iota(jnp.int32, (8, cols), 0)
    lane = lax.broadcasted_iota(jnp.int32, (8, cols), 1)
    off = lax.rem(lane, 4)
    quad = lax.div(lane, 4)
    odd8 = lax.rem(row8 + lane, 2) == 1
    odd_edge = lax.rem(row8 + off, 2) == 0
    first8, last8 = lane == 0, lane == cols - 1

    def rep(mask, n):
        return jnp.broadcast_to(mask[None], (n, 8, cols))

    def roll(v, k):
        k = k % cols
        return v if k == 0 else pltpu.roll(v, k, v.ndim - 1)

    def three(v):
        return v.reshape(v.shape[0] // 8, 8, cols)

    def flat(v):
        return v.reshape(v.shape[0] * 8, cols)

    def pick(parts, y, blk0):
        for k in range(y.shape[0]):
            blk = blk0 + k
            j = blk % len(parts)
            parts[j] = jnp.where(quad == blk, roll(y[k], 4 * blk + 2), parts[j])
        return parts

    def merge(parts):
        while len(parts) > 1:
            parts = [p + q for p, q in zip(parts[::2], parts[1::2])]
        return parts[0]

    zeros8 = jnp.zeros((8, cols), jnp.float32)

    def copy(k, t, src, dst, to, back):
        return pltpu.make_async_remote_copy(
            src_ref=src, dst_ref=dst, send_sem=send.at[k, t], recv_sem=recv.at[back, t], device_id=to, device_id_type=MESH
        )

    def x_copy(t, e, via=None):
        m, to = (0, nm) if e == 0 else (nm - 1, -1)
        return copy(e, t, xb.at[t, OFF + m, pl.ds(PAD, rows)], xb.at[t, OFF + to, pl.ds(PAD, rows)], {"gx": x_to[e if via is None else via]}, 1 - e)

    def y_copy(t, e):
        return copy(2 + e, t, ystage.at[e, t], yland.at[1 - e, t], {"gy": y_to[e]}, 3 - e)

    def z_copy(t, e):
        src, dst = (ml, hz) if e == 0 else (mh, lz)
        return copy(4 + e, t, src.at[t], dst.at[t], {"gz": z_to[e]}, 5 - e)

    def xy_copy(t, e, d, via=None):
        k, back = 6 + 2 * e + d, 6 + 2 * (1 - e) + 1 - d
        return copy(k, t, xystage.at[k - 6, t], xyland.at[back - 6, t], {"gx": x_to[e if via is None else via], "gy": y_to[d]}, back)

    def xz_copy(t, e, d, via=None):
        k, back = 10 + 2 * e + d, 10 + 2 * (1 - e) + 1 - d
        j = 0 if e == 0 else nm // 2 - 1
        return copy(k, t, (ml, mh)[d].at[t, j], dg.at[t, back - 10], {"gx": x_to[e if via is None else via], "gz": z_to[d]}, back)

    def yz_copy(t, e, d):
        k, back = 14 + 2 * e + d, 14 + 2 * (1 - e) + 1 - d
        return copy(k, t, cn.at[1, t, k - 14], cn.at[0, t, back - 14], {"gy": y_to[e], "gz": z_to[d]}, back)

    def sx_copy(e, via=None):
        m, to = (0, nm) if e == 0 else (nm - 1, -1)
        return copy(18 + e, 0, sr.at[OFF + m, pl.ds(PAD, rows)], sr.at[OFF + to, pl.ds(PAD, rows)], {"gx": x_to[e if via is None else via]}, 19 - e)

    def sy_copy(e):
        return copy(20 + e, 0, ystage.at[e, SWEEPS], yland.at[1 - e, SWEEPS], {"gy": y_to[e]}, 21 - e)

    def sz_copy(e):
        src, dst = (ml, hz) if e == 0 else (mh, lz)
        return copy(22 + e, 0, src.at[SWEEPS], dst.at[SWEEPS], {"gz": z_to[e]}, 23 - e)

    def face_copies(t):
        return [y_copy(t, e) for e in range(2)] + [z_copy(t, e) for e in range(2)] + [yz_copy(t, e, d) for e in range(2) for d in range(2)]

    def wall_copies(t, e):
        return [x_copy(t, e)] + [xy_copy(t, e, d) for d in range(2)] + [xz_copy(t, e, d) for d in range(2)]

    def messages(t, src):
        for j in range(nm // 2):
            even, odd = src(2 * j), src(2 * j + 1)
            mh[t, j] = jnp.where(off < 2, even, roll(odd, 2))
            ml[t, j] = jnp.where(off < 2, roll(even, -2), odd)

    def send_all(t):
        for e in range(2):
            r = 0 if e == 0 else 7
            for d in range(2):
                cn[1, t, 2 * e + d] = (ml, mh)[d][t, :, r, :]
        for e in range(2):
            for d in range(2):
                m = 0 if e == 0 else nm - 1
                r = PAD if d == 0 else PAD + rows - 1
                xystage[2 * e + d, t] = xb[t, OFF + m, pl.ds(r, 1), :]
        for e in range(2):
            r = PAD if e == 0 else PAD + rows - 2
            for m in range(nm):
                ystage[e, t, m] = xb[t, OFF + m, pl.ds(r, 2), :]
        for e in range(2):
            for d in range(2):
                yz_copy(t, e, d).start()
        for e in range(2):
            @pl.when(has[e])
            def _():
                for d in range(2):
                    xz_copy(t, e, d).start()
                for d in range(2):
                    xy_copy(t, e, d).start()
        for e in range(2):
            z_copy(t, e).start()
        for e in range(2):
            y_copy(t, e).start()
        for e in range(2):
            @pl.when(has[e])
            def _():
                x_copy(t, e).start()

    def arrive_faces(t):
        for e in range(2):
            z_copy(t, e).wait_recv()
        for e in range(2):
            y_copy(t, e).wait_recv()
        for e in range(2):
            r = PAD - 2 if e == 0 else PAD + rows
            for m in range(nm):
                xb[t, OFF + m, pl.ds(r, 2), :] = yland[e, t, m]
        for j in range(nm // 2):
            low, high = lz[t, j], hz[t, j]
            l1, l3, lm = roll(low, 1), roll(low, 3), roll(low, -1)
            h1, h3, hm = roll(high, 1), roll(high, -3), roll(high, -1)
            g[1 + 2 * j] = jnp.where(off < 2, jnp.where(off == 0, hm, h1), jnp.where(off == 2, l1, l3))
            g[2 + 2 * j] = jnp.where(off < 2, jnp.where(off == 0, h3, hm), jnp.where(off == 2, lm, l1))

    def arrive_diagonals(t):
        for e in range(2):
            for d in range(2):
                yz_copy(t, e, d).wait_recv()
        for j in range(nm // 2):
            for p in range(2):
                a, b = (jnp.broadcast_to(cn[0, t, k, pl.ds(j, 1), :], (8, cols)) for k in (0, 1))
                cu[2 * j + p] = jnp.where(off == 2, roll(a, 5 - 2 * p), roll(b, 5 - 2 * p))
                a, b = (jnp.broadcast_to(cn[0, t, k, pl.ds(j, 1), :], (8, cols)) for k in (2, 3))
                cd[2 * j + p] = jnp.where(off == 2, roll(a, -3 - 2 * p), roll(b, -3 - 2 * p))
        for e in range(2):
            @pl.when(has[e])
            def _():
                for d in range(2):
                    xz_copy(t, 1 - e, d, e).wait_recv()
                    xy_copy(t, 1 - e, d, e).wait_recv()
                i = OFF - 1 if e == 0 else OFF + nm
                for d in range(2):
                    r = PAD - 1 if d == 0 else PAD + rows
                    xb[t, i, pl.ds(r, 1), :] = xyland[2 * e + d, t]
                k = -1 if e == 0 else 1
                g[0 if e == 0 else nm + 1] = jnp.where(off == 2, roll(dg[t, 2 * e], k), roll(dg[t, 2 * e + 1], k))

    def arrive_x(t, late):
        for e in range(2):
            @pl.when(has[e] & (flip if (e == 0) == late else jnp.logical_not(flip)))
            def _():
                x_copy(t, 1 - e, e).wait_recv()

    def edge_red(t):
        for m in range(nm):
            v = g[1 + m]
            up = pltpu.roll(jnp.where(row8 == 7, jnp.where(lane < 4, cu[m], roll(v, 4)), v), 1, 0)
            down = pltpu.roll(jnp.where(row8 == 0, jnp.where(lane >= cols - 4, cd[m], roll(v, -4)), v), 7, 0)
            side = jnp.where(off == 1, roll(v, 1), roll(v, -1))
            beside = jnp.where(odd_edge, g[2 + m], g[m])
            rd[m] = (((sg[m] + v) + (beside + up)) + ((down + side) + fb[t, m])) * jnp.float32(THIRD)

    def relax(read, i, blk0, n, src, edges, c):
        rs = PAD + 8 * blk0
        here = three(read(i, rs, 8 * n))
        below, above = three(read(i - 1, rs, 8 * n)), three(read(i + 1, rs, 8 * n))
        odd = rep(odd8, n)
        beside = jnp.where(odd, above, below) if c == 0 else jnp.where(odd, below, above)
        total = (three(src) + here) + beside
        total = total + three(read(i, rs - 1, 8 * n))
        total = total + three(read(i, rs + 1, 8 * n))
        edge = jnp.stack(edges, axis=0)
        total = total + jnp.where(rep(first8, n), edge, roll(here, 1))
        total = total + jnp.where(rep(last8, n), edge, roll(here, -1))
        return total * jnp.float32(THIRD)

    def red_pair(t, m):
        i = m + OFF

        def read(i, r, n):
            return xb[t, i, pl.ds(r, n), :]

        edges_from = g[m + 1]

        def edge(blk):
            return roll(edges_from, -(4 * blk + 2))

        for blk0 in range(0, blocks, GROUP):
            y = relax(read, i, blk0, GROUP, sr[i, pl.ds(PAD + 8 * blk0, 8 * GROUP), :], [edge(blk0 + k) for k in range(GROUP)], 0)
            rb[i, pl.ds(PAD + 8 * blk0, 8 * GROUP), :] = flat(y)

    def red_rows(t):
        odd = rep(odd8, nm)
        for r, e in ((PAD - 8, [roll(cu[m], -2) for m in range(nm)]), (PAD + rows, [roll(cd[m], 2) for m in range(nm)])):
            def read(i, r):
                return xb[t, pl.ds(i, nm), pl.ds(r, 8), :]

            here = read(OFF, r)
            total = (sr[pl.ds(OFF, nm), pl.ds(r, 8), :] + here) + jnp.where(odd, read(OFF + 1, r), read(OFF - 1, r))
            total = total + read(OFF, r - 1)
            total = total + read(OFF, r + 1)
            edge = jnp.stack(e, axis=0)
            total = total + jnp.where(rep(first8, nm), edge, roll(here, 1))
            total = total + jnp.where(rep(last8, nm), edge, roll(here, -1))
            rb[pl.ds(OFF, nm), pl.ds(r, 8), :] = total * jnp.float32(THIRD)

    def black_pair(m, emit):
        i = m + OFF

        def read(i, r, n):
            return rb[i, pl.ds(r, n), :]

        edges_from = rd[m]
        for blk0 in range(0, blocks, GROUP):
            rs = pl.ds(8 * blk0, 8 * GROUP)
            edges = [roll(edges_from, -(4 * (blk0 + k) + 2)) for k in range(GROUP)]
            emit(blk0, relax(read, i, blk0, GROUP, sb[m, rs, :], edges, 1))

    zero = jnp.zeros((rows + 16, cols), jnp.float32)
    for e in range(2):
        @pl.when(jnp.logical_not(has[e]))
        def _():
            i = OFF - 1 if e == 0 else OFF + nm
            for t in range(SWEEPS):
                xb[t, i, pl.ds(PAD - 8, rows + 16), :] = zero
            rb[i, pl.ds(PAD - 8, rows + 16), :] = zero
            g[0 if e == 0 else nm + 1] = zeros8

    def pack_field(a, carry):
        for m in (a, nm - 1 - a):
            load(f_hbm, fv, fsem, m).wait()
            parts = [zeros8] * 4
            for blk0 in range(0, blocks, GROUP):
                rs = pl.ds(8 * blk0, 8 * GROUP)
                y = jnp.where(rep(odd8, GROUP), three(fv[2 * m, rs, :]), three(fv[2 * m + 1, rs, :]))
                xb[0, OFF + m, pl.ds(PAD + 8 * blk0, 8 * GROUP), :] = flat(y)
                parts = pick(parts, y, blk0)
            fb[0, m] = merge(parts)
        return carry

    def pack_source(a, carry):
        for m in (a, nm - 1 - a):
            load(s_hbm, sv, ssem, m).wait()
            parts = [zeros8] * 4
            for blk0 in range(0, blocks, GROUP):
                rs = pl.ds(8 * blk0, 8 * GROUP)
                low, high = three(sv[2 * m, rs, :]), three(sv[2 * m + 1, rs, :])
                y = jnp.where(rep(odd8, GROUP), high, low)
                sr[OFF + m, pl.ds(PAD + 8 * blk0, 8 * GROUP), :] = flat(y)
                sb[m, rs, :] = flat(jnp.where(rep(odd8, GROUP), low, high))
                parts = pick(parts, y, blk0)
            sg[m] = merge(parts)
        return carry

    lax.fori_loop(0, nm // 2, pack_field, 0)
    messages(0, lambda m: fb[0, m])
    pl.semaphore_wait(barrier, 8 + 5 * (has_lo.astype(jnp.int32) + has_hi.astype(jnp.int32)))
    send_all(0)
    lax.fori_loop(0, nm // 2, pack_source, 0)
    messages(SWEEPS, lambda m: sg[m])
    for e in range(2):
        @pl.when(has[e])
        def _():
            sx_copy(e).start()
        sz_copy(e).start()
        r = PAD if e == 0 else PAD + rows - 1
        for m in range(nm):
            ystage[e, SWEEPS, m, pl.ds(0, 1), :] = sr[OFF + m, pl.ds(r, 1), :]
        sy_copy(e).start()

    for e in range(2):
        sz_copy(e).wait_recv()
        sy_copy(e).wait_recv()
    for e in range(2):
        r = PAD - 1 if e == 0 else PAD + rows
        for m in range(nm):
            sr[OFF + m, pl.ds(r, 1), :] = yland[e, SWEEPS, m, pl.ds(0, 1), :]
    for j in range(nm // 2):
        low, high = lz[SWEEPS, j], hz[SWEEPS, j]
        sg[2 * j] = jnp.where(off == 1, roll(high, 1), roll(low, 1))
        sg[2 * j + 1] = jnp.where(off == 1, roll(high, -1), roll(low, -1))
    for e in range(2):
        @pl.when(has[e])
        def _():
            sx_copy(1 - e, e).wait_recv()

    def at(p):
        return jnp.where(flip, nm - 1 - p, p)

    def half_red(t, p):
        red_pair(t, at(p))

    def halo_red(t, late):
        late = int(late)

        @pl.when((flip & has[1 - late]) | (jnp.logical_not(flip) & has[late]))
        def _():
            red_pair(t, at(nm if late else -1))

    def sweep(t, emitter):
        arrive_faces(t)
        arrive_x(t, False)

        def red_body(p, carry):
            half_red(t, p)
            return carry

        lax.fori_loop(0, nm - 1, red_body, 0)
        arrive_diagonals(t)
        edge_red(t)
        red_rows(t)
        halo_red(t, False)

        def black_body(p, carry):
            emitter(at(p))
            return carry

        lax.fori_loop(0, nm - 2, black_body, 0)
        arrive_x(t, True)
        lax.fori_loop(nm - 1, nm, red_body, 0)
        halo_red(t, True)
        lax.fori_loop(nm - 2, nm, black_body, 0)

    def full(t, carry):
        def emitter(m):
            parts = [zeros8] * 4

            def emit(blk0, y):
                xb[t + 1, OFF + m, pl.ds(PAD + 8 * blk0, 8 * GROUP), :] = flat(y)
                pick(parts, y, blk0)

            black_pair(m, emit)
            fb[t + 1, m] = merge(parts)

        sweep(t, emitter)
        messages(t + 1, lambda m: fb[t + 1, m])
        send_all(t + 1)
        return carry

    lax.fori_loop(0, SWEEPS - 1, full, 0)

    def final(m):
        def emit(blk0, y):
            red = three(rb[OFF + m, pl.ds(PAD + 8 * blk0, 8 * GROUP), :])
            rs = pl.ds(8 * blk0, 8 * GROUP)
            odd = rep(odd8, GROUP)
            ov[2 * m, rs, :] = flat(jnp.where(odd, y, red))
            ov[2 * m + 1, rs, :] = flat(jnp.where(odd, red, y))

        black_pair(m, emit)

    sweep(SWEEPS - 1, final)

    def drain(t, carry):
        for c in face_copies(t):
            c.wait_send()
        for e in range(2):
            @pl.when(has[e])
            def _():
                for c in wall_copies(t, e):
                    c.wait_send()
        return carry

    lax.fori_loop(0, SWEEPS, drain, 0)
    for e in range(2):
        sz_copy(e).wait_send()
        sy_copy(e).wait_send()

        @pl.when(has[e])
        def _():
            sx_copy(e).wait_send()


def solution(mesh):
    sizes = tuple(mesh.shape[a] for a in ("gx", "gy", "gz"))

    def on_device(field, source):
        planes, rows, cols = field.shape
        nm = planes // 2
        assert planes % 4 == 0 and rows == 256 and cols == 128 and rows % (8 * GROUP) == 0
        f32 = jnp.float32
        wide = (nm + 2 * OFF, rows + 2 * PAD, cols)
        return pl.pallas_call(
            functools.partial(kernel, sizes),
            out_shape=jax.ShapeDtypeStruct(field.shape, f32),
            in_specs=[pl.BlockSpec(memory_space=pltpu.HBM)] * 2,
            out_specs=pl.BlockSpec(memory_space=pltpu.VMEM),
            scratch_shapes=[
                pltpu.VMEM(field.shape, f32),
                pltpu.VMEM(field.shape, f32),
                pltpu.VMEM((SWEEPS, *wide), f32),
                pltpu.VMEM(wide, f32),
                pltpu.VMEM(wide, f32),
                pltpu.VMEM((nm, rows, cols), f32),
                pltpu.VMEM((SWEEPS, nm, 8, cols), f32),
                *[pltpu.VMEM((SWEEPS + 1, nm // 2, 8, cols), f32)] * 4,
                pltpu.VMEM((SWEEPS, 4, 8, cols), f32),
                pltpu.VMEM((2, SWEEPS, 4, nm // 2, cols), f32),
                pltpu.VMEM((nm + 2, 8, cols), f32),
                *[pltpu.VMEM((nm, 8, cols), f32)] * 4,
                *[pltpu.VMEM((2, SWEEPS + 1, nm, 2, cols), f32)] * 2,
                *[pltpu.VMEM((4, SWEEPS, 1, cols), f32)] * 2,
                pltpu.SemaphoreType.DMA((24, SWEEPS)),
                pltpu.SemaphoreType.DMA((24, SWEEPS)),
                pltpu.SemaphoreType.DMA((nm,)),
                pltpu.SemaphoreType.DMA((nm,)),
            ],
            compiler_params=pltpu.CompilerParams(
                collective_id=0, has_side_effects=True, vmem_limit_bytes=60 * 1024 * 1024
            ),
        )(field, source)

    spec = P("gx", "gy", "gz")
    return jax.shard_map(on_device, mesh=mesh, in_specs=(spec, spec), out_specs=spec, check_vma=False)
```

```python
import functools

import jax
import jax.numpy as jnp
from jax import lax
from jax.experimental import pallas as pl
from jax.experimental.pallas import tpu as pltpu
from jax.sharding import PartitionSpec as P

SWEEPS = 3
MESH = pl.DeviceIdType.MESH
PAD = 16
OFF = 2
GROUP = 8
THIRD = 1.0 / 6.0


def kernel(sizes, f_hbm, s_hbm, ov, fv, sv, xb, rb, sr, sb, fb, mh, ml, lz, hz, dg, cn, g, rd, sg, cu, cd, ystage, yland, xystage, xyland, sface, sedge,
           send, recv, fsem, ssem):
    ngx, ngy, ngz = sizes
    planes, rows, cols = f_hbm.shape
    nm = planes // 2
    blocks = rows // 8
    gx, gy, gz = (lax.axis_index(a) for a in ("gx", "gy", "gz"))
    has_lo, has_hi = gx > 0, gx < ngx - 1
    y_lo, y_hi = lax.rem(gy + ngy - 1, ngy), lax.rem(gy + 1, ngy)
    z_lo, z_hi = lax.rem(gz + ngz - 1, ngz), lax.rem(gz + 1, ngz)
    x_to = (gx - 1, gx + 1)
    y_to = (y_lo, y_hi)
    z_to = (z_lo, z_hi)
    has = (has_lo, has_hi)
    flip = gx >= ngx // 2
    order = [m for a in range(nm // 2) for m in (a, nm - 1 - a)]

    def load(ref, to, sem, m):
        return pltpu.make_async_copy(ref.at[pl.ds(2 * m, 2)], to.at[pl.ds(2 * m, 2)], sem.at[m])

    for m in order:
        load(f_hbm, fv, fsem, m).start()
    for m in order:
        load(s_hbm, sv, ssem, m).start()

    barrier = pltpu.get_barrier_semaphore()

    def greet(device):
        pl.semaphore_signal(barrier, inc=1, device_id=device, device_id_type=MESH)

    for e in range(2):
        greet({"gy": y_to[e]})
        greet({"gz": z_to[e]})
        for d in range(2):
            greet({"gy": y_to[e], "gz": z_to[d]})

        @pl.when(has[e])
        def _():
            greet({"gx": x_to[e]})
            for d in range(2):
                greet({"gx": x_to[e], "gy": y_to[d]})
                greet({"gx": x_to[e], "gz": z_to[d]})

    row8 = lax.broadcasted_iota(jnp.int32, (8, cols), 0)
    lane = lax.broadcasted_iota(jnp.int32, (8, cols), 1)
    off = lax.rem(lane, 4)
    quad = lax.div(lane, 4)
    odd8 = lax.rem(row8 + lane, 2) == 1
    odd_edge = lax.rem(row8 + off, 2) == 0
    first8, last8 = lane == 0, lane == cols - 1

    def rep(mask, n):
        return jnp.broadcast_to(mask[None], (n, 8, cols))

    def roll(v, k):
        k = k % cols
        return v if k == 0 else pltpu.roll(v, k, v.ndim - 1)

    def three(v):
        return v.reshape(v.shape[0] // 8, 8, cols)

    def flat(v):
        return v.reshape(v.shape[0] * 8, cols)

    def pick(parts, y, blk0):
        for k in range(y.shape[0]):
            blk = blk0 + k
            j = blk % len(parts)
            parts[j] = jnp.where(quad == blk, roll(y[k], 4 * blk + 2), parts[j])
        return parts

    def merge(parts):
        while len(parts) > 1:
            parts = [p + q for p, q in zip(parts[::2], parts[1::2])]
        return parts[0]

    zeros8 = jnp.zeros((8, cols), jnp.float32)

    def copy(k, t, src, dst, to, back):
        return pltpu.make_async_remote_copy(
            src_ref=src, dst_ref=dst, send_sem=send.at[k, t], recv_sem=recv.at[back, t], device_id=to, device_id_type=MESH
        )

    def x_copy(t, e, via=None):
        m, to = (0, nm) if e == 0 else (nm - 1, -1)
        return copy(e, t, xb.at[t, OFF + m, pl.ds(PAD, rows)], xb.at[t, OFF + to, pl.ds(PAD, rows)], {"gx": x_to[e if via is None else via]}, 1 - e)

    def y_copy(t, e):
        return copy(2 + e, t, ystage.at[e, t], yland.at[1 - e, t], {"gy": y_to[e]}, 3 - e)

    def z_copy(t, e):
        src, dst = (ml, hz) if e == 0 else (mh, lz)
        return copy(4 + e, t, src.at[t], dst.at[t], {"gz": z_to[e]}, 5 - e)

    def xy_copy(t, e, d, via=None):
        k, back = 6 + 2 * e + d, 6 + 2 * (1 - e) + 1 - d
        return copy(k, t, xystage.at[k - 6, t], xyland.at[back - 6, t], {"gx": x_to[e if via is None else via], "gy": y_to[d]}, back)

    def xz_copy(t, e, d, via=None):
        k, back = 10 + 2 * e + d, 10 + 2 * (1 - e) + 1 - d
        j = 0 if e == 0 else nm // 2 - 1
        return copy(k, t, (ml, mh)[d].at[t, j], dg.at[t, back - 10], {"gx": x_to[e if via is None else via], "gz": z_to[d]}, back)

    def yz_copy(t, e, d):
        k, back = 14 + 2 * e + d, 14 + 2 * (1 - e) + 1 - d
        return copy(k, t, cn.at[1, t, k - 14], cn.at[0, t, back - 14], {"gy": y_to[e], "gz": z_to[d]}, back)

    def sx_copy(e, via=None):
        return copy(18 + e, 0, sface.at[0, e], sface.at[1, 1 - e], {"gx": x_to[e if via is None else via]}, 19 - e)

    def sy_copy(e):
        return copy(20 + e, 0, ystage.at[e, SWEEPS], yland.at[1 - e, SWEEPS], {"gy": y_to[e]}, 21 - e)

    def sz_copy(e):
        return copy(22 + e, 0, sedge.at[0, e], sedge.at[1, 1 - e], {"gz": z_to[e]}, 23 - e)

    def face_copies(t):
        return [y_copy(t, e) for e in range(2)] + [z_copy(t, e) for e in range(2)] + [yz_copy(t, e, d) for e in range(2) for d in range(2)]

    def wall_copies(t, e):
        return [x_copy(t, e)] + [xy_copy(t, e, d) for d in range(2)] + [xz_copy(t, e, d) for d in range(2)]

    def messages(t, src):
        for j in range(nm // 2):
            even, odd = src(2 * j), src(2 * j + 1)
            mh[t, j] = jnp.where(off < 2, even, roll(odd, 2))
            ml[t, j] = jnp.where(off < 2, roll(even, -2), odd)

    def send_all(t):
        for e in range(2):
            r = 0 if e == 0 else 7
            for d in range(2):
                cn[1, t, 2 * e + d] = (ml, mh)[d][t, :, r, :]
        for e in range(2):
            for d in range(2):
                m = 0 if e == 0 else nm - 1
                r = PAD if d == 0 else PAD + rows - 1
                xystage[2 * e + d, t] = xb[t, OFF + m, pl.ds(r, 1), :]
        for e in range(2):
            r = PAD if e == 0 else PAD + rows - 2
            for m in range(nm):
                ystage[e, t, m] = xb[t, OFF + m, pl.ds(r, 2), :]
        for e in range(2):
            for d in range(2):
                yz_copy(t, e, d).start()
        for e in range(2):
            @pl.when(has[e])
            def _():
                for d in range(2):
                    xz_copy(t, e, d).start()
                for d in range(2):
                    xy_copy(t, e, d).start()
        for e in range(2):
            z_copy(t, e).start()
        for e in range(2):
            y_copy(t, e).start()
        for e in range(2):
            @pl.when(has[e])
            def _():
                x_copy(t, e).start()

    def arrive_faces(t):
        for e in range(2):
            z_copy(t, e).wait_recv()
        for e in range(2):
            y_copy(t, e).wait_recv()
        for e in range(2):
            r = PAD - 2 if e == 0 else PAD + rows
            for m in range(nm):
                xb[t, OFF + m, pl.ds(r, 2), :] = yland[e, t, m]
        for j in range(nm // 2):
            low, high = lz[t, j], hz[t, j]
            l1, l3, lm = roll(low, 1), roll(low, 3), roll(low, -1)
            h1, h3, hm = roll(high, 1), roll(high, -3), roll(high, -1)
            g[1 + 2 * j] = jnp.where(off < 2, jnp.where(off == 0, hm, h1), jnp.where(off == 2, l1, l3))
            g[2 + 2 * j] = jnp.where(off < 2, jnp.where(off == 0, h3, hm), jnp.where(off == 2, lm, l1))

    def arrive_diagonals(t):
        for e in range(2):
            for d in range(2):
                yz_copy(t, e, d).wait_recv()
        for j in range(nm // 2):
            for p in range(2):
                a, b = (jnp.broadcast_to(cn[0, t, k, pl.ds(j, 1), :], (8, cols)) for k in (0, 1))
                cu[2 * j + p] = jnp.where(off == 2, roll(a, 5 - 2 * p), roll(b, 5 - 2 * p))
                a, b = (jnp.broadcast_to(cn[0, t, k, pl.ds(j, 1), :], (8, cols)) for k in (2, 3))
                cd[2 * j + p] = jnp.where(off == 2, roll(a, -3 - 2 * p), roll(b, -3 - 2 * p))
        for e in range(2):
            @pl.when(has[e])
            def _():
                for d in range(2):
                    xz_copy(t, 1 - e, d, e).wait_recv()
                    xy_copy(t, 1 - e, d, e).wait_recv()
                i = OFF - 1 if e == 0 else OFF + nm
                for d in range(2):
                    r = PAD - 1 if d == 0 else PAD + rows
                    xb[t, i, pl.ds(r, 1), :] = xyland[2 * e + d, t]
                k = -1 if e == 0 else 1
                g[0 if e == 0 else nm + 1] = jnp.where(off == 2, roll(dg[t, 2 * e], k), roll(dg[t, 2 * e + 1], k))

    def arrive_x(t, late):
        for e in range(2):
            @pl.when(has[e] & (flip if (e == 0) == late else jnp.logical_not(flip)))
            def _():
                x_copy(t, 1 - e, e).wait_recv()

    def edge_red(t):
        for m in range(nm):
            v = g[1 + m]
            up = pltpu.roll(jnp.where(row8 == 7, jnp.where(lane < 4, cu[m], roll(v, 4)), v), 1, 0)
            down = pltpu.roll(jnp.where(row8 == 0, jnp.where(lane >= cols - 4, cd[m], roll(v, -4)), v), 7, 0)
            side = jnp.where(off == 1, roll(v, 1), roll(v, -1))
            beside = jnp.where(odd_edge, g[2 + m], g[m])
            rd[m] = (((sg[m] + v) + (beside + up)) + ((down + side) + fb[t, m])) * jnp.float32(THIRD)

    def relax(read, i, blk0, n, src, edges, c):
        rs = PAD + 8 * blk0
        here = three(read(i, rs, 8 * n))
        below, above = three(read(i - 1, rs, 8 * n)), three(read(i + 1, rs, 8 * n))
        odd = rep(odd8, n)
        beside = jnp.where(odd, above, below) if c == 0 else jnp.where(odd, below, above)
        total = (three(src) + here) + beside
        total = total + three(read(i, rs - 1, 8 * n))
        total = total + three(read(i, rs + 1, 8 * n))
        edge = jnp.stack(edges, axis=0)
        total = total + jnp.where(rep(first8, n), edge, roll(here, 1))
        total = total + jnp.where(rep(last8, n), edge, roll(here, -1))
        return total * jnp.float32(THIRD)

    def red_pair(t, m):
        i = m + OFF

        def read(i, r, n):
            return xb[t, i, pl.ds(r, n), :]

        edges_from = g[m + 1]

        def edge(blk):
            return roll(edges_from, -(4 * blk + 2))

        for blk0 in range(0, blocks, GROUP):
            y = relax(read, i, blk0, GROUP, sr[i, pl.ds(PAD + 8 * blk0, 8 * GROUP), :], [edge(blk0 + k) for k in range(GROUP)], 0)
            rb[i, pl.ds(PAD + 8 * blk0, 8 * GROUP), :] = flat(y)

    def red_rows(t):
        odd = rep(odd8, nm)
        for r, e in ((PAD - 8, [roll(cu[m], -2) for m in range(nm)]), (PAD + rows, [roll(cd[m], 2) for m in range(nm)])):
            def read(i, r):
                return xb[t, pl.ds(i, nm), pl.ds(r, 8), :]

            here = read(OFF, r)
            total = (sr[pl.ds(OFF, nm), pl.ds(r, 8), :] + here) + jnp.where(odd, read(OFF + 1, r), read(OFF - 1, r))
            total = total + read(OFF, r - 1)
            total = total + read(OFF, r + 1)
            edge = jnp.stack(e, axis=0)
            total = total + jnp.where(rep(first8, nm), edge, roll(here, 1))
            total = total + jnp.where(rep(last8, nm), edge, roll(here, -1))
            rb[pl.ds(OFF, nm), pl.ds(r, 8), :] = total * jnp.float32(THIRD)

    def black_pair(m, emit):
        i = m + OFF

        def read(i, r, n):
            return rb[i, pl.ds(r, n), :]

        edges_from = rd[m]
        for blk0 in range(0, blocks, GROUP):
            rs = pl.ds(8 * blk0, 8 * GROUP)
            edges = [roll(edges_from, -(4 * (blk0 + k) + 2)) for k in range(GROUP)]
            emit(blk0, relax(read, i, blk0, GROUP, sb[m, rs, :], edges, 1))

    zero = jnp.zeros((rows + 16, cols), jnp.float32)
    for e in range(2):
        @pl.when(jnp.logical_not(has[e]))
        def _():
            i = OFF - 1 if e == 0 else OFF + nm
            for t in range(SWEEPS):
                xb[t, i, pl.ds(PAD - 8, rows + 16), :] = zero
            rb[i, pl.ds(PAD - 8, rows + 16), :] = zero
            g[0 if e == 0 else nm + 1] = zeros8

    def pack_field(a, carry):
        for m in (a, nm - 1 - a):
            load(f_hbm, fv, fsem, m).wait()
            parts = [zeros8] * 4
            for blk0 in range(0, blocks, GROUP):
                rs = pl.ds(8 * blk0, 8 * GROUP)
                y = jnp.where(rep(odd8, GROUP), three(fv[2 * m, rs, :]), three(fv[2 * m + 1, rs, :]))
                xb[0, OFF + m, pl.ds(PAD + 8 * blk0, 8 * GROUP), :] = flat(y)
                parts = pick(parts, y, blk0)
            fb[0, m] = merge(parts)
        return carry

    def pack_source(a, carry):
        for m in (a, nm - 1 - a):
            load(s_hbm, sv, ssem, m).wait()
            parts = [zeros8] * 4
            for blk0 in range(0, blocks, GROUP):
                rs = pl.ds(8 * blk0, 8 * GROUP)
                low, high = three(sv[2 * m, rs, :]), three(sv[2 * m + 1, rs, :])
                y = jnp.where(rep(odd8, GROUP), high, low)
                sr[OFF + m, pl.ds(PAD + 8 * blk0, 8 * GROUP), :] = flat(y)
                sb[m, rs, :] = flat(jnp.where(rep(odd8, GROUP), low, high))
                parts = pick(parts, y, blk0)
            sg[m] = merge(parts)
        return carry

    lax.fori_loop(0, nm // 2, pack_field, 0)
    messages(0, lambda m: fb[0, m])
    pl.semaphore_wait(barrier, 8 + 5 * (has_lo.astype(jnp.int32) + has_hi.astype(jnp.int32)))
    send_all(0)
    lax.fori_loop(0, nm // 2, pack_source, 0)
    half = rows // 2
    odd_lane = lax.rem(lax.broadcasted_iota(jnp.int32, (half, cols), 1), 2) == 1
    for e in range(2):
        for j in range(nm // 4):
            parts = [roll(sg[4 * j + k], k - 2 + e) for k in range(4)]
            sedge[0, e, j] = jnp.where(off < 2, jnp.where(off == 0, parts[0], parts[1]), jnp.where(off == 2, parts[2], parts[3]))
        sz_copy(e).start()
    for e in range(2):
        r = PAD if e == 0 else PAD + rows - 1
        for m in range(nm):
            ystage[e, SWEEPS, m, pl.ds(0, 1), :] = sr[OFF + m, pl.ds(r, 1), :]
        sy_copy(e).start()
    for e in range(2):
        @pl.when(has[e])
        def _():
            i = OFF if e == 0 else OFF + nm - 1
            even = sr[i, pl.ds(PAD, half, stride=2), :]
            odd = sr[i, pl.ds(PAD + 1, half, stride=2), :]
            sface[0, e] = jnp.where(odd_lane, odd, even) if e == 0 else jnp.where(odd_lane, even, odd)
            sx_copy(e).start()

    def take_source():
        for e in range(2):
            sz_copy(e).wait_recv()
            sy_copy(e).wait_recv()
        for e in range(2):
            r = PAD - 1 if e == 0 else PAD + rows
            for m in range(nm):
                sr[OFF + m, pl.ds(r, 1), :] = yland[e, SWEEPS, m, pl.ds(0, 1), :]
        for j in range(nm // 4):
            low, high = sedge[1, 0, j], sedge[1, 1, j]
            for k in range(4):
                sg[4 * j + k] = jnp.where(off == 1, roll(high, 1 - k), roll(low, 2 - k))

    def take_source_x(late):
        for e in range(2):
            @pl.when(has[e] & (flip if (e == 0) == late else jnp.logical_not(flip)))
            def _():
                sx_copy(1 - e, e).wait_recv()
                i = OFF - 1 if e == 0 else OFF + nm
                got = sface[1, e]
                sr[i, pl.ds(PAD, half, stride=2), :] = got
                sr[i, pl.ds(PAD + 1, half, stride=2), :] = got

    def at(p):
        return jnp.where(flip, nm - 1 - p, p)

    def half_red(t, p):
        red_pair(t, at(p))

    def halo_red(t, late):
        late = int(late)

        @pl.when((flip & has[1 - late]) | (jnp.logical_not(flip) & has[late]))
        def _():
            red_pair(t, at(nm if late else -1))

    def on_first(t, do):
        if not isinstance(t, int):
            pl.when(t == 0)(do)
        elif t == 0:
            do()

    def sweep(t, emitter):
        arrive_faces(t)
        arrive_x(t, False)

        def red_body(p, carry):
            half_red(t, p)
            return carry

        lax.fori_loop(0, nm - 1, red_body, 0)
        arrive_diagonals(t)
        on_first(t, take_source)
        edge_red(t)
        red_rows(t)
        on_first(t, lambda: take_source_x(False))
        halo_red(t, False)

        def black_body(p, carry):
            emitter(at(p))
            return carry

        lax.fori_loop(0, nm - 2, black_body, 0)
        arrive_x(t, True)
        lax.fori_loop(nm - 1, nm, red_body, 0)
        on_first(t, lambda: take_source_x(True))
        halo_red(t, True)
        lax.fori_loop(nm - 2, nm, black_body, 0)

    def full(t, carry):
        def emitter(m):
            parts = [zeros8] * 4

            def emit(blk0, y):
                xb[t + 1, OFF + m, pl.ds(PAD + 8 * blk0, 8 * GROUP), :] = flat(y)
                pick(parts, y, blk0)

            black_pair(m, emit)
            fb[t + 1, m] = merge(parts)

        sweep(t, emitter)
        messages(t + 1, lambda m: fb[t + 1, m])
        send_all(t + 1)
        return carry

    lax.fori_loop(0, SWEEPS - 1, full, 0)

    def final(m):
        def emit(blk0, y):
            red = three(rb[OFF + m, pl.ds(PAD + 8 * blk0, 8 * GROUP), :])
            rs = pl.ds(8 * blk0, 8 * GROUP)
            odd = rep(odd8, GROUP)
            ov[2 * m, rs, :] = flat(jnp.where(odd, y, red))
            ov[2 * m + 1, rs, :] = flat(jnp.where(odd, red, y))

        black_pair(m, emit)

    sweep(SWEEPS - 1, final)

    def drain(t, carry):
        for c in face_copies(t):
            c.wait_send()
        for e in range(2):
            @pl.when(has[e])
            def _():
                for c in wall_copies(t, e):
                    c.wait_send()
        return carry

    lax.fori_loop(0, SWEEPS, drain, 0)
    for e in range(2):
        sz_copy(e).wait_send()
        sy_copy(e).wait_send()

        @pl.when(has[e])
        def _():
            sx_copy(e).wait_send()


def solution(mesh):
    sizes = tuple(mesh.shape[a] for a in ("gx", "gy", "gz"))

    def on_device(field, source):
        planes, rows, cols = field.shape
        nm = planes // 2
        assert planes % 4 == 0 and rows == 256 and cols == 128 and rows % (8 * GROUP) == 0
        f32 = jnp.float32
        wide = (nm + 2 * OFF, rows + 2 * PAD, cols)
        return pl.pallas_call(
            functools.partial(kernel, sizes),
            out_shape=jax.ShapeDtypeStruct(field.shape, f32),
            in_specs=[pl.BlockSpec(memory_space=pltpu.HBM)] * 2,
            out_specs=pl.BlockSpec(memory_space=pltpu.VMEM),
            scratch_shapes=[
                pltpu.VMEM(field.shape, f32),
                pltpu.VMEM(field.shape, f32),
                pltpu.VMEM((SWEEPS, *wide), f32),
                pltpu.VMEM(wide, f32),
                pltpu.VMEM(wide, f32),
                pltpu.VMEM((nm, rows, cols), f32),
                pltpu.VMEM((SWEEPS, nm, 8, cols), f32),
                *[pltpu.VMEM((SWEEPS, nm // 2, 8, cols), f32)] * 4,
                pltpu.VMEM((SWEEPS, 4, 8, cols), f32),
                pltpu.VMEM((2, SWEEPS, 4, nm // 2, cols), f32),
                pltpu.VMEM((nm + 2, 8, cols), f32),
                *[pltpu.VMEM((nm, 8, cols), f32)] * 4,
                *[pltpu.VMEM((2, SWEEPS + 1, nm, 2, cols), f32)] * 2,
                *[pltpu.VMEM((4, SWEEPS, 1, cols), f32)] * 2,
                pltpu.VMEM((2, 2, rows // 2, cols), f32),
                pltpu.VMEM((2, 2, nm // 4, 8, cols), f32),
                pltpu.SemaphoreType.DMA((24, SWEEPS)),
                pltpu.SemaphoreType.DMA((24, SWEEPS)),
                pltpu.SemaphoreType.DMA((nm,)),
                pltpu.SemaphoreType.DMA((nm,)),
            ],
            compiler_params=pltpu.CompilerParams(
                collective_id=0, has_side_effects=True, vmem_limit_bytes=60 * 1024 * 1024
            ),
        )(field, source)

    spec = P("gx", "gy", "gz")
    return jax.shard_map(on_device, mesh=mesh, in_specs=(spec, spec), out_specs=spec, check_vma=False)
```

```python
import functools

import jax
import jax.numpy as jnp
from jax import lax
from jax.experimental import pallas as pl
from jax.experimental.pallas import tpu as pltpu
from jax.sharding import PartitionSpec as P

SWEEPS = 3
MESH = pl.DeviceIdType.MESH
PAD = 16
OFF = 2
GROUP = 8
THIRD = 1.0 / 6.0


def kernel(sizes, f_hbm, s_hbm, ov, fv, sv, xb, rb, sr, sb, fb, mh, ml, lz, hz, dg, cn, g, rd, sg, cu, cd, dz, ystage, yland, xystage, xyland, sface, sedge,
           send, recv, fsem, ssem):
    ngx, ngy, ngz = sizes
    planes, rows, cols = f_hbm.shape
    nm = planes // 2
    blocks = rows // 8
    gx, gy, gz = (lax.axis_index(a) for a in ("gx", "gy", "gz"))
    has_lo, has_hi = gx > 0, gx < ngx - 1
    y_lo, y_hi = lax.rem(gy + ngy - 1, ngy), lax.rem(gy + 1, ngy)
    z_lo, z_hi = lax.rem(gz + ngz - 1, ngz), lax.rem(gz + 1, ngz)
    x_to = (gx - 1, gx + 1)
    y_to = (y_lo, y_hi)
    z_to = (z_lo, z_hi)
    has = (has_lo, has_hi)
    flip = gx >= ngx // 2
    order = [m for a in range(nm // 2) for m in (a, nm - 1 - a)]

    def load(ref, to, sem, m):
        return pltpu.make_async_copy(ref.at[pl.ds(2 * m, 2)], to.at[pl.ds(2 * m, 2)], sem.at[m])

    for m in order:
        load(f_hbm, fv, fsem, m).start()
    for m in order:
        load(s_hbm, sv, ssem, m).start()

    barrier = pltpu.get_barrier_semaphore()

    def greet(device):
        pl.semaphore_signal(barrier, inc=1, device_id=device, device_id_type=MESH)

    for e in range(2):
        greet({"gy": y_to[e]})
        greet({"gz": z_to[e]})
        for d in range(2):
            greet({"gy": y_to[e], "gz": z_to[d]})

        @pl.when(has[e])
        def _():
            greet({"gx": x_to[e]})
            for d in range(2):
                greet({"gx": x_to[e], "gy": y_to[d]})
                greet({"gx": x_to[e], "gz": z_to[d]})

    row8 = lax.broadcasted_iota(jnp.int32, (8, cols), 0)
    lane = lax.broadcasted_iota(jnp.int32, (8, cols), 1)
    off = lax.rem(lane, 4)
    quad = lax.div(lane, 4)
    odd8 = lax.rem(row8 + lane, 2) == 1
    odd_edge = lax.rem(row8 + off, 2) == 0
    mid = lax.rem(off + 1, 4) >= 2
    brim = lax.rem(lane + 2, cols) < 4
    first8, last8 = lane == 0, lane == cols - 1

    def rep(mask, n):
        return jnp.broadcast_to(mask[None], (n, 8, cols))

    def roll(v, k):
        k = k % cols
        return v if k == 0 else pltpu.roll(v, k, v.ndim - 1)

    def three(v):
        return v.reshape(v.shape[0] // 8, 8, cols)

    def flat(v):
        return v.reshape(v.shape[0] * 8, cols)

    def pick(parts, y, blk0):
        for k in range(y.shape[0]):
            blk = blk0 + k
            j = blk % len(parts)
            parts[j] = jnp.where(quad == blk, roll(y[k], 4 * blk + 2), parts[j])
        return parts

    def merge(parts):
        while len(parts) > 1:
            parts = [p + q for p, q in zip(parts[::2], parts[1::2])]
        return parts[0]

    zeros8 = jnp.zeros((8, cols), jnp.float32)

    def copy(k, t, src, dst, to, back):
        return pltpu.make_async_remote_copy(
            src_ref=src, dst_ref=dst, send_sem=send.at[k, t], recv_sem=recv.at[back, t], device_id=to, device_id_type=MESH
        )

    def x_copy(t, e, via=None):
        m, to = (0, nm) if e == 0 else (nm - 1, -1)
        return copy(e, t, xb.at[t, OFF + m, pl.ds(PAD, rows)], xb.at[t, OFF + to, pl.ds(PAD, rows)], {"gx": x_to[e if via is None else via]}, 1 - e)

    def y_copy(t, e):
        return copy(2 + e, t, ystage.at[e, t], yland.at[1 - e, t], {"gy": y_to[e]}, 3 - e)

    def z_copy(t, e):
        src, dst = (ml, hz) if e == 0 else (mh, lz)
        return copy(4 + e, t, src.at[t], dst.at[t], {"gz": z_to[e]}, 5 - e)

    def xy_copy(t, e, d, via=None):
        k, back = 6 + 2 * e + d, 6 + 2 * (1 - e) + 1 - d
        return copy(k, t, xystage.at[k - 6, t], xyland.at[back - 6, t], {"gx": x_to[e if via is None else via], "gy": y_to[d]}, back)

    def xz_copy(t, e, d, via=None):
        k, back = 10 + 2 * e + d, 10 + 2 * (1 - e) + 1 - d
        j = 0 if e == 0 else nm // 2 - 1
        return copy(k, t, (ml, mh)[d].at[t, j], dg.at[t, back - 10], {"gx": x_to[e if via is None else via], "gz": z_to[d]}, back)

    def yz_copy(t, e, d):
        k, back = 14 + 2 * e + d, 14 + 2 * (1 - e) + 1 - d
        return copy(k, t, cn.at[1, t, k - 14], cn.at[0, t, back - 14], {"gy": y_to[e], "gz": z_to[d]}, back)

    def sx_copy(e, via=None):
        return copy(18 + e, 0, sface.at[0, e], sface.at[1, 1 - e], {"gx": x_to[e if via is None else via]}, 19 - e)

    def sy_copy(e):
        return copy(20 + e, 0, ystage.at[e, SWEEPS], yland.at[1 - e, SWEEPS], {"gy": y_to[e]}, 21 - e)

    def sz_copy(e):
        return copy(22 + e, 0, sedge.at[0, e], sedge.at[1, 1 - e], {"gz": z_to[e]}, 23 - e)

    def face_copies(t):
        return [y_copy(t, e) for e in range(2)] + [z_copy(t, e) for e in range(2)] + [yz_copy(t, e, d) for e in range(2) for d in range(2)]

    def wall_copies(t, e):
        return [x_copy(t, e)] + [xy_copy(t, e, d) for d in range(2)] + [xz_copy(t, e, d) for d in range(2)]

    def messages(t, src):
        for j in range(nm // 2):
            even, odd = src(2 * j), src(2 * j + 1)
            mh[t, j] = jnp.where(off < 2, even, roll(odd, 2))
            ml[t, j] = jnp.where(off < 2, roll(even, -2), odd)

    def send_all(t):
        for e in range(2):
            r = 0 if e == 0 else 7
            for d in range(2):
                cn[1, t, 2 * e + d] = (ml, mh)[d][t, :, r, :]
        for e in range(2):
            for d in range(2):
                m = 0 if e == 0 else nm - 1
                r = PAD if d == 0 else PAD + rows - 1
                xystage[2 * e + d, t] = xb[t, OFF + m, pl.ds(r, 1), :]
        for e in range(2):
            r = PAD if e == 0 else PAD + rows - 2
            for m in range(nm):
                ystage[e, t, m] = xb[t, OFF + m, pl.ds(r, 2), :]
        for e in range(2):
            for d in range(2):
                yz_copy(t, e, d).start()
        for e in range(2):
            @pl.when(has[e])
            def _():
                for d in range(2):
                    xz_copy(t, e, d).start()
                for d in range(2):
                    xy_copy(t, e, d).start()
        for e in range(2):
            z_copy(t, e).start()
        for e in range(2):
            y_copy(t, e).start()
        for e in range(2):
            @pl.when(has[e])
            def _():
                x_copy(t, e).start()

    def arrive_faces(t):
        for e in range(2):
            z_copy(t, e).wait_recv()
        for e in range(2):
            y_copy(t, e).wait_recv()
        for e in range(2):
            r = PAD - 2 if e == 0 else PAD + rows
            for m in range(nm):
                xb[t, OFF + m, pl.ds(r, 2), :] = yland[e, t, m]
        for j in range(nm // 2):
            low, high = lz[t, j], hz[t, j]
            l1, l3, lm = roll(low, 1), roll(low, 3), roll(low, -1)
            h1, h3, hm = roll(high, 1), roll(high, -3), roll(high, -1)
            g[1 + 2 * j] = jnp.where(off < 2, jnp.where(off == 0, hm, h1), jnp.where(off == 2, l1, l3))
            g[2 + 2 * j] = jnp.where(off < 2, jnp.where(off == 0, h3, hm), jnp.where(off == 2, lm, l1))

    def arrive_diagonals(t):
        for e in range(2):
            for d in range(2):
                yz_copy(t, e, d).wait_recv()
        for j in range(nm // 2):
            for p in range(2):
                a, b = (jnp.broadcast_to(cn[0, t, k, pl.ds(j, 1), :], (8, cols)) for k in (0, 1))
                cu[2 * j + p] = jnp.where(off == 2, roll(a, 5 - 2 * p), roll(b, 5 - 2 * p))
                a, b = (jnp.broadcast_to(cn[0, t, k, pl.ds(j, 1), :], (8, cols)) for k in (2, 3))
                cd[2 * j + p] = jnp.where(off == 2, roll(a, -3 - 2 * p), roll(b, -3 - 2 * p))
        for e in range(2):
            @pl.when(has[e])
            def _():
                for d in range(2):
                    xz_copy(t, 1 - e, d, e).wait_recv()
                    xy_copy(t, 1 - e, d, e).wait_recv()
                i = OFF - 1 if e == 0 else OFF + nm
                for d in range(2):
                    r = PAD - 1 if d == 0 else PAD + rows
                    xb[t, i, pl.ds(r, 1), :] = xyland[2 * e + d, t]
                k = -1 if e == 0 else 1
                g[0 if e == 0 else nm + 1] = jnp.where(off == 2, roll(dg[t, 2 * e], k), roll(dg[t, 2 * e + 1], k))

    def arrive_x(t, late):
        for e in range(2):
            @pl.when(has[e] & (flip if (e == 0) == late else jnp.logical_not(flip)))
            def _():
                x_copy(t, 1 - e, e).wait_recv()

    def edge_red(t):
        for m in range(nm):
            v = g[1 + m]
            up = pltpu.roll(jnp.where(row8 == 7, jnp.where(lane < 4, cu[m], roll(v, 4)), v), 1, 0)
            down = pltpu.roll(jnp.where(row8 == 0, jnp.where(lane >= cols - 4, cd[m], roll(v, -4)), v), 7, 0)
            side = jnp.where(off == 1, roll(v, 1), roll(v, -1))
            beside = jnp.where(odd_edge, g[2 + m], g[m])
            rd[m] = (((sg[m] + v) + (beside + up)) + ((down + side) + fb[t, m])) * jnp.float32(THIRD)

    def relax(read, i, blk0, n, src, edges, c, inner=False):
        rs = PAD + 8 * blk0
        here = three(read(i, rs, 8 * n))
        below_at, above_at = i - 1, i + 1
        if inner:
            below_at, above_at = below_at + (nm - (i - OFF)) // nm, above_at - (i - OFF) // (nm - 1)
        below, above = three(read(below_at, rs, 8 * n)), three(read(above_at, rs, 8 * n))
        odd = rep(odd8, n)
        beside = jnp.where(odd, above, below) if c == 0 else jnp.where(odd, below, above)
        total = (three(src) + here) + beside
        total = total + three(read(i, rs - 1, 8 * n))
        total = total + three(read(i, rs + 1, 8 * n))
        return beside_lanes(total, here, edges) * jnp.float32(THIRD)

    def beside_lanes(total, here, edges):
        n = here.shape[0]
        edge = jnp.zeros_like(here) if edges is None else jnp.stack(edges, axis=0)
        total = total + jnp.where(rep(first8, n), edge, roll(here, 1))
        return total + jnp.where(rep(last8, n), edge, roll(here, -1))

    def red_pair(t, m, inner=False, edged=True):
        i = m + OFF

        def read(i, r, n):
            return xb[t, i, pl.ds(r, n), :]

        edges_from = g[m + 1]

        def edge(blk):
            return roll(edges_from, -(4 * blk + 2))

        for blk0 in range(0, blocks, GROUP):
            edges = [edge(blk0 + k) for k in range(GROUP)] if edged else None
            y = relax(read, i, blk0, GROUP, sr[i, pl.ds(PAD + 8 * blk0, 8 * GROUP), :], edges, 0, inner)
            rb[i, pl.ds(PAD + 8 * blk0, 8 * GROUP), :] = flat(y)

    def relax_block(x, src, lo, n, r, edges, c):
        def read(i, r):
            return x[pl.ds(i, n), pl.ds(r, 8), :]

        odd = rep(odd8, n)
        here, below, above = read(lo, r), read(lo - 1, r), read(lo + 1, r)
        total = (src + here) + (jnp.where(odd, above, below) if c == 0 else jnp.where(odd, below, above))
        total = (total + read(lo, r - 1)) + read(lo, r + 1)
        return beside_lanes(total, here, edges) * jnp.float32(THIRD)

    def red_rows(t, edged=True):
        for r, e in ((PAD - 8, [roll(cu[m], -2) for m in range(nm)]), (PAD + rows, [roll(cd[m], 2) for m in range(nm)])):
            src = sr[pl.ds(OFF, nm), pl.ds(r, 8), :]
            rb[pl.ds(OFF, nm), pl.ds(r, 8), :] = relax_block(xb.at[t], src, OFF, nm, r, e if edged else None, 0)

    def red_borders(t):
        for r in (PAD, PAD + rows - 8):
            src = sr[pl.ds(OFF + 1, nm - 2), pl.ds(r, 8), :]
            rb[pl.ds(OFF + 1, nm - 2), pl.ds(r, 8), :] = relax_block(xb.at[t], src, OFF + 1, nm - 2, r, None, 0)

    def lift(m, blk):
        return jnp.where(brim, roll(dz[m], -(4 * blk + 2)), 0.0)

    def black_borders(t):
        for blk in (0, blocks - 1):
            r = PAD + 8 * blk
            y = relax_block(rb, sb[pl.ds(1, nm - 2), pl.ds(8 * blk, 8), :], OFF + 1, nm - 2, r, None, 1)
            for m in range(1, nm - 1):
                v = y[m - 1] + lift(m, blk)
                xb[t + 1, OFF + m, pl.ds(r, 8), :] = v
                fb[t + 1, m] = jnp.where(quad == blk, roll(v, 4 * blk + 2), fb[t + 1, m] + (dz[m] if blk == 0 else 0.0))

    def edge_response(t):
        def middle(v):
            return jnp.where(mid, v, 0.0)

        for m in range(nm):
            v = middle(g[1 + m])
            up = pltpu.roll(jnp.where(row8 == 7, jnp.where(lane < 4, middle(cu[m]), roll(v, 4)), v), 1, 0)
            down = pltpu.roll(jnp.where(row8 == 0, jnp.where(lane >= cols - 4, middle(cd[m]), roll(v, -4)), v), 7, 0)
            beside = jnp.where(odd_edge, middle(g[2 + m]), middle(g[m]))
            near = (rd[m] + ((v + beside) + (up + down)) * jnp.float32(THIRD)) * jnp.float32(THIRD)
            far = jnp.where(off == 0, roll(v, -1), roll(v, 1)) * jnp.float32(THIRD * THIRD)
            dz[m] = jnp.where(mid, near, far)

    def lift_rest(t):
        def body(m, carry):
            v = dz[m]
            for blk0 in range(0, blocks, GROUP):
                lo, hi = max(blk0, 1), min(blk0 + GROUP, blocks - 1)
                rs = pl.ds(PAD + 8 * lo, 8 * (hi - lo))
                y = jnp.stack([roll(v, -(4 * blk + 2)) for blk in range(lo, hi)], axis=0)
                xb[t, OFF + m, rs, :] = xb[t, OFF + m, rs, :] + flat(jnp.where(rep(brim, hi - lo), y, 0.0))
            return carry

        lax.fori_loop(1, nm - 1, body, 0)

    def black_pair(m, emit, edged=True):
        i = m + OFF

        def read(i, r, n):
            return rb[i, pl.ds(r, n), :]

        edges_from = rd[m]
        for blk0 in range(0, blocks, GROUP):
            rs = pl.ds(8 * blk0, 8 * GROUP)
            edges = [roll(edges_from, -(4 * (blk0 + k) + 2)) for k in range(GROUP)] if edged else None
            emit(blk0, relax(read, i, blk0, GROUP, sb[m, rs, :], edges, 1))

    zero = jnp.zeros((rows + 16, cols), jnp.float32)
    for e in range(2):
        @pl.when(jnp.logical_not(has[e]))
        def _():
            i = OFF - 1 if e == 0 else OFF + nm
            for t in range(SWEEPS):
                xb[t, i, pl.ds(PAD - 8, rows + 16), :] = zero
            rb[i, pl.ds(PAD - 8, rows + 16), :] = zero
            g[0 if e == 0 else nm + 1] = zeros8

    def pack_field(a, carry):
        for m in (a, nm - 1 - a):
            load(f_hbm, fv, fsem, m).wait()
            parts = [zeros8] * 4
            for blk0 in range(0, blocks, GROUP):
                rs = pl.ds(8 * blk0, 8 * GROUP)
                y = jnp.where(rep(odd8, GROUP), three(fv[2 * m, rs, :]), three(fv[2 * m + 1, rs, :]))
                xb[0, OFF + m, pl.ds(PAD + 8 * blk0, 8 * GROUP), :] = flat(y)
                parts = pick(parts, y, blk0)
            fb[0, m] = merge(parts)
        return carry

    def pack_source(a, carry):
        for m in (a, nm - 1 - a):
            load(s_hbm, sv, ssem, m).wait()
            parts = [zeros8] * 4
            for blk0 in range(0, blocks, GROUP):
                rs = pl.ds(8 * blk0, 8 * GROUP)
                low, high = three(sv[2 * m, rs, :]), three(sv[2 * m + 1, rs, :])
                y = jnp.where(rep(odd8, GROUP), high, low)
                sr[OFF + m, pl.ds(PAD + 8 * blk0, 8 * GROUP), :] = flat(y)
                sb[m, rs, :] = flat(jnp.where(rep(odd8, GROUP), low, high))
                parts = pick(parts, y, blk0)
            sg[m] = merge(parts)
        return carry

    lax.fori_loop(0, nm // 2, pack_field, 0)
    messages(0, lambda m: fb[0, m])
    pl.semaphore_wait(barrier, 8 + 5 * (has_lo.astype(jnp.int32) + has_hi.astype(jnp.int32)))
    send_all(0)
    lax.fori_loop(0, nm // 2, pack_source, 0)
    half = rows // 2
    odd_lane = lax.rem(lax.broadcasted_iota(jnp.int32, (half, cols), 1), 2) == 1
    for e in range(2):
        for j in range(nm // 4):
            parts = [roll(sg[4 * j + k], k - 2 + e) for k in range(4)]
            sedge[0, e, j] = jnp.where(off < 2, jnp.where(off == 0, parts[0], parts[1]), jnp.where(off == 2, parts[2], parts[3]))
        sz_copy(e).start()
    for e in range(2):
        r = PAD if e == 0 else PAD + rows - 1
        for m in range(nm):
            ystage[e, SWEEPS, m, pl.ds(0, 1), :] = sr[OFF + m, pl.ds(r, 1), :]
        sy_copy(e).start()
    for e in range(2):
        @pl.when(has[e])
        def _():
            i = OFF if e == 0 else OFF + nm - 1
            even = sr[i, pl.ds(PAD, half, stride=2), :]
            odd = sr[i, pl.ds(PAD + 1, half, stride=2), :]
            sface[0, e] = jnp.where(odd_lane, odd, even) if e == 0 else jnp.where(odd_lane, even, odd)
            sx_copy(e).start()

    def take_source():
        for e in range(2):
            sz_copy(e).wait_recv()
            sy_copy(e).wait_recv()
        for e in range(2):
            r = PAD - 1 if e == 0 else PAD + rows
            for m in range(nm):
                sr[OFF + m, pl.ds(r, 1), :] = yland[e, SWEEPS, m, pl.ds(0, 1), :]
        for j in range(nm // 4):
            low, high = sedge[1, 0, j], sedge[1, 1, j]
            for k in range(4):
                sg[4 * j + k] = jnp.where(off == 1, roll(high, 1 - k), roll(low, 2 - k))

    def take_source_x(late):
        for e in range(2):
            @pl.when(has[e] & (flip if (e == 0) == late else jnp.logical_not(flip)))
            def _():
                sx_copy(1 - e, e).wait_recv()
                i = OFF - 1 if e == 0 else OFF + nm
                got = sface[1, e]
                sr[i, pl.ds(PAD, half, stride=2), :] = got
                sr[i, pl.ds(PAD + 1, half, stride=2), :] = got

    def at(p):
        return jnp.where(flip, nm - 1 - p, p)

    def half_red(t, p):
        red_pair(t, at(p))

    def halo_red(t, late):
        late = int(late)

        @pl.when((flip & has[1 - late]) | (jnp.logical_not(flip) & has[late]))
        def _():
            red_pair(t, at(nm if late else -1))

    def on_first(t, do):
        if not isinstance(t, int):
            pl.when(t == 0)(do)
        elif t == 0:
            do()

    def sweep(t, emitter):
        arrive_faces(t)
        arrive_x(t, False)

        def red_body(p, carry):
            half_red(t, p)
            return carry

        lax.fori_loop(0, nm - 1, red_body, 0)
        arrive_diagonals(t)
        on_first(t, take_source)
        edge_red(t)
        red_rows(t)
        on_first(t, lambda: take_source_x(False))
        halo_red(t, False)

        def black_body(p, carry):
            emitter(at(p))
            return carry

        lax.fori_loop(0, nm - 2, black_body, 0)
        arrive_x(t, True)
        lax.fori_loop(nm - 1, nm, red_body, 0)
        on_first(t, lambda: take_source_x(True))
        halo_red(t, True)
        lax.fori_loop(nm - 2, nm, black_body, 0)

    def full(t, carry):
        def red_inner(m, carry):
            red_pair(t, m, inner=True, edged=False)
            return carry

        def black_inner(m, carry):
            parts = [zeros8] * 4

            def emit(blk0, y):
                xb[t + 1, OFF + m, pl.ds(PAD + 8 * blk0, 8 * GROUP), :] = flat(y)
                pick(parts, y, blk0)

            black_pair(m, emit, edged=False)
            fb[t + 1, m] = merge(parts)
            return carry

        lax.fori_loop(0, nm, red_inner, 0)
        lax.fori_loop(1, nm - 1, black_inner, 0)

        def side(late):
            arrive_x(t, late)
            on_first(t, lambda: take_source_x(late))
            q = at(nm - 1 if late else 0)
            red_pair(t, q, edged=False)
            h = int(late)

            @pl.when((flip & has[1 - h]) | (jnp.logical_not(flip) & has[h]))
            def _():
                red_pair(t, at(nm if late else -1), edged=False)

            parts = [zeros8] * 4

            def emit(blk0, y):
                v = y + jnp.stack([lift(q, blk0 + k) for k in range(GROUP)], axis=0)
                xb[t + 1, OFF + q, pl.ds(PAD + 8 * blk0, 8 * GROUP), :] = flat(v)
                pick(parts, v, blk0)

            black_pair(q, emit, edged=False)
            fb[t + 1, q] = merge(parts)

        arrive_faces(t)
        arrive_diagonals(t)
        on_first(t, take_source)
        edge_red(t)
        edge_response(t)
        red_rows(t, edged=False)
        red_borders(t)
        side(False)
        side(True)
        black_borders(t)
        messages(t + 1, lambda m: fb[t + 1, m])
        send_all(t + 1)
        lift_rest(t + 1)
        return carry

    lax.fori_loop(0, SWEEPS - 1, full, 0)

    def final(m):
        def emit(blk0, y):
            red = three(rb[OFF + m, pl.ds(PAD + 8 * blk0, 8 * GROUP), :])
            rs = pl.ds(8 * blk0, 8 * GROUP)
            odd = rep(odd8, GROUP)
            ov[2 * m, rs, :] = flat(jnp.where(odd, y, red))
            ov[2 * m + 1, rs, :] = flat(jnp.where(odd, red, y))

        black_pair(m, emit)

    sweep(SWEEPS - 1, final)

    def drain(t, carry):
        for c in face_copies(t):
            c.wait_send()
        for e in range(2):
            @pl.when(has[e])
            def _():
                for c in wall_copies(t, e):
                    c.wait_send()
        return carry

    lax.fori_loop(0, SWEEPS, drain, 0)
    for e in range(2):
        sz_copy(e).wait_send()
        sy_copy(e).wait_send()

        @pl.when(has[e])
        def _():
            sx_copy(e).wait_send()


def solution(mesh):
    sizes = tuple(mesh.shape[a] for a in ("gx", "gy", "gz"))

    def on_device(field, source):
        planes, rows, cols = field.shape
        nm = planes // 2
        assert planes % 4 == 0 and rows == 256 and cols == 128 and rows % (8 * GROUP) == 0
        f32 = jnp.float32
        wide = (nm + 2 * OFF, rows + 2 * PAD, cols)
        return pl.pallas_call(
            functools.partial(kernel, sizes),
            out_shape=jax.ShapeDtypeStruct(field.shape, f32),
            in_specs=[pl.BlockSpec(memory_space=pltpu.HBM)] * 2,
            out_specs=pl.BlockSpec(memory_space=pltpu.VMEM),
            scratch_shapes=[
                pltpu.VMEM(field.shape, f32),
                pltpu.VMEM(field.shape, f32),
                pltpu.VMEM((SWEEPS, *wide), f32),
                pltpu.VMEM(wide, f32),
                pltpu.VMEM(wide, f32),
                pltpu.VMEM((nm, rows, cols), f32),
                pltpu.VMEM((SWEEPS, nm, 8, cols), f32),
                *[pltpu.VMEM((SWEEPS, nm // 2, 8, cols), f32)] * 4,
                pltpu.VMEM((SWEEPS, 4, 8, cols), f32),
                pltpu.VMEM((2, SWEEPS, 4, nm // 2, cols), f32),
                pltpu.VMEM((nm + 2, 8, cols), f32),
                *[pltpu.VMEM((nm, 8, cols), f32)] * 5,
                *[pltpu.VMEM((2, SWEEPS + 1, nm, 2, cols), f32)] * 2,
                *[pltpu.VMEM((4, SWEEPS, 1, cols), f32)] * 2,
                pltpu.VMEM((2, 2, rows // 2, cols), f32),
                pltpu.VMEM((2, 2, nm // 4, 8, cols), f32),
                pltpu.SemaphoreType.DMA((24, SWEEPS)),
                pltpu.SemaphoreType.DMA((24, SWEEPS)),
                pltpu.SemaphoreType.DMA((nm,)),
                pltpu.SemaphoreType.DMA((nm,)),
            ],
            compiler_params=pltpu.CompilerParams(
                collective_id=0, has_side_effects=True, vmem_limit_bytes=60 * 1024 * 1024
            ),
        )(field, source)

    spec = P("gx", "gy", "gz")
    return jax.shard_map(on_device, mesh=mesh, in_specs=(spec, spec), out_specs=spec, check_vma=False)
```

```python
import functools

import jax
import jax.numpy as jnp
from jax import lax
from jax.experimental import pallas as pl
from jax.experimental.pallas import tpu as pltpu
from jax.sharding import PartitionSpec as P

SWEEPS = 3
MESH = pl.DeviceIdType.MESH
PAD = 16
OFF = 2
GROUP = 8
THIRD = 1.0 / 6.0


def kernel(sizes, f_hbm, s_hbm, ov, fv, sv, xb, rb, sr, sb, fb, mh, ml, lz, hz, dg, cn, g, rd, sg, cu, cd, dz, ystage, yland, xystage, xyland, sface, sedge,
           send, recv, fsem, ssem):
    ngx, ngy, ngz = sizes
    planes, rows, cols = f_hbm.shape
    nm = planes // 2
    blocks = rows // 8
    gx, gy, gz = (lax.axis_index(a) for a in ("gx", "gy", "gz"))
    has_lo, has_hi = gx > 0, gx < ngx - 1
    y_lo, y_hi = lax.rem(gy + ngy - 1, ngy), lax.rem(gy + 1, ngy)
    z_lo, z_hi = lax.rem(gz + ngz - 1, ngz), lax.rem(gz + 1, ngz)
    x_to = (gx - 1, gx + 1)
    y_to = (y_lo, y_hi)
    z_to = (z_lo, z_hi)
    has = (has_lo, has_hi)
    flip = gx >= ngx // 2
    order = [m for a in range(nm // 2) for m in (a, nm - 1 - a)]

    def load(ref, to, sem, m):
        return pltpu.make_async_copy(ref.at[pl.ds(2 * m, 2)], to.at[pl.ds(2 * m, 2)], sem.at[m])

    barrier = pltpu.get_barrier_semaphore()

    def greet(device):
        pl.semaphore_signal(barrier, inc=1, device_id=device, device_id_type=MESH)

    for e in range(2):
        greet({"gy": y_to[e]})
        greet({"gz": z_to[e]})
        for d in range(2):
            greet({"gy": y_to[e], "gz": z_to[d]})

        @pl.when(has[e])
        def _():
            greet({"gx": x_to[e]})
            for d in range(2):
                greet({"gx": x_to[e], "gy": y_to[d]})
                greet({"gx": x_to[e], "gz": z_to[d]})

    for m in order:
        load(f_hbm, fv, fsem, m).start()
    for m in order:
        load(s_hbm, sv, ssem, m).start()

    row8 = lax.broadcasted_iota(jnp.int32, (8, cols), 0)
    lane = lax.broadcasted_iota(jnp.int32, (8, cols), 1)
    off = lax.rem(lane, 4)
    quad = lax.div(lane, 4)
    odd8 = lax.rem(row8 + lane, 2) == 1
    odd_edge = lax.rem(row8 + off, 2) == 0
    mid = lax.rem(off + 1, 4) >= 2
    brim = lax.rem(lane + 2, cols) < 4
    first8, last8 = lane == 0, lane == cols - 1

    def rep(mask, n):
        return jnp.broadcast_to(mask[None], (n, 8, cols))

    def roll(v, k):
        k = k % cols
        return v if k == 0 else pltpu.roll(v, k, v.ndim - 1)

    def three(v):
        return v.reshape(v.shape[0] // 8, 8, cols)

    def flat(v):
        return v.reshape(v.shape[0] * 8, cols)

    def pick(parts, y, blk0):
        for k in range(y.shape[0]):
            blk = blk0 + k
            j = blk % len(parts)
            parts[j] = jnp.where(quad == blk, roll(y[k], 4 * blk + 2), parts[j])
        return parts

    def merge(parts):
        while len(parts) > 1:
            parts = [p + q for p, q in zip(parts[::2], parts[1::2])]
        return parts[0]

    zeros8 = jnp.zeros((8, cols), jnp.float32)

    def copy(k, t, src, dst, to, back):
        return pltpu.make_async_remote_copy(
            src_ref=src, dst_ref=dst, send_sem=send.at[k, t], recv_sem=recv.at[back, t], device_id=to, device_id_type=MESH
        )

    def x_copy(t, e, via=None):
        m, to = (0, nm) if e == 0 else (nm - 1, -1)
        return copy(e, t, xb.at[t, OFF + m, pl.ds(PAD, rows)], xb.at[t, OFF + to, pl.ds(PAD, rows)], {"gx": x_to[e if via is None else via]}, 1 - e)

    def y_copy(t, e):
        return copy(2 + e, t, ystage.at[e, t], yland.at[1 - e, t], {"gy": y_to[e]}, 3 - e)

    def z_copy(t, e):
        src, dst = (ml, hz) if e == 0 else (mh, lz)
        return copy(4 + e, t, src.at[t], dst.at[t], {"gz": z_to[e]}, 5 - e)

    def xy_copy(t, e, d, via=None):
        k, back = 6 + 2 * e + d, 6 + 2 * (1 - e) + 1 - d
        return copy(k, t, xystage.at[k - 6, t], xyland.at[back - 6, t], {"gx": x_to[e if via is None else via], "gy": y_to[d]}, back)

    def xz_copy(t, e, d, via=None):
        k, back = 10 + 2 * e + d, 10 + 2 * (1 - e) + 1 - d
        j = 0 if e == 0 else nm // 2 - 1
        return copy(k, t, (ml, mh)[d].at[t, j], dg.at[t, back - 10], {"gx": x_to[e if via is None else via], "gz": z_to[d]}, back)

    def yz_copy(t, e, d):
        k, back = 14 + 2 * e + d, 14 + 2 * (1 - e) + 1 - d
        return copy(k, t, cn.at[1, t, k - 14], cn.at[0, t, back - 14], {"gy": y_to[e], "gz": z_to[d]}, back)

    def sx_copy(e, via=None):
        return copy(18 + e, 0, sface.at[0, e], sface.at[1, 1 - e], {"gx": x_to[e if via is None else via]}, 19 - e)

    def sy_copy(e):
        return copy(20 + e, 0, ystage.at[e, SWEEPS], yland.at[1 - e, SWEEPS], {"gy": y_to[e]}, 21 - e)

    def sz_copy(e):
        return copy(22 + e, 0, sedge.at[0, e], sedge.at[1, 1 - e], {"gz": z_to[e]}, 23 - e)

    def face_copies(t):
        return [y_copy(t, e) for e in range(2)] + [z_copy(t, e) for e in range(2)] + [yz_copy(t, e, d) for e in range(2) for d in range(2)]

    def wall_copies(t, e):
        return [x_copy(t, e)] + [xy_copy(t, e, d) for d in range(2)] + [xz_copy(t, e, d) for d in range(2)]

    def messages(t, src):
        for j in range(nm // 2):
            even, odd = src(2 * j), src(2 * j + 1)
            mh[t, j] = jnp.where(off < 2, even, roll(odd, 2))
            ml[t, j] = jnp.where(off < 2, roll(even, -2), odd)

    def send_all(t, between=None):
        for e in range(2):
            r = 0 if e == 0 else 7
            for d in range(2):
                cn[1, t, 2 * e + d] = (ml, mh)[d][t, :, r, :]
        for e in range(2):
            for d in range(2):
                m = 0 if e == 0 else nm - 1
                r = PAD if d == 0 else PAD + rows - 1
                xystage[2 * e + d, t] = xb[t, OFF + m, pl.ds(r, 1), :]
        for e in range(2):
            for d in range(2):
                yz_copy(t, e, d).start()
        for e in range(2):
            @pl.when(has[e])
            def _():
                for d in range(2):
                    xz_copy(t, e, d).start()
                for d in range(2):
                    xy_copy(t, e, d).start()
        for e in range(2):
            z_copy(t, e).start()
        for e in range(2):
            r = PAD if e == 0 else PAD + rows - 2
            for m in range(nm):
                ystage[e, t, m] = xb[t, OFF + m, pl.ds(r, 2), :]
            y_copy(t, e).start()
        if between is not None:
            between()
        for e in range(2):
            @pl.when(has[e])
            def _():
                x_copy(t, e).start()

    def arrive_faces(t):
        for e in range(2):
            z_copy(t, e).wait_recv()
        for e in range(2):
            y_copy(t, e).wait_recv()
        for e in range(2):
            r = PAD - 2 if e == 0 else PAD + rows
            for m in range(nm):
                xb[t, OFF + m, pl.ds(r, 2), :] = yland[e, t, m]
        for j in range(nm // 2):
            low, high = lz[t, j], hz[t, j]
            l1, l3, lm = roll(low, 1), roll(low, 3), roll(low, -1)
            h1, h3, hm = roll(high, 1), roll(high, -3), roll(high, -1)
            g[1 + 2 * j] = jnp.where(off < 2, jnp.where(off == 0, hm, h1), jnp.where(off == 2, l1, l3))
            g[2 + 2 * j] = jnp.where(off < 2, jnp.where(off == 0, h3, hm), jnp.where(off == 2, lm, l1))

    def arrive_diagonals(t):
        for e in range(2):
            for d in range(2):
                yz_copy(t, e, d).wait_recv()
        for j in range(nm // 2):
            for p in range(2):
                a, b = (jnp.broadcast_to(cn[0, t, k, pl.ds(j, 1), :], (8, cols)) for k in (0, 1))
                cu[2 * j + p] = jnp.where(off == 2, roll(a, 5 - 2 * p), roll(b, 5 - 2 * p))
                a, b = (jnp.broadcast_to(cn[0, t, k, pl.ds(j, 1), :], (8, cols)) for k in (2, 3))
                cd[2 * j + p] = jnp.where(off == 2, roll(a, -3 - 2 * p), roll(b, -3 - 2 * p))
        for e in range(2):
            @pl.when(has[e])
            def _():
                for d in range(2):
                    xz_copy(t, 1 - e, d, e).wait_recv()
                k = -1 if e == 0 else 1
                g[0 if e == 0 else nm + 1] = jnp.where(off == 2, roll(dg[t, 2 * e], k), roll(dg[t, 2 * e + 1], k))

    def arrive_xy(t):
        for e in range(2):
            @pl.when(has[e])
            def _():
                for d in range(2):
                    xy_copy(t, 1 - e, d, e).wait_recv()
                i = OFF - 1 if e == 0 else OFF + nm
                for d in range(2):
                    r = PAD - 1 if d == 0 else PAD + rows
                    xb[t, i, pl.ds(r, 1), :] = xyland[2 * e + d, t]

    def arrive_x(t, late):
        for e in range(2):
            @pl.when(has[e] & (flip if (e == 0) == late else jnp.logical_not(flip)))
            def _():
                x_copy(t, 1 - e, e).wait_recv()

    def edge_red(t):
        for m in range(nm):
            v = g[1 + m]
            up = pltpu.roll(jnp.where(row8 == 7, jnp.where(lane < 4, cu[m], roll(v, 4)), v), 1, 0)
            down = pltpu.roll(jnp.where(row8 == 0, jnp.where(lane >= cols - 4, cd[m], roll(v, -4)), v), 7, 0)
            side = jnp.where(off == 1, roll(v, 1), roll(v, -1))
            beside = jnp.where(odd_edge, g[2 + m], g[m])
            rd[m] = (((sg[m] + v) + (beside + up)) + ((down + side) + fb[t, m])) * jnp.float32(THIRD)

    def relax(read, i, blk0, n, src, c, inner=False):
        rs = PAD + 8 * blk0
        here = three(read(i, rs, 8 * n))
        below_at, above_at = i - 1, i + 1
        if inner:
            below_at, above_at = below_at + (nm - (i - OFF)) // nm, above_at - (i - OFF) // (nm - 1)
        below, above = three(read(below_at, rs, 8 * n)), three(read(above_at, rs, 8 * n))
        odd = rep(odd8, n)
        beside = jnp.where(odd, above, below) if c == 0 else jnp.where(odd, below, above)
        total = (three(src) + here) + beside
        total = total + three(read(i, rs - 1, 8 * n))
        total = total + three(read(i, rs + 1, 8 * n))
        return beside_lanes(total, here) * jnp.float32(THIRD)

    def beside_lanes(total, here):
        n = here.shape[0]
        total = total + jnp.where(rep(first8, n), 0.0, roll(here, 1))
        return total + jnp.where(rep(last8, n), 0.0, roll(here, -1))

    def red_pair(t, m, inner=False, keep=None):
        i = m + OFF

        def read(i, r, n):
            return xb[t, i, pl.ds(r, n), :]

        for blk0 in range(0, blocks, GROUP):
            y = relax(read, i, blk0, GROUP, sr[i, pl.ds(PAD + 8 * blk0, 8 * GROUP), :], 0, inner)
            if keep is not None:
                y = jnp.where(keep, y, 0.0)
            rb[i, pl.ds(PAD + 8 * blk0, 8 * GROUP), :] = flat(y)

    def relax_block(x, src, lo, n, r, c, inner=False):
        def read(i, r):
            return x[pl.ds(i, n), pl.ds(r, 8), :]

        odd = rep(odd8, n)
        here = read(lo, r)
        if inner:
            below, above = (jnp.concatenate(p, axis=0) for p in ((here[:1], here[:-1]), (here[1:], here[-1:])))
        else:
            below, above = read(lo - 1, r), read(lo + 1, r)
        total = (src + here) + (jnp.where(odd, above, below) if c == 0 else jnp.where(odd, below, above))
        total = (total + read(lo, r - 1)) + read(lo, r + 1)
        return beside_lanes(total, here) * jnp.float32(THIRD)

    def red_rows(t):
        for r in (PAD - 8, PAD + rows):
            src = sr[pl.ds(OFF, nm), pl.ds(r, 8), :]
            rb[pl.ds(OFF, nm), pl.ds(r, 8), :] = relax_block(xb.at[t], src, OFF, nm, r, 0)

    def red_borders(t):
        for r in (PAD, PAD + rows - 8):
            src = sr[pl.ds(OFF, nm), pl.ds(r, 8), :]
            rb[pl.ds(OFF, nm), pl.ds(r, 8), :] = relax_block(xb.at[t], src, OFF, nm, r, 0, inner=True)

    def lift(m, blk):
        return jnp.where(brim, roll(dz[m], -(4 * blk + 2)), 0.0)

    def black_borders(t):
        for blk in (0, blocks - 1):
            r = PAD + 8 * blk
            y = relax_block(rb, sb[pl.ds(1, nm - 2), pl.ds(8 * blk, 8), :], OFF + 1, nm - 2, r, 1)
            xb[t + 1, pl.ds(OFF + 1, nm - 2), pl.ds(r, 8), :] = y
            for m in range(1, nm - 1):
                fb[t + 1, m] = jnp.where(quad == blk, roll(y[m - 1], 4 * blk + 2), fb[t + 1, m])

    def lift_borders(t):
        for m in range(1, nm - 1):
            for blk in (0, blocks - 1):
                rs = pl.ds(PAD + 8 * blk, 8)
                xb[t, OFF + m, rs, :] = xb[t, OFF + m, rs, :] + lift(m, blk)
            fb[t, m] = fb[t, m] + dz[m]

    def edge_response(t):
        def middle(v):
            return jnp.where(mid, v, 0.0)

        for m in range(nm):
            v = middle(g[1 + m])
            up = pltpu.roll(jnp.where(row8 == 7, jnp.where(lane < 4, middle(cu[m]), roll(v, 4)), v), 1, 0)
            down = pltpu.roll(jnp.where(row8 == 0, jnp.where(lane >= cols - 4, middle(cd[m]), roll(v, -4)), v), 7, 0)
            beside = jnp.where(odd_edge, middle(g[2 + m]), middle(g[m]))
            near = (rd[m] + ((v + beside) + (up + down)) * jnp.float32(THIRD)) * jnp.float32(THIRD)
            far = jnp.where(off == 0, roll(v, -1), roll(v, 1)) * jnp.float32(THIRD * THIRD)
            dz[m] = jnp.where(mid, near, far)

    def lift_pair(t, m, first, last):
        v = dz[m]
        for blk0 in range(0, blocks, GROUP):
            lo, hi = max(blk0, first), min(blk0 + GROUP, last)
            rs = pl.ds(PAD + 8 * lo, 8 * (hi - lo))
            y = jnp.stack([roll(v, -(4 * blk + 2)) for blk in range(lo, hi)], axis=0)
            xb[t, OFF + m, rs, :] = xb[t, OFF + m, rs, :] + flat(jnp.where(rep(brim, hi - lo), y, 0.0))

    def lift_rest(t):
        def body(m, carry):
            lift_pair(t, m, 1, blocks - 1)
            return carry

        lax.fori_loop(1, nm - 1, body, 0)

    def black_pair(m, emit):
        i = m + OFF

        def read(i, r, n):
            return rb[i, pl.ds(r, n), :]

        for blk0 in range(0, blocks, GROUP):
            rs = pl.ds(8 * blk0, 8 * GROUP)
            emit(blk0, relax(read, i, blk0, GROUP, sb[m, rs, :], 1))

    zero = jnp.zeros((rows + 16, cols), jnp.float32)
    for e in range(2):
        @pl.when(jnp.logical_not(has[e]))
        def _():
            i = OFF - 1 if e == 0 else OFF + nm
            for t in range(SWEEPS):
                xb[t, i, pl.ds(PAD - 8, rows + 16), :] = zero
            rb[i, pl.ds(PAD - 8, rows + 16), :] = zero
            g[0 if e == 0 else nm + 1] = zeros8

    def pack_field(a, carry):
        for m in (a, nm - 1 - a):
            load(f_hbm, fv, fsem, m).wait()
            parts = [zeros8] * 4
            for blk0 in range(0, blocks, GROUP):
                rs = pl.ds(8 * blk0, 8 * GROUP)
                y = jnp.where(rep(odd8, GROUP), three(fv[2 * m, rs, :]), three(fv[2 * m + 1, rs, :]))
                xb[0, OFF + m, pl.ds(PAD + 8 * blk0, 8 * GROUP), :] = flat(y)
                parts = pick(parts, y, blk0)
            fb[0, m] = merge(parts)
        return carry

    def pack_source(a, carry):
        for m in (a, nm - 1 - a):
            load(s_hbm, sv, ssem, m).wait()
            parts = [zeros8] * 4
            for blk0 in range(0, blocks, GROUP):
                rs = pl.ds(8 * blk0, 8 * GROUP)
                low, high = three(sv[2 * m, rs, :]), three(sv[2 * m + 1, rs, :])
                y = jnp.where(rep(odd8, GROUP), high, low)
                sr[OFF + m, pl.ds(PAD + 8 * blk0, 8 * GROUP), :] = flat(y)
                sb[m, rs, :] = flat(jnp.where(rep(odd8, GROUP), low, high))
                parts = pick(parts, y, blk0)
            sg[m] = merge(parts)
        return carry

    lax.fori_loop(0, nm // 2, pack_field, 0)
    messages(0, lambda m: fb[0, m])
    lax.fori_loop(0, nm // 2, pack_source, 0)
    half = rows // 2
    odd_lane = lax.rem(lax.broadcasted_iota(jnp.int32, (half, cols), 1), 2) == 1
    for e in range(2):
        for j in range(nm // 4):
            parts = [roll(sg[4 * j + k], k - 2 + e) for k in range(4)]
            sedge[0, e, j] = jnp.where(off < 2, jnp.where(off == 0, parts[0], parts[1]), jnp.where(off == 2, parts[2], parts[3]))
        r = PAD if e == 0 else PAD + rows - 1
        for m in range(nm):
            ystage[e, SWEEPS, m, pl.ds(0, 1), :] = sr[OFF + m, pl.ds(r, 1), :]

    pl.semaphore_wait(barrier, 8 + 5 * (has_lo.astype(jnp.int32) + has_hi.astype(jnp.int32)))
    def send_source():
        for e in range(2):
            sz_copy(e).start()
            sy_copy(e).start()

    send_all(0, send_source)
    for e in range(2):
        @pl.when(has[e])
        def _():
            i = OFF if e == 0 else OFF + nm - 1
            even = sr[i, pl.ds(PAD, half, stride=2), :]
            odd = sr[i, pl.ds(PAD + 1, half, stride=2), :]
            sface[0, e] = jnp.where(odd_lane, odd, even) if e == 0 else jnp.where(odd_lane, even, odd)
            sx_copy(e).start()

    def take_source():
        for e in range(2):
            sz_copy(e).wait_recv()
            sy_copy(e).wait_recv()
        for e in range(2):
            r = PAD - 1 if e == 0 else PAD + rows
            for m in range(nm):
                sr[OFF + m, pl.ds(r, 1), :] = yland[e, SWEEPS, m, pl.ds(0, 1), :]
        for j in range(nm // 4):
            low, high = sedge[1, 0, j], sedge[1, 1, j]
            for k in range(4):
                sg[4 * j + k] = jnp.where(off == 1, roll(high, 1 - k), roll(low, 2 - k))

    def take_source_x(late):
        for e in range(2):
            @pl.when(has[e] & (flip if (e == 0) == late else jnp.logical_not(flip)))
            def _():
                sx_copy(1 - e, e).wait_recv()
                i = OFF - 1 if e == 0 else OFF + nm
                got = sface[1, e]
                sr[i, pl.ds(PAD, half, stride=2), :] = got
                sr[i, pl.ds(PAD + 1, half, stride=2), :] = got

    def at(p):
        return jnp.where(flip, nm - 1 - p, p)

    def on_first(t, do):
        pl.when(t == 0)(do)

    def full(t, carry):
        def red_inner(m, carry):
            red_pair(t, m, inner=True)
            return carry

        def black_inner(m, carry):
            parts = [zeros8] * 4

            def emit(blk0, y):
                xb[t + 1, OFF + m, pl.ds(PAD + 8 * blk0, 8 * GROUP), :] = flat(y)
                pick(parts, y, blk0)

            black_pair(m, emit)
            fb[t + 1, m] = merge(parts)
            return carry

        lax.fori_loop(0, nm, red_inner, 0)
        lax.fori_loop(1, nm - 1, black_inner, 0)

        def side_red(late):
            arrive_x(t, late)
            on_first(t, lambda: take_source_x(late))
            h = int(late)
            keep = jnp.where(flip, has[1 - h], has[h])
            red_pair(t, at(nm - 1 if late else 0))
            red_pair(t, at(nm if late else -1), keep=keep)

        def side_black(late):
            q = at(nm - 1 if late else 0)
            parts = [zeros8] * 4

            def emit(blk0, y):
                if late:
                    y = y + jnp.stack([lift(q, blk0 + k) for k in range(GROUP)], axis=0)
                xb[t + 1, OFF + q, pl.ds(PAD + 8 * blk0, 8 * GROUP), :] = flat(y)
                pick(parts, y, blk0)

            black_pair(q, emit)
            fb[t + 1, q] = merge(parts)

        arrive_faces(t)
        arrive_xy(t)
        red_borders(t)
        side_red(False)
        on_first(t, take_source)
        red_rows(t)
        black_borders(t)
        side_black(False)
        arrive_diagonals(t)
        edge_red(t)
        edge_response(t)
        lift_borders(t + 1)
        early = at(0)
        lift_pair(t + 1, early, 0, blocks)
        fb[t + 1, early] = fb[t + 1, early] + dz[early]
        side_red(True)
        side_black(True)

        @pl.when(t < SWEEPS - 1)
        def _():
            messages(t + 1, lambda m: fb[t + 1, m])
            send_all(t + 1)
            lift_rest(t + 1)

        return carry

    lax.fori_loop(0, SWEEPS, full, 0)
    for m in (0, nm - 1):
        dz[m] = zeros8

    def write(m, carry):
        lr = jnp.where(mid, g[1 + m], 0.0) * jnp.float32(THIRD)
        lb = dz[m]
        low, high = jnp.where(odd_edge, lr, lb), jnp.where(odd_edge, lb, lr)
        low_red, high_red = jnp.where(odd_edge, lr, 0.0), jnp.where(odd_edge, 0.0, lr)
        for blk0 in range(0, blocks, GROUP):
            rs, ps = pl.ds(8 * blk0, 8 * GROUP), pl.ds(PAD + 8 * blk0, 8 * GROUP)
            red, black = three(rb[OFF + m, ps, :]), three(xb[SWEEPS, OFF + m, ps, :])
            odd, edge = rep(odd8, GROUP), rep(brim, GROUP)

            def add(inside, outer):
                return jnp.stack([roll(outer if blk in (0, blocks - 1) else inside, -(4 * blk + 2)) for blk in range(blk0, blk0 + GROUP)], axis=0)

            ov[2 * m, rs, :] = flat(jnp.where(odd, black, red) + jnp.where(edge, add(low, low_red), 0.0))
            ov[2 * m + 1, rs, :] = flat(jnp.where(odd, red, black) + jnp.where(edge, add(high, high_red), 0.0))
        return carry

    lax.fori_loop(0, nm, write, 0, unroll=2)

    def drain(t, carry):
        for c in face_copies(t):
            c.wait_send()
        for e in range(2):
            @pl.when(has[e])
            def _():
                for c in wall_copies(t, e):
                    c.wait_send()
        return carry

    lax.fori_loop(0, SWEEPS, drain, 0)
    for e in range(2):
        sz_copy(e).wait_send()
        sy_copy(e).wait_send()

        @pl.when(has[e])
        def _():
            sx_copy(e).wait_send()


def solution(mesh):
    sizes = tuple(mesh.shape[a] for a in ("gx", "gy", "gz"))

    def on_device(field, source):
        planes, rows, cols = field.shape
        nm = planes // 2
        assert planes % 4 == 0 and rows == 256 and cols == 128 and rows % (8 * GROUP) == 0
        f32 = jnp.float32
        wide = (nm + 2 * OFF, rows + 2 * PAD, cols)
        return pl.pallas_call(
            functools.partial(kernel, sizes),
            out_shape=jax.ShapeDtypeStruct(field.shape, f32),
            in_specs=[pl.BlockSpec(memory_space=pltpu.HBM)] * 2,
            out_specs=pl.BlockSpec(memory_space=pltpu.VMEM),
            scratch_shapes=[
                pltpu.VMEM(field.shape, f32),
                pltpu.VMEM(field.shape, f32),
                pltpu.VMEM((SWEEPS + 1, *wide), f32),
                pltpu.VMEM(wide, f32),
                pltpu.VMEM(wide, f32),
                pltpu.VMEM((nm, rows, cols), f32),
                pltpu.VMEM((SWEEPS + 1, nm, 8, cols), f32),
                *[pltpu.VMEM((SWEEPS, nm // 2, 8, cols), f32)] * 4,
                pltpu.VMEM((SWEEPS, 4, 8, cols), f32),
                pltpu.VMEM((2, SWEEPS, 4, nm // 2, cols), f32),
                pltpu.VMEM((nm + 2, 8, cols), f32),
                *[pltpu.VMEM((nm, 8, cols), f32)] * 5,
                *[pltpu.VMEM((2, SWEEPS + 1, nm, 2, cols), f32)] * 2,
                *[pltpu.VMEM((4, SWEEPS, 1, cols), f32)] * 2,
                pltpu.VMEM((2, 2, rows // 2, cols), f32),
                pltpu.VMEM((2, 2, nm // 4, 8, cols), f32),
                pltpu.SemaphoreType.DMA((24, SWEEPS)),
                pltpu.SemaphoreType.DMA((24, SWEEPS)),
                pltpu.SemaphoreType.DMA((nm,)),
                pltpu.SemaphoreType.DMA((nm,)),
            ],
            compiler_params=pltpu.CompilerParams(
                collective_id=0, has_side_effects=True, vmem_limit_bytes=60 * 1024 * 1024
            ),
        )(field, source)

    spec = P("gx", "gy", "gz")
    return jax.shard_map(on_device, mesh=mesh, in_specs=(spec, spec), out_specs=spec, check_vma=False)
```

```python
import functools

import jax
import jax.numpy as jnp
from jax import lax
from jax.experimental import pallas as pl
from jax.experimental.pallas import tpu as pltpu
from jax.sharding import PartitionSpec as P

SWEEPS = 3
MESH = pl.DeviceIdType.MESH
PAD = 16
OFF = 2
GROUP = 8
THIRD = 1.0 / 6.0


def kernel(sizes, f_hbm, s_hbm, ov, fv, sv, xb, rb, sr, sb, fb, mh, ml, lz, hz, dg, cn, g, rd, sg, cu, cd, dz, ystage, yland, xystage, xyland, sface, sedge,
           send, recv, fsem, ssem):
    ngx, ngy, ngz = sizes
    planes, rows, cols = f_hbm.shape
    nm = planes // 2
    blocks = rows // 8
    gx, gy, gz = (lax.axis_index(a) for a in ("gx", "gy", "gz"))
    has_lo, has_hi = gx > 0, gx < ngx - 1
    y_lo, y_hi = lax.rem(gy + ngy - 1, ngy), lax.rem(gy + 1, ngy)
    z_lo, z_hi = lax.rem(gz + ngz - 1, ngz), lax.rem(gz + 1, ngz)
    x_to = (gx - 1, gx + 1)
    y_to = (y_lo, y_hi)
    z_to = (z_lo, z_hi)
    has = (has_lo, has_hi)
    flip = gx >= ngx // 2
    order = [m for a in range(nm // 2) for m in (a, nm - 1 - a)]

    def load(ref, to, sem, m):
        return pltpu.make_async_copy(ref.at[pl.ds(2 * m, 2)], to.at[pl.ds(2 * m, 2)], sem.at[m])

    barrier = pltpu.get_barrier_semaphore()

    def greet(device):
        pl.semaphore_signal(barrier, inc=1, device_id=device, device_id_type=MESH)

    for e in range(2):
        greet({"gy": y_to[e]})
        greet({"gz": z_to[e]})
        for d in range(2):
            greet({"gy": y_to[e], "gz": z_to[d]})

        @pl.when(has[e])
        def _():
            greet({"gx": x_to[e]})
            for d in range(2):
                greet({"gx": x_to[e], "gy": y_to[d]})
                greet({"gx": x_to[e], "gz": z_to[d]})

    for m in order:
        load(f_hbm, fv, fsem, m).start()
    for m in order:
        load(s_hbm, sv, ssem, m).start()

    row8 = lax.broadcasted_iota(jnp.int32, (8, cols), 0)
    lane = lax.broadcasted_iota(jnp.int32, (8, cols), 1)
    off = lax.rem(lane, 4)
    quad = lax.div(lane, 4)
    parity8 = lax.rem(row8 + lane, 2)
    odd8 = parity8 == 1
    odd_edge = lax.rem(row8 + off, 2) == 0
    mid = lax.rem(off + 1, 4) >= 2
    brim = lax.rem(lane + 2, cols) < 4
    first8, last8 = lane == 0, lane == cols - 1

    def rep(mask, n):
        return jnp.broadcast_to(mask[None], (n, 8, cols))

    def roll(v, k):
        k = k % cols
        return v if k == 0 else pltpu.roll(v, k, v.ndim - 1)

    def three(v):
        return v.reshape(v.shape[0] // 8, 8, cols)

    def flat(v):
        return v.reshape(v.shape[0] * 8, cols)

    def pick(parts, y, blk0):
        for k in range(y.shape[0]):
            blk = blk0 + k
            j = blk % len(parts)
            parts[j] = jnp.where(quad == blk, roll(y[k], 4 * blk + 2), parts[j])
        return parts

    def merge(parts):
        while len(parts) > 1:
            parts = [p + q for p, q in zip(parts[::2], parts[1::2])]
        return parts[0]

    zeros8 = jnp.zeros((8, cols), jnp.float32)

    def copy(k, t, src, dst, to, back):
        return pltpu.make_async_remote_copy(
            src_ref=src, dst_ref=dst, send_sem=send.at[k, t], recv_sem=recv.at[back, t], device_id=to, device_id_type=MESH
        )

    def x_copy(t, e, via=None):
        m, to = (0, nm) if e == 0 else (nm - 1, -1)
        return copy(e, t, xb.at[t, OFF + m, pl.ds(PAD, rows)], xb.at[t, OFF + to, pl.ds(PAD, rows)], {"gx": x_to[e if via is None else via]}, 1 - e)

    def y_copy(t, e):
        return copy(2 + e, t, ystage.at[e, t], yland.at[1 - e, t], {"gy": y_to[e]}, 3 - e)

    def z_copy(t, e):
        src, dst = (ml, hz) if e == 0 else (mh, lz)
        return copy(4 + e, t, src.at[t], dst.at[t], {"gz": z_to[e]}, 5 - e)

    def xy_copy(t, e, d, via=None):
        k, back = 6 + 2 * e + d, 6 + 2 * (1 - e) + 1 - d
        return copy(k, t, xystage.at[k - 6, t], xyland.at[back - 6, t], {"gx": x_to[e if via is None else via], "gy": y_to[d]}, back)

    def xz_copy(t, e, d, via=None):
        k, back = 10 + 2 * e + d, 10 + 2 * (1 - e) + 1 - d
        j = 0 if e == 0 else nm // 2 - 1
        return copy(k, t, (ml, mh)[d].at[t, j], dg.at[t, back - 10], {"gx": x_to[e if via is None else via], "gz": z_to[d]}, back)

    def yz_copy(t, e, d):
        k, back = 14 + 2 * e + d, 14 + 2 * (1 - e) + 1 - d
        return copy(k, t, cn.at[1, t, k - 14], cn.at[0, t, back - 14], {"gy": y_to[e], "gz": z_to[d]}, back)

    def sx_copy(e, via=None):
        return copy(18 + e, 0, sface.at[0, e], sface.at[1, 1 - e], {"gx": x_to[e if via is None else via]}, 19 - e)

    def sy_copy(e):
        return copy(20 + e, 0, ystage.at[e, SWEEPS], yland.at[1 - e, SWEEPS], {"gy": y_to[e]}, 21 - e)

    def sz_copy(e):
        return copy(22 + e, 0, sedge.at[0, e], sedge.at[1, 1 - e], {"gz": z_to[e]}, 23 - e)

    def face_copies(t):
        return [y_copy(t, e) for e in range(2)] + [z_copy(t, e) for e in range(2)] + [yz_copy(t, e, d) for e in range(2) for d in range(2)]

    def wall_copies(t, e):
        return [x_copy(t, e)] + [xy_copy(t, e, d) for d in range(2)] + [xz_copy(t, e, d) for d in range(2)]

    def messages(t, src):
        for j in range(nm // 2):
            even, odd = src(2 * j), src(2 * j + 1)
            mh[t, j] = jnp.where(off < 2, even, roll(odd, 2))
            ml[t, j] = jnp.where(off < 2, roll(even, -2), odd)

    def send_all(t, between=None):
        for e in range(2):
            r = 0 if e == 0 else 7
            for d in range(2):
                cn[1, t, 2 * e + d] = (ml, mh)[d][t, :, r, :]
        for e in range(2):
            for d in range(2):
                m = 0 if e == 0 else nm - 1
                r = PAD if d == 0 else PAD + rows - 1
                xystage[2 * e + d, t] = xb[t, OFF + m, pl.ds(r, 1), :]
        for e in range(2):
            for d in range(2):
                yz_copy(t, e, d).start()
        for e in range(2):
            @pl.when(has[e])
            def _():
                for d in range(2):
                    xz_copy(t, e, d).start()
                for d in range(2):
                    xy_copy(t, e, d).start()
        for e in range(2):
            z_copy(t, e).start()
        for e in range(2):
            r = PAD if e == 0 else PAD + rows - 2
            for m in range(nm):
                ystage[e, t, m] = xb[t, OFF + m, pl.ds(r, 2), :]
            y_copy(t, e).start()
        if between is not None:
            between()
        for e in range(2):
            @pl.when(has[e])
            def _():
                x_copy(t, e).start()

    def arrive_y(t):
        for e in range(2):
            y_copy(t, e).wait_recv()
        for e in range(2):
            r = PAD - 2 if e == 0 else PAD + rows
            for m in range(nm):
                xb[t, OFF + m, pl.ds(r, 2), :] = yland[e, t, m]

    def arrive_z(t):
        for e in range(2):
            z_copy(t, e).wait_recv()
        for j in range(nm // 2):
            low, high = lz[t, j], hz[t, j]
            l1, l3, lm = roll(low, 1), roll(low, 3), roll(low, -1)
            h1, h3, hm = roll(high, 1), roll(high, -3), roll(high, -1)
            g[1 + 2 * j] = jnp.where(off < 2, jnp.where(off == 0, hm, h1), jnp.where(off == 2, l1, l3))
            g[2 + 2 * j] = jnp.where(off < 2, jnp.where(off == 0, h3, hm), jnp.where(off == 2, lm, l1))

    def arrive_diagonals(t):
        for e in range(2):
            for d in range(2):
                yz_copy(t, e, d).wait_recv()
        for j in range(nm // 2):
            for p in range(2):
                a, b = (jnp.broadcast_to(cn[0, t, k, pl.ds(j, 1), :], (8, cols)) for k in (0, 1))
                cu[2 * j + p] = jnp.where(off == 2, roll(a, 5 - 2 * p), roll(b, 5 - 2 * p))
                a, b = (jnp.broadcast_to(cn[0, t, k, pl.ds(j, 1), :], (8, cols)) for k in (2, 3))
                cd[2 * j + p] = jnp.where(off == 2, roll(a, -3 - 2 * p), roll(b, -3 - 2 * p))
    def arrive_xz(t):
        for e in range(2):
            @pl.when(has[e])
            def _():
                for d in range(2):
                    xz_copy(t, 1 - e, d, e).wait_recv()
                k = -1 if e == 0 else 1
                g[0 if e == 0 else nm + 1] = jnp.where(off == 2, roll(dg[t, 2 * e], k), roll(dg[t, 2 * e + 1], k))

    def arrive_xy(t):
        for e in range(2):
            @pl.when(has[e])
            def _():
                for d in range(2):
                    xy_copy(t, 1 - e, d, e).wait_recv()
                i = OFF - 1 if e == 0 else OFF + nm
                for d in range(2):
                    r = PAD - 1 if d == 0 else PAD + rows
                    xb[t, i, pl.ds(r, 1), :] = xyland[2 * e + d, t]

    def arrive_x(t, late):
        for e in range(2):
            @pl.when(has[e] & (flip if (e == 0) == late else jnp.logical_not(flip)))
            def _():
                x_copy(t, 1 - e, e).wait_recv()

    def edge_red(t):
        for m in range(nm):
            v = g[1 + m]
            up = pltpu.roll(jnp.where(row8 == 7, jnp.where(lane < 4, cu[m], roll(v, 4)), v), 1, 0)
            down = pltpu.roll(jnp.where(row8 == 0, jnp.where(lane >= cols - 4, cd[m], roll(v, -4)), v), 7, 0)
            side = jnp.where(off == 1, roll(v, 1), roll(v, -1))
            beside = jnp.where(odd_edge, g[2 + m], g[m])
            rd[m] = (((sg[m] + v) + (beside + up)) + ((down + side) + fb[t, m])) * jnp.float32(THIRD)

    def relax(read, i, blk0, n, src, c, inner=False):
        rs = PAD + 8 * blk0
        here = three(read(i, rs, 8 * n))
        below_at, above_at = i - 1, i + 1
        if inner:
            below_at, above_at = below_at - (nm - (i - OFF)) // nm, above_at - (OFF + nm) * ((i - OFF) // (nm - 1))
        below, above = three(read(below_at, rs, 8 * n)), three(read(above_at, rs, 8 * n))
        odd = rep(odd8, n)
        beside = jnp.where(odd, above, below) if c == 0 else jnp.where(odd, below, above)
        total = (three(src) + here) + beside
        total = total + three(read(i, rs - 1, 8 * n))
        total = total + three(read(i, rs + 1, 8 * n))
        return beside_lanes(total, here) * jnp.float32(THIRD)

    def beside_lanes(total, here):
        n = here.shape[0]
        total = total + jnp.where(rep(first8, n), 0.0, roll(here, 1))
        return total + jnp.where(rep(last8, n), 0.0, roll(here, -1))

    def red_pair(t, m, inner=False, keep=None):
        i = m + OFF

        def read(i, r, n):
            return xb[t, i, pl.ds(r, n), :]

        for blk0 in range(0, blocks, GROUP):
            y = relax(read, i, blk0, GROUP, sr[i, pl.ds(PAD + 8 * blk0, 8 * GROUP), :], 0, inner)
            if keep is not None:
                y = jnp.where(keep, y, 0.0)
            rb[i, pl.ds(PAD + 8 * blk0, 8 * GROUP), :] = flat(y)

    def relax_block(x, src, lo, n, r, c):
        def read(i, r):
            return x[pl.ds(i, n), pl.ds(r, 8), :]

        odd = rep(odd8, n)
        here, below, above = read(lo, r), read(lo - 1, r), read(lo + 1, r)
        total = (src + here) + (jnp.where(odd, above, below) if c == 0 else jnp.where(odd, below, above))
        total = (total + read(lo, r - 1)) + read(lo, r + 1)
        return beside_lanes(total, here) * jnp.float32(THIRD)

    def red_rows(t):
        for r in (PAD - 8, PAD + rows):
            src = sr[pl.ds(OFF, nm), pl.ds(r, 8), :]
            rb[pl.ds(OFF, nm), pl.ds(r, 8), :] = relax_block(xb.at[t], src, OFF, nm, r, 0)

    def red_borders(t):
        for r, d, k in ((PAD, -1, 0), (PAD + rows - 8, 1, 7)):
            halo = xb[t, pl.ds(OFF, nm), pl.ds(r + d, 8), :]
            own = pl.ds(OFF, nm), pl.ds(r, 8), slice(None)
            rb[own] = rb[own] + jnp.where(jnp.broadcast_to((row8 == k)[None], (nm, 8, cols)), halo, 0.0) * jnp.float32(THIRD)

    def red_side(t, q, h, low):
        near = parity8 == jnp.where(low, 0, 1)
        for blk0 in range(0, blocks, GROUP):
            rs = pl.ds(PAD + 8 * blk0, 8 * GROUP)
            halo = jnp.where(rep(near, GROUP), three(xb[t, h + OFF, rs, :]), 0.0)
            rb[q + OFF, rs, :] = rb[q + OFF, rs, :] + flat(halo * jnp.float32(THIRD))

    def lift(m, blk):
        return jnp.where(brim, roll(dz[m], -(4 * blk + 2)), 0.0)

    def black_borders(t):
        for blk in (0, blocks - 1):
            r = PAD + 8 * blk
            y = relax_block(rb, sb[pl.ds(1, nm - 2), pl.ds(8 * blk, 8), :], OFF + 1, nm - 2, r, 1)
            xb[t + 1, pl.ds(OFF + 1, nm - 2), pl.ds(r, 8), :] = y
            for m in range(1, nm - 1):
                fb[t + 1, m] = jnp.where(quad == blk, roll(y[m - 1], 4 * blk + 2), fb[t + 1, m])

    def lift_borders(t):
        for m in range(1, nm - 1):
            for blk in (0, blocks - 1):
                rs = pl.ds(PAD + 8 * blk, 8)
                xb[t, OFF + m, rs, :] = xb[t, OFF + m, rs, :] + lift(m, blk)
            fb[t, m] = fb[t, m] + dz[m]

    def edge_response(t):
        def middle(v):
            return jnp.where(mid, v, 0.0)

        for m in range(nm):
            v = middle(g[1 + m])
            up = pltpu.roll(jnp.where(row8 == 7, jnp.where(lane < 4, middle(cu[m]), roll(v, 4)), v), 1, 0)
            down = pltpu.roll(jnp.where(row8 == 0, jnp.where(lane >= cols - 4, middle(cd[m]), roll(v, -4)), v), 7, 0)
            beside = jnp.where(odd_edge, middle(g[2 + m]), middle(g[m]))
            near = (rd[m] + ((v + beside) + (up + down)) * jnp.float32(THIRD)) * jnp.float32(THIRD)
            far = jnp.where(off == 0, roll(v, -1), roll(v, 1)) * jnp.float32(THIRD * THIRD)
            dz[m] = jnp.where(mid, near, far)

    def lift_pair(t, m, first, last):
        v = dz[m]
        for blk0 in range(0, blocks, GROUP):
            lo, hi = max(blk0, first), min(blk0 + GROUP, last)
            rs = pl.ds(PAD + 8 * lo, 8 * (hi - lo))
            y = jnp.stack([roll(v, -(4 * blk + 2)) for blk in range(lo, hi)], axis=0)
            xb[t, OFF + m, rs, :] = xb[t, OFF + m, rs, :] + flat(jnp.where(rep(brim, hi - lo), y, 0.0))

    def lift_rest(t):
        def body(m, carry):
            lift_pair(t, m, 1, blocks - 1)
            return carry

        lax.fori_loop(1, nm - 1, body, 0)

    def black_pair(m, emit):
        i = m + OFF

        def read(i, r, n):
            return rb[i, pl.ds(r, n), :]

        for blk0 in range(0, blocks, GROUP):
            rs = pl.ds(8 * blk0, 8 * GROUP)
            emit(blk0, relax(read, i, blk0, GROUP, sb[m, rs, :], 1))

    zero = jnp.zeros((rows + 16, cols), jnp.float32)
    for e in range(2):
        @pl.when(jnp.logical_not(has[e]))
        def _():
            i = OFF - 1 if e == 0 else OFF + nm
            for t in range(SWEEPS):
                xb[t, i, pl.ds(PAD - 8, rows + 16), :] = zero
            rb[i, pl.ds(PAD - 8, rows + 16), :] = zero
            g[0 if e == 0 else nm + 1] = zeros8

    def pack_field(a, carry):
        for m in (a, nm - 1 - a):
            load(f_hbm, fv, fsem, m).wait()
            parts = [zeros8] * 4
            for blk0 in range(0, blocks, GROUP):
                rs = pl.ds(8 * blk0, 8 * GROUP)
                y = jnp.where(rep(odd8, GROUP), three(fv[2 * m, rs, :]), three(fv[2 * m + 1, rs, :]))
                xb[0, OFF + m, pl.ds(PAD + 8 * blk0, 8 * GROUP), :] = flat(y)
                parts = pick(parts, y, blk0)
            fb[0, m] = merge(parts)
        return carry

    def pack_source(a, carry):
        for m in (a, nm - 1 - a):
            load(s_hbm, sv, ssem, m).wait()
            parts = [zeros8] * 4
            for blk0 in range(0, blocks, GROUP):
                rs = pl.ds(8 * blk0, 8 * GROUP)
                low, high = three(sv[2 * m, rs, :]), three(sv[2 * m + 1, rs, :])
                y = jnp.where(rep(odd8, GROUP), high, low)
                sr[OFF + m, pl.ds(PAD + 8 * blk0, 8 * GROUP), :] = flat(y)
                sb[m, rs, :] = flat(jnp.where(rep(odd8, GROUP), low, high))
                parts = pick(parts, y, blk0)
            sg[m] = merge(parts)
        return carry

    lax.fori_loop(0, nm // 2, pack_field, 0)
    messages(0, lambda m: fb[0, m])
    lax.fori_loop(0, nm // 2, pack_source, 0)
    half = rows // 2
    odd_lane = lax.rem(lax.broadcasted_iota(jnp.int32, (half, cols), 1), 2) == 1
    for e in range(2):
        for j in range(nm // 4):
            parts = [roll(sg[4 * j + k], k - 2 + e) for k in range(4)]
            sedge[0, e, j] = jnp.where(off < 2, jnp.where(off == 0, parts[0], parts[1]), jnp.where(off == 2, parts[2], parts[3]))
        r = PAD if e == 0 else PAD + rows - 1
        for m in range(nm):
            ystage[e, SWEEPS, m, pl.ds(0, 1), :] = sr[OFF + m, pl.ds(r, 1), :]

    pl.semaphore_wait(barrier, 8 + 5 * (has_lo.astype(jnp.int32) + has_hi.astype(jnp.int32)))
    def send_source():
        for e in range(2):
            sz_copy(e).start()
            sy_copy(e).start()

    send_all(0, send_source)
    for e in range(2):
        @pl.when(has[e])
        def _():
            i = OFF if e == 0 else OFF + nm - 1
            even = sr[i, pl.ds(PAD, half, stride=2), :]
            odd = sr[i, pl.ds(PAD + 1, half, stride=2), :]
            sface[0, e] = jnp.where(odd_lane, odd, even) if e == 0 else jnp.where(odd_lane, even, odd)
            sx_copy(e).start()

    for t in range(SWEEPS):
        xb[t, 0, pl.ds(PAD, rows), :] = zero[:rows]
        for r in (PAD - 8, PAD + rows):
            xb[t, pl.ds(OFF, nm), pl.ds(r, 8), :] = jnp.zeros((nm, 8, cols), jnp.float32)

    def take_source():
        for e in range(2):
            sz_copy(e).wait_recv()
            sy_copy(e).wait_recv()
        for e in range(2):
            r = PAD - 1 if e == 0 else PAD + rows
            for m in range(nm):
                sr[OFF + m, pl.ds(r, 1), :] = yland[e, SWEEPS, m, pl.ds(0, 1), :]
        for j in range(nm // 4):
            low, high = sedge[1, 0, j], sedge[1, 1, j]
            for k in range(4):
                sg[4 * j + k] = jnp.where(off == 1, roll(high, 1 - k), roll(low, 2 - k))

    def take_source_x(late):
        for e in range(2):
            @pl.when(has[e] & (flip if (e == 0) == late else jnp.logical_not(flip)))
            def _():
                sx_copy(1 - e, e).wait_recv()
                i = OFF - 1 if e == 0 else OFF + nm
                got = sface[1, e]
                sr[i, pl.ds(PAD, half, stride=2), :] = got
                sr[i, pl.ds(PAD + 1, half, stride=2), :] = got

    def at(p):
        return jnp.where(flip, nm - 1 - p, p)

    def on_first(t, do):
        pl.when(t == 0)(do)

    def full(t, carry):
        def red_inner(m, carry):
            red_pair(t, m, inner=True)
            return carry

        def black_inner(m, carry):
            parts = [zeros8] * 4

            def emit(blk0, y):
                xb[t + 1, OFF + m, pl.ds(PAD + 8 * blk0, 8 * GROUP), :] = flat(y)
                pick(parts, y, blk0)

            black_pair(m, emit)
            fb[t + 1, m] = merge(parts)
            return carry

        lax.fori_loop(0, nm, red_inner, 0)
        lax.fori_loop(1, nm - 1, black_inner, 0)

        def side_red(late):
            h = int(late)
            q = at(nm - 1 if late else 0)
            out = at(nm if late else -1)
            red_side(t, q, out, flip if late else jnp.logical_not(flip))
            red_pair(t, out, keep=jnp.where(flip, has[1 - h], has[h]))

        def side_black(late):
            q = at(nm - 1 if late else 0)
            parts = [zeros8] * 4

            def emit(blk0, y):
                if late:
                    y = y + jnp.stack([lift(q, blk0 + k) for k in range(GROUP)], axis=0)
                xb[t + 1, OFF + q, pl.ds(PAD + 8 * blk0, 8 * GROUP), :] = flat(y)
                pick(parts, y, blk0)

            black_pair(q, emit)
            fb[t + 1, q] = merge(parts)

        arrive_y(t)
        red_borders(t)
        arrive_x(t, False)
        on_first(t, lambda: take_source_x(False))
        arrive_xy(t)
        side_red(False)
        on_first(t, take_source)
        red_rows(t)
        black_borders(t)
        side_black(False)
        arrive_xz(t)
        arrive_z(t)
        arrive_diagonals(t)
        edge_red(t)
        edge_response(t)
        lift_borders(t + 1)
        early = at(0)
        lift_pair(t + 1, early, 0, blocks)
        fb[t + 1, early] = fb[t + 1, early] + dz[early]
        arrive_x(t, True)
        on_first(t, lambda: take_source_x(True))
        side_red(True)
        side_black(True)

        @pl.when(t < SWEEPS - 1)
        def _():
            messages(t + 1, lambda m: fb[t + 1, m])
            send_all(t + 1)
            lift_rest(t + 1)

        return carry

    lax.fori_loop(0, SWEEPS, full, 0)
    for m in (0, nm - 1):
        dz[m] = zeros8

    def write(m, carry):
        lr = jnp.where(mid, g[1 + m], 0.0) * jnp.float32(THIRD)
        lb = dz[m]
        low, high = jnp.where(odd_edge, lr, lb), jnp.where(odd_edge, lb, lr)
        low_red, high_red = jnp.where(odd_edge, lr, 0.0), jnp.where(odd_edge, 0.0, lr)
        for blk0 in range(0, blocks, GROUP):
            rs, ps = pl.ds(8 * blk0, 8 * GROUP), pl.ds(PAD + 8 * blk0, 8 * GROUP)
            red, black = three(rb[OFF + m, ps, :]), three(xb[SWEEPS, OFF + m, ps, :])
            odd, edge = rep(odd8, GROUP), rep(brim, GROUP)

            def add(inside, outer):
                return jnp.stack([roll(outer if blk in (0, blocks - 1) else inside, -(4 * blk + 2)) for blk in range(blk0, blk0 + GROUP)], axis=0)

            ov[2 * m, rs, :] = flat(jnp.where(odd, black, red) + jnp.where(edge, add(low, low_red), 0.0))
            ov[2 * m + 1, rs, :] = flat(jnp.where(odd, red, black) + jnp.where(edge, add(high, high_red), 0.0))
        return carry

    lax.fori_loop(0, nm, write, 0, unroll=2)

    def drain(t, carry):
        for c in face_copies(t):
            c.wait_send()
        for e in range(2):
            @pl.when(has[e])
            def _():
                for c in wall_copies(t, e):
                    c.wait_send()
        return carry

    lax.fori_loop(0, SWEEPS, drain, 0)
    for e in range(2):
        sz_copy(e).wait_send()
        sy_copy(e).wait_send()

        @pl.when(has[e])
        def _():
            sx_copy(e).wait_send()


def solution(mesh):
    sizes = tuple(mesh.shape[a] for a in ("gx", "gy", "gz"))

    def on_device(field, source):
        planes, rows, cols = field.shape
        nm = planes // 2
        assert planes % 4 == 0 and rows == 256 and cols == 128 and rows % (8 * GROUP) == 0
        f32 = jnp.float32
        wide = (nm + 2 * OFF, rows + 2 * PAD, cols)
        return pl.pallas_call(
            functools.partial(kernel, sizes),
            out_shape=jax.ShapeDtypeStruct(field.shape, f32),
            in_specs=[pl.BlockSpec(memory_space=pltpu.HBM)] * 2,
            out_specs=pl.BlockSpec(memory_space=pltpu.VMEM),
            scratch_shapes=[
                pltpu.VMEM(field.shape, f32),
                pltpu.VMEM(field.shape, f32),
                pltpu.VMEM((SWEEPS + 1, *wide), f32),
                pltpu.VMEM(wide, f32),
                pltpu.VMEM(wide, f32),
                pltpu.VMEM((nm, rows, cols), f32),
                pltpu.VMEM((SWEEPS + 1, nm, 8, cols), f32),
                *[pltpu.VMEM((SWEEPS, nm // 2, 8, cols), f32)] * 4,
                pltpu.VMEM((SWEEPS, 4, 8, cols), f32),
                pltpu.VMEM((2, SWEEPS, 4, nm // 2, cols), f32),
                pltpu.VMEM((nm + 2, 8, cols), f32),
                *[pltpu.VMEM((nm, 8, cols), f32)] * 5,
                *[pltpu.VMEM((2, SWEEPS + 1, nm, 2, cols), f32)] * 2,
                *[pltpu.VMEM((4, SWEEPS, 1, cols), f32)] * 2,
                pltpu.VMEM((2, 2, rows // 2, cols), f32),
                pltpu.VMEM((2, 2, nm // 4, 8, cols), f32),
                pltpu.SemaphoreType.DMA((24, SWEEPS)),
                pltpu.SemaphoreType.DMA((24, SWEEPS)),
                pltpu.SemaphoreType.DMA((nm,)),
                pltpu.SemaphoreType.DMA((nm,)),
            ],
            compiler_params=pltpu.CompilerParams(
                collective_id=0, has_side_effects=True, vmem_limit_bytes=60 * 1024 * 1024
            ),
        )(field, source)

    spec = P("gx", "gy", "gz")
    return jax.shard_map(on_device, mesh=mesh, in_specs=(spec, spec), out_specs=spec, check_vma=False)
```

```python
import functools

import jax
import jax.numpy as jnp
from jax import lax
from jax.experimental import pallas as pl
from jax.experimental.pallas import tpu as pltpu
from jax.sharding import PartitionSpec as P

SWEEPS = 3
MESH = pl.DeviceIdType.MESH
PAD = 16
OFF = 2
GROUP = 8
THIRD = 1.0 / 6.0


def kernel(sizes, f_hbm, s_hbm, ov, fv, sv, xb, rb, sr, sb, fb, mh, ml, lz, hz, dg, cn, g, rd, sg, cu, cd, dz, ystage, yland, xystage, xyland, sface, sedge,
           send, recv, fsem, ssem):
    ngx, ngy, ngz = sizes
    planes, rows, cols = f_hbm.shape
    nm = planes // 2
    blocks = rows // 8
    gx, gy, gz = (lax.axis_index(a) for a in ("gx", "gy", "gz"))
    has_lo, has_hi = gx > 0, gx < ngx - 1
    y_lo, y_hi = lax.rem(gy + ngy - 1, ngy), lax.rem(gy + 1, ngy)
    z_lo, z_hi = lax.rem(gz + ngz - 1, ngz), lax.rem(gz + 1, ngz)
    x_to = (gx - 1, gx + 1)
    y_to = (y_lo, y_hi)
    z_to = (z_lo, z_hi)
    has = (has_lo, has_hi)
    flip = gx >= ngx // 2
    order = [m for a in range(nm // 2) for m in (a, nm - 1 - a)]

    def load(ref, to, sem, m):
        return pltpu.make_async_copy(ref.at[pl.ds(2 * m, 2)], to.at[pl.ds(2 * m, 2)], sem.at[m])

    barrier = pltpu.get_barrier_semaphore()

    def greet(device):
        pl.semaphore_signal(barrier, inc=1, device_id=device, device_id_type=MESH)

    for e in range(2):
        greet({"gy": y_to[e]})
        greet({"gz": z_to[e]})
        for d in range(2):
            greet({"gy": y_to[e], "gz": z_to[d]})

        @pl.when(has[e])
        def _():
            greet({"gx": x_to[e]})
            for d in range(2):
                greet({"gx": x_to[e], "gy": y_to[d]})
                greet({"gx": x_to[e], "gz": z_to[d]})

    for m in order:
        load(f_hbm, fv, fsem, m).start()
    for m in order:
        load(s_hbm, sv, ssem, m).start()

    row8 = lax.broadcasted_iota(jnp.int32, (8, cols), 0)
    lane = lax.broadcasted_iota(jnp.int32, (8, cols), 1)
    off = lax.rem(lane, 4)
    quad = lax.div(lane, 4)
    parity8 = lax.rem(row8 + lane, 2)
    odd8 = parity8 == 1
    odd_edge = lax.rem(row8 + off, 2) == 0
    mid = lax.rem(off + 1, 4) >= 2
    brim = lax.rem(lane + 2, cols) < 4
    first8, last8 = lane == 0, lane == cols - 1

    def rep(mask, n):
        return jnp.broadcast_to(mask[None], (n, 8, cols))

    def roll(v, k):
        k = k % cols
        return v if k == 0 else pltpu.roll(v, k, v.ndim - 1)

    def three(v):
        return v.reshape(v.shape[0] // 8, 8, cols)

    def flat(v):
        return v.reshape(v.shape[0] * 8, cols)

    def pick(parts, y, blk0):
        for k in range(y.shape[0]):
            blk = blk0 + k
            j = blk % len(parts)
            parts[j] = jnp.where(quad == blk, roll(y[k], 4 * blk + 2), parts[j])
        return parts

    def merge(parts):
        while len(parts) > 1:
            parts = [p + q for p, q in zip(parts[::2], parts[1::2])]
        return parts[0]

    zeros8 = jnp.zeros((8, cols), jnp.float32)

    def copy(k, t, src, dst, to, back):
        return pltpu.make_async_remote_copy(
            src_ref=src, dst_ref=dst, send_sem=send.at[k, t], recv_sem=recv.at[back, t], device_id=to, device_id_type=MESH
        )

    def x_copy(t, e, via=None):
        m, to = (0, nm) if e == 0 else (nm - 1, -1)
        return copy(e, t, xb.at[t, OFF + m, pl.ds(PAD, rows)], xb.at[t, OFF + to, pl.ds(PAD, rows)], {"gx": x_to[e if via is None else via]}, 1 - e)

    def y_copy(t, e):
        return copy(2 + e, t, ystage.at[e, t], yland.at[1 - e, t], {"gy": y_to[e]}, 3 - e)

    def z_copy(t, e):
        src, dst = (ml, hz) if e == 0 else (mh, lz)
        return copy(4 + e, t, src.at[t], dst.at[t], {"gz": z_to[e]}, 5 - e)

    def xy_copy(t, e, d, via=None):
        k, back = 6 + 2 * e + d, 6 + 2 * (1 - e) + 1 - d
        return copy(k, t, xystage.at[k - 6, t], xyland.at[back - 6, t], {"gx": x_to[e if via is None else via], "gy": y_to[d]}, back)

    def xz_copy(t, e, d, via=None):
        k, back = 10 + 2 * e + d, 10 + 2 * (1 - e) + 1 - d
        j = 0 if e == 0 else nm // 2 - 1
        return copy(k, t, (ml, mh)[d].at[t, j], dg.at[t, back - 10], {"gx": x_to[e if via is None else via], "gz": z_to[d]}, back)

    def yz_copy(t, e, d):
        k, back = 14 + 2 * e + d, 14 + 2 * (1 - e) + 1 - d
        return copy(k, t, cn.at[1, t, k - 14], cn.at[0, t, back - 14], {"gy": y_to[e], "gz": z_to[d]}, back)

    def sx_copy(e, via=None):
        return copy(18 + e, 0, sface.at[0, e], sface.at[1, 1 - e], {"gx": x_to[e if via is None else via]}, 19 - e)

    def sy_copy(e):
        return copy(20 + e, 0, ystage.at[e, SWEEPS], yland.at[1 - e, SWEEPS], {"gy": y_to[e]}, 21 - e)

    def sz_copy(e):
        return copy(22 + e, 0, sedge.at[0, e], sedge.at[1, 1 - e], {"gz": z_to[e]}, 23 - e)

    def face_copies(t):
        return [y_copy(t, e) for e in range(2)] + [z_copy(t, e) for e in range(2)] + [yz_copy(t, e, d) for e in range(2) for d in range(2)]

    def wall_copies(t, e):
        return [x_copy(t, e)] + [xy_copy(t, e, d) for d in range(2)] + [xz_copy(t, e, d) for d in range(2)]

    def messages(t, src):
        for j in range(nm // 2):
            even, odd = src(2 * j), src(2 * j + 1)
            mh[t, j] = jnp.where(off < 2, even, roll(odd, 2))
            ml[t, j] = jnp.where(off < 2, roll(even, -2), odd)

    def send_all(t, between=None):
        for e in range(2):
            r = 0 if e == 0 else 7
            for d in range(2):
                cn[1, t, 2 * e + d] = (ml, mh)[d][t, :, r, :]
        for e in range(2):
            for d in range(2):
                m = 0 if e == 0 else nm - 1
                r = PAD if d == 0 else PAD + rows - 1
                xystage[2 * e + d, t] = xb[t, OFF + m, pl.ds(r, 1), :]
        for e in range(2):
            for d in range(2):
                yz_copy(t, e, d).start()
        for e in range(2):
            @pl.when(has[e])
            def _():
                for d in range(2):
                    xz_copy(t, e, d).start()
                for d in range(2):
                    xy_copy(t, e, d).start()
        for e in range(2):
            z_copy(t, e).start()
        for e in range(2):
            r = PAD if e == 0 else PAD + rows - 2
            for m in range(nm):
                ystage[e, t, m] = xb[t, OFF + m, pl.ds(r, 2), :]
            y_copy(t, e).start()
        if between is not None:
            between()
        for e in range(2):
            @pl.when(has[e])
            def _():
                x_copy(t, e).start()

    def arrive_y(t):
        for e in range(2):
            y_copy(t, e).wait_recv()
        for e in range(2):
            r = PAD - 2 if e == 0 else PAD + rows
            for m in range(nm):
                xb[t, OFF + m, pl.ds(r, 2), :] = yland[e, t, m]

    def arrive_z(t):
        for e in range(2):
            z_copy(t, e).wait_recv()
        for j in range(nm // 2):
            low, high = lz[t, j], hz[t, j]
            l1, l3, lm = roll(low, 1), roll(low, 3), roll(low, -1)
            h1, h3, hm = roll(high, 1), roll(high, -3), roll(high, -1)
            g[1 + 2 * j] = jnp.where(off < 2, jnp.where(off == 0, hm, h1), jnp.where(off == 2, l1, l3))
            g[2 + 2 * j] = jnp.where(off < 2, jnp.where(off == 0, h3, hm), jnp.where(off == 2, lm, l1))

    def arrive_diagonals(t):
        for e in range(2):
            for d in range(2):
                yz_copy(t, e, d).wait_recv()
        for j in range(nm // 2):
            for p in range(2):
                a, b = (jnp.broadcast_to(cn[0, t, k, pl.ds(j, 1), :], (8, cols)) for k in (0, 1))
                cu[2 * j + p] = jnp.where(off == 2, roll(a, 5 - 2 * p), roll(b, 5 - 2 * p))
                a, b = (jnp.broadcast_to(cn[0, t, k, pl.ds(j, 1), :], (8, cols)) for k in (2, 3))
                cd[2 * j + p] = jnp.where(off == 2, roll(a, -3 - 2 * p), roll(b, -3 - 2 * p))
    def arrive_xz(t):
        for e in range(2):
            @pl.when(has[e])
            def _():
                for d in range(2):
                    xz_copy(t, 1 - e, d, e).wait_recv()
                k = -1 if e == 0 else 1
                g[0 if e == 0 else nm + 1] = jnp.where(off == 2, roll(dg[t, 2 * e], k), roll(dg[t, 2 * e + 1], k))

    def arrive_xy(t):
        for e in range(2):
            @pl.when(has[e])
            def _():
                for d in range(2):
                    xy_copy(t, 1 - e, d, e).wait_recv()
                i = OFF - 1 if e == 0 else OFF + nm
                for d in range(2):
                    r = PAD - 1 if d == 0 else PAD + rows
                    xb[t, i, pl.ds(r, 1), :] = xyland[2 * e + d, t]

    def arrive_x(t, late):
        for e in range(2):
            @pl.when(has[e] & (flip if (e == 0) == late else jnp.logical_not(flip)))
            def _():
                x_copy(t, 1 - e, e).wait_recv()

    def edge_red(t):
        for m in range(nm):
            v = g[1 + m]
            up = pltpu.roll(jnp.where(row8 == 7, jnp.where(lane < 4, cu[m], roll(v, 4)), v), 1, 0)
            down = pltpu.roll(jnp.where(row8 == 0, jnp.where(lane >= cols - 4, cd[m], roll(v, -4)), v), 7, 0)
            side = jnp.where(off == 1, roll(v, 1), roll(v, -1))
            beside = jnp.where(odd_edge, g[2 + m], g[m])
            rd[m] = (((sg[m] + v) + (beside + up)) + ((down + side) + fb[t, m])) * jnp.float32(THIRD)

    def relax(read, i, blk0, n, src, c, inner=False):
        rs = PAD + 8 * blk0
        here = three(read(i, rs, 8 * n))
        below_at, above_at = i - 1, i + 1
        if inner:
            below_at, above_at = below_at - (nm - (i - OFF)) // nm, above_at - (OFF + nm) * ((i - OFF) // (nm - 1))
        below, above = three(read(below_at, rs, 8 * n)), three(read(above_at, rs, 8 * n))
        odd = rep(odd8, n)
        beside = jnp.where(odd, above, below) if c == 0 else jnp.where(odd, below, above)
        total = (three(src) + here) + beside
        total = total + three(read(i, rs - 1, 8 * n))
        total = total + three(read(i, rs + 1, 8 * n))
        return beside_lanes(total, here) * jnp.float32(THIRD)

    def beside_lanes(total, here):
        n = here.shape[0]
        total = total + jnp.where(rep(first8, n), 0.0, roll(here, 1))
        return total + jnp.where(rep(last8, n), 0.0, roll(here, -1))

    def red_pair(t, m, inner=False, keep=None):
        i = m + OFF

        def read(i, r, n):
            return xb[t, i, pl.ds(r, n), :]

        for blk0 in range(0, blocks, GROUP):
            y = relax(read, i, blk0, GROUP, sr[i, pl.ds(PAD + 8 * blk0, 8 * GROUP), :], 0, inner)
            if keep is not None:
                y = jnp.where(keep, y, 0.0)
            rb[i, pl.ds(PAD + 8 * blk0, 8 * GROUP), :] = flat(y)

    def relax_block(x, src, lo, n, r, c):
        def read(i, r):
            return x[pl.ds(i, n), pl.ds(r, 8), :]

        odd = rep(odd8, n)
        here, below, above = read(lo, r), read(lo - 1, r), read(lo + 1, r)
        total = (src + here) + (jnp.where(odd, above, below) if c == 0 else jnp.where(odd, below, above))
        total = (total + read(lo, r - 1)) + read(lo, r + 1)
        return beside_lanes(total, here) * jnp.float32(THIRD)

    def red_rows(t):
        for r in (PAD - 8, PAD + rows):
            src = sr[pl.ds(OFF, nm), pl.ds(r, 8), :]
            rb[pl.ds(OFF, nm), pl.ds(r, 8), :] = relax_block(xb.at[t], src, OFF, nm, r, 0)

    def red_borders(t, i, n):
        for r, d, k in ((PAD, -1, 0), (PAD + rows - 8, 1, 7)):
            halo = xb[t, pl.ds(i, n), pl.ds(r + d, 8), :]
            own = pl.ds(i, n), pl.ds(r, 8), slice(None)
            rb[own] = rb[own] + jnp.where(jnp.broadcast_to((row8 == k)[None], (n, 8, cols)), halo, 0.0) * jnp.float32(THIRD)

    def red_side(t, q, h, low):
        near = parity8 == jnp.where(low, 0, 1)
        for blk0 in range(0, blocks, GROUP):
            rs = pl.ds(PAD + 8 * blk0, 8 * GROUP)
            halo = jnp.where(rep(near, GROUP), three(xb[t, h + OFF, rs, :]), 0.0)
            rb[q + OFF, rs, :] = rb[q + OFF, rs, :] + flat(halo * jnp.float32(THIRD))

    def lift(m, blk):
        return jnp.where(brim, roll(dz[m], -(4 * blk + 2)), 0.0)

    def black_borders(t):
        for blk in (0, blocks - 1):
            r = PAD + 8 * blk
            y = relax_block(rb, sb[:, pl.ds(8 * blk, 8), :], OFF, nm, r, 1)
            xb[t + 1, pl.ds(OFF, nm), pl.ds(r, 8), :] = y
            for m in range(nm):
                fb[t + 1, m] = jnp.where(quad == blk, roll(y[m], 4 * blk + 2), fb[t + 1, m])

    def lift_borders(t):
        for m in range(1, nm - 1):
            for blk in (0, blocks - 1):
                rs = pl.ds(PAD + 8 * blk, 8)
                xb[t, OFF + m, rs, :] = xb[t, OFF + m, rs, :] + lift(m, blk)
            fb[t, m] = fb[t, m] + dz[m]

    def edge_response(t):
        def middle(v):
            return jnp.where(mid, v, 0.0)

        for m in range(nm):
            v = middle(g[1 + m])
            up = pltpu.roll(jnp.where(row8 == 7, jnp.where(lane < 4, middle(cu[m]), roll(v, 4)), v), 1, 0)
            down = pltpu.roll(jnp.where(row8 == 0, jnp.where(lane >= cols - 4, middle(cd[m]), roll(v, -4)), v), 7, 0)
            beside = jnp.where(odd_edge, middle(g[2 + m]), middle(g[m]))
            near = (rd[m] + ((v + beside) + (up + down)) * jnp.float32(THIRD)) * jnp.float32(THIRD)
            far = jnp.where(off == 0, roll(v, -1), roll(v, 1)) * jnp.float32(THIRD * THIRD)
            dz[m] = jnp.where(mid, near, far)

    def lift_pair(t, m, first, last):
        v = dz[m]
        for blk0 in range(0, blocks, GROUP):
            lo, hi = max(blk0, first), min(blk0 + GROUP, last)
            rs = pl.ds(PAD + 8 * lo, 8 * (hi - lo))
            y = jnp.stack([roll(v, -(4 * blk + 2)) for blk in range(lo, hi)], axis=0)
            xb[t, OFF + m, rs, :] = xb[t, OFF + m, rs, :] + flat(jnp.where(rep(brim, hi - lo), y, 0.0))

    def lift_rest(t):
        def body(m, carry):
            lift_pair(t, m, 1, blocks - 1)
            return carry

        lax.fori_loop(1, nm - 1, body, 0)

    def black_pair(m, emit):
        i = m + OFF

        def read(i, r, n):
            return rb[i, pl.ds(r, n), :]

        for blk0 in range(0, blocks, GROUP):
            rs = pl.ds(8 * blk0, 8 * GROUP)
            emit(blk0, relax(read, i, blk0, GROUP, sb[m, rs, :], 1))

    zero = jnp.zeros((rows + 16, cols), jnp.float32)
    for e in range(2):
        @pl.when(jnp.logical_not(has[e]))
        def _():
            i = OFF - 1 if e == 0 else OFF + nm
            for t in range(SWEEPS):
                xb[t, i, pl.ds(PAD - 8, rows + 16), :] = zero
            rb[i, pl.ds(PAD - 8, rows + 16), :] = zero
            g[0 if e == 0 else nm + 1] = zeros8

    def pack_field(a, carry):
        for m in (a, nm - 1 - a):
            load(f_hbm, fv, fsem, m).wait()
            parts = [zeros8] * 4
            for blk0 in range(0, blocks, GROUP):
                rs = pl.ds(8 * blk0, 8 * GROUP)
                y = jnp.where(rep(odd8, GROUP), three(fv[2 * m, rs, :]), three(fv[2 * m + 1, rs, :]))
                xb[0, OFF + m, pl.ds(PAD + 8 * blk0, 8 * GROUP), :] = flat(y)
                parts = pick(parts, y, blk0)
            fb[0, m] = merge(parts)
        return carry

    def pack_source(a, carry):
        for m in (a, nm - 1 - a):
            load(s_hbm, sv, ssem, m).wait()
            parts = [zeros8] * 4
            for blk0 in range(0, blocks, GROUP):
                rs = pl.ds(8 * blk0, 8 * GROUP)
                low, high = three(sv[2 * m, rs, :]), three(sv[2 * m + 1, rs, :])
                y = jnp.where(rep(odd8, GROUP), high, low)
                sr[OFF + m, pl.ds(PAD + 8 * blk0, 8 * GROUP), :] = flat(y)
                sb[m, rs, :] = flat(jnp.where(rep(odd8, GROUP), low, high))
                parts = pick(parts, y, blk0)
            sg[m] = merge(parts)
        return carry

    lax.fori_loop(0, nm // 2, pack_field, 0)
    messages(0, lambda m: fb[0, m])
    lax.fori_loop(0, nm // 2, pack_source, 0)
    half = rows // 2
    odd_lane = lax.rem(lax.broadcasted_iota(jnp.int32, (half, cols), 1), 2) == 1
    for e in range(2):
        for j in range(nm // 4):
            parts = [roll(sg[4 * j + k], k - 2 + e) for k in range(4)]
            sedge[0, e, j] = jnp.where(off < 2, jnp.where(off == 0, parts[0], parts[1]), jnp.where(off == 2, parts[2], parts[3]))
        r = PAD if e == 0 else PAD + rows - 1
        for m in range(nm):
            ystage[e, SWEEPS, m, pl.ds(0, 1), :] = sr[OFF + m, pl.ds(r, 1), :]

    pl.semaphore_wait(barrier, 8 + 5 * (has_lo.astype(jnp.int32) + has_hi.astype(jnp.int32)))
    def send_source():
        for e in range(2):
            sz_copy(e).start()
            sy_copy(e).start()

    send_all(0, send_source)
    for e in range(2):
        @pl.when(has[e])
        def _():
            i = OFF if e == 0 else OFF + nm - 1
            even = sr[i, pl.ds(PAD, half, stride=2), :]
            odd = sr[i, pl.ds(PAD + 1, half, stride=2), :]
            sface[0, e] = jnp.where(odd_lane, odd, even) if e == 0 else jnp.where(odd_lane, even, odd)
            sx_copy(e).start()

    for t in range(SWEEPS):
        xb[t, 0, pl.ds(PAD, rows), :] = zero[:rows]
        for r in (PAD - 8, PAD + rows):
            xb[t, pl.ds(OFF - 1, nm + 2), pl.ds(r, 8), :] = jnp.zeros((nm + 2, 8, cols), jnp.float32)

    def take_source():
        for e in range(2):
            sz_copy(e).wait_recv()
            sy_copy(e).wait_recv()
        for e in range(2):
            r = PAD - 1 if e == 0 else PAD + rows
            for m in range(nm):
                sr[OFF + m, pl.ds(r, 1), :] = yland[e, SWEEPS, m, pl.ds(0, 1), :]
        for j in range(nm // 4):
            low, high = sedge[1, 0, j], sedge[1, 1, j]
            for k in range(4):
                sg[4 * j + k] = jnp.where(off == 1, roll(high, 1 - k), roll(low, 2 - k))

    def take_source_x(late):
        for e in range(2):
            @pl.when(has[e] & (flip if (e == 0) == late else jnp.logical_not(flip)))
            def _():
                sx_copy(1 - e, e).wait_recv()
                i = OFF - 1 if e == 0 else OFF + nm
                got = sface[1, e]
                sr[i, pl.ds(PAD, half, stride=2), :] = got
                sr[i, pl.ds(PAD + 1, half, stride=2), :] = got

    def at(p):
        return jnp.where(flip, nm - 1 - p, p)

    def on_first(t, do):
        pl.when(t == 0)(do)

    def full(t, carry):
        def red_inner(m, carry):
            red_pair(t, m, inner=True)
            return carry

        def black_inner(m, carry):
            parts = [zeros8] * 4

            def emit(blk0, y):
                xb[t + 1, OFF + m, pl.ds(PAD + 8 * blk0, 8 * GROUP), :] = flat(y)
                pick(parts, y, blk0)

            black_pair(m, emit)
            fb[t + 1, m] = merge(parts)
            return carry

        lax.fori_loop(0, nm, red_inner, 0)
        lax.fori_loop(1, nm - 1, black_inner, 0)

        def side_red(late):
            h = int(late)
            q = at(nm - 1 if late else 0)
            out = at(nm if late else -1)
            red_side(t, q, out, flip if late else jnp.logical_not(flip))
            red_pair(t, out, keep=jnp.where(flip, has[1 - h], has[h]))

        def side_black(late):
            q = at(nm - 1 if late else 0)
            parts = [zeros8] * 4

            def emit(blk0, y):
                if late:
                    y = y + jnp.stack([lift(q, blk0 + k) for k in range(GROUP)], axis=0)
                xb[t + 1, OFF + q, pl.ds(PAD + 8 * blk0, 8 * GROUP), :] = flat(y)
                pick(parts, y, blk0)

            black_pair(q, emit)
            fb[t + 1, q] = merge(parts)

        arrive_x(t, False)
        on_first(t, lambda: take_source_x(False))
        side_red(False)
        side_black(False)
        arrive_y(t)
        red_borders(t, OFF, nm)
        arrive_xy(t)
        red_borders(t, at(-1) + OFF, 1)
        on_first(t, take_source)
        red_rows(t)
        black_borders(t)
        arrive_xz(t)
        arrive_z(t)
        arrive_diagonals(t)
        edge_red(t)
        edge_response(t)
        lift_borders(t + 1)
        early = at(0)
        lift_pair(t + 1, early, 0, blocks)
        fb[t + 1, early] = fb[t + 1, early] + dz[early]
        arrive_x(t, True)
        on_first(t, lambda: take_source_x(True))
        side_red(True)
        side_black(True)

        @pl.when(t < SWEEPS - 1)
        def _():
            messages(t + 1, lambda m: fb[t + 1, m])
            send_all(t + 1)
            lift_rest(t + 1)

        return carry

    lax.fori_loop(0, SWEEPS, full, 0)
    for m in (0, nm - 1):
        dz[m] = zeros8

    def write(m, carry):
        lr = jnp.where(mid, g[1 + m], 0.0) * jnp.float32(THIRD)
        lb = dz[m]
        low, high = jnp.where(odd_edge, lr, lb), jnp.where(odd_edge, lb, lr)
        low_red, high_red = jnp.where(odd_edge, lr, 0.0), jnp.where(odd_edge, 0.0, lr)
        for blk0 in range(0, blocks, GROUP):
            rs, ps = pl.ds(8 * blk0, 8 * GROUP), pl.ds(PAD + 8 * blk0, 8 * GROUP)
            red, black = three(rb[OFF + m, ps, :]), three(xb[SWEEPS, OFF + m, ps, :])
            odd, edge = rep(odd8, GROUP), rep(brim, GROUP)

            def add(inside, outer):
                return jnp.stack([roll(outer if blk in (0, blocks - 1) else inside, -(4 * blk + 2)) for blk in range(blk0, blk0 + GROUP)], axis=0)

            ov[2 * m, rs, :] = flat(jnp.where(odd, black, red) + jnp.where(edge, add(low, low_red), 0.0))
            ov[2 * m + 1, rs, :] = flat(jnp.where(odd, red, black) + jnp.where(edge, add(high, high_red), 0.0))
        return carry

    lax.fori_loop(0, nm, write, 0, unroll=2)

    def drain(t, carry):
        for c in face_copies(t):
            c.wait_send()
        for e in range(2):
            @pl.when(has[e])
            def _():
                for c in wall_copies(t, e):
                    c.wait_send()
        return carry

    lax.fori_loop(0, SWEEPS, drain, 0)
    for e in range(2):
        sz_copy(e).wait_send()
        sy_copy(e).wait_send()

        @pl.when(has[e])
        def _():
            sx_copy(e).wait_send()


def solution(mesh):
    sizes = tuple(mesh.shape[a] for a in ("gx", "gy", "gz"))

    def on_device(field, source):
        planes, rows, cols = field.shape
        nm = planes // 2
        assert planes % 4 == 0 and rows == 256 and cols == 128 and rows % (8 * GROUP) == 0
        f32 = jnp.float32
        wide = (nm + 2 * OFF, rows + 2 * PAD, cols)
        return pl.pallas_call(
            functools.partial(kernel, sizes),
            out_shape=jax.ShapeDtypeStruct(field.shape, f32),
            in_specs=[pl.BlockSpec(memory_space=pltpu.HBM)] * 2,
            out_specs=pl.BlockSpec(memory_space=pltpu.VMEM),
            scratch_shapes=[
                pltpu.VMEM(field.shape, f32),
                pltpu.VMEM(field.shape, f32),
                pltpu.VMEM((SWEEPS + 1, *wide), f32),
                pltpu.VMEM(wide, f32),
                pltpu.VMEM(wide, f32),
                pltpu.VMEM((nm, rows, cols), f32),
                pltpu.VMEM((SWEEPS + 1, nm, 8, cols), f32),
                *[pltpu.VMEM((SWEEPS, nm // 2, 8, cols), f32)] * 4,
                pltpu.VMEM((SWEEPS, 4, 8, cols), f32),
                pltpu.VMEM((2, SWEEPS, 4, nm // 2, cols), f32),
                pltpu.VMEM((nm + 2, 8, cols), f32),
                *[pltpu.VMEM((nm, 8, cols), f32)] * 5,
                *[pltpu.VMEM((2, SWEEPS + 1, nm, 2, cols), f32)] * 2,
                *[pltpu.VMEM((4, SWEEPS, 1, cols), f32)] * 2,
                pltpu.VMEM((2, 2, rows // 2, cols), f32),
                pltpu.VMEM((2, 2, nm // 4, 8, cols), f32),
                pltpu.SemaphoreType.DMA((24, SWEEPS)),
                pltpu.SemaphoreType.DMA((24, SWEEPS)),
                pltpu.SemaphoreType.DMA((nm,)),
                pltpu.SemaphoreType.DMA((nm,)),
            ],
            compiler_params=pltpu.CompilerParams(
                collective_id=0, has_side_effects=True, vmem_limit_bytes=60 * 1024 * 1024
            ),
        )(field, source)

    spec = P("gx", "gy", "gz")
    return jax.shard_map(on_device, mesh=mesh, in_specs=(spec, spec), out_specs=spec, check_vma=False)
```

```python
import functools

import jax
import jax.numpy as jnp
from jax import lax
from jax.experimental import pallas as pl
from jax.experimental.pallas import tpu as pltpu
from jax.sharding import PartitionSpec as P

SWEEPS = 3
MESH = pl.DeviceIdType.MESH
PAD = 16
OFF = 2
GROUP = 8
THIRD = 1.0 / 6.0


def kernel(sizes, f_hbm, s_hbm, ov, fv, sv, xb, rb, sr, sb, fb, mh, ml, lz, hz, dg, cn, g, rd, sg, cu, cd, dz, ystage, yland, xystage, xyland, sface, sedge,
           send, recv, fsem, ssem):
    ngx, ngy, ngz = sizes
    planes, rows, cols = f_hbm.shape
    nm = planes // 2
    blocks = rows // 8
    gx, gy, gz = (lax.axis_index(a) for a in ("gx", "gy", "gz"))
    has_lo, has_hi = gx > 0, gx < ngx - 1
    y_lo, y_hi = lax.rem(gy + ngy - 1, ngy), lax.rem(gy + 1, ngy)
    z_lo, z_hi = lax.rem(gz + ngz - 1, ngz), lax.rem(gz + 1, ngz)
    x_to = (gx - 1, gx + 1)
    y_to = (y_lo, y_hi)
    z_to = (z_lo, z_hi)
    has = (has_lo, has_hi)
    flip = gx >= ngx // 2
    order = [m for a in range(nm // 2) for m in (a, nm - 1 - a)]

    def load(ref, to, sem, m):
        return pltpu.make_async_copy(ref.at[pl.ds(2 * m, 2)], to.at[pl.ds(2 * m, 2)], sem.at[m])

    barrier = pltpu.get_barrier_semaphore()

    def greet(device):
        pl.semaphore_signal(barrier, inc=1, device_id=device, device_id_type=MESH)

    for e in range(2):
        greet({"gy": y_to[e]})
        greet({"gz": z_to[e]})
        for d in range(2):
            greet({"gy": y_to[e], "gz": z_to[d]})

        @pl.when(has[e])
        def _():
            greet({"gx": x_to[e]})
            for d in range(2):
                greet({"gx": x_to[e], "gy": y_to[d]})
                greet({"gx": x_to[e], "gz": z_to[d]})

    for m in order:
        load(f_hbm, fv, fsem, m).start()
    for m in order:
        load(s_hbm, sv, ssem, m).start()

    row8 = lax.broadcasted_iota(jnp.int32, (8, cols), 0)
    lane = lax.broadcasted_iota(jnp.int32, (8, cols), 1)
    off = lax.rem(lane, 4)
    quad = lax.div(lane, 4)
    parity8 = lax.rem(row8 + lane, 2)
    odd8 = parity8 == 1
    odd_edge = lax.rem(row8 + off, 2) == 0
    mid = lax.rem(off + 1, 4) >= 2
    brim = lax.rem(lane + 2, cols) < 4
    first8, last8 = lane == 0, lane == cols - 1

    def rep(mask, n):
        return jnp.broadcast_to(mask[None], (n, 8, cols))

    def roll(v, k):
        k = k % cols
        return v if k == 0 else pltpu.roll(v, k, v.ndim - 1)

    def three(v):
        return v.reshape(v.shape[0] // 8, 8, cols)

    def flat(v):
        return v.reshape(v.shape[0] * 8, cols)

    def pick(parts, y, blk0):
        for k in range(y.shape[0]):
            blk = blk0 + k
            j = blk % len(parts)
            parts[j] = jnp.where(quad == blk, roll(y[k], 4 * blk + 2), parts[j])
        return parts

    def merge(parts):
        while len(parts) > 1:
            parts = [p + q for p, q in zip(parts[::2], parts[1::2])]
        return parts[0]

    zeros8 = jnp.zeros((8, cols), jnp.float32)

    def copy(k, t, src, dst, to, back):
        return pltpu.make_async_remote_copy(
            src_ref=src, dst_ref=dst, send_sem=send.at[k, t], recv_sem=recv.at[back, t], device_id=to, device_id_type=MESH
        )

    def x_copy(t, e, via=None):
        m, to = (0, nm) if e == 0 else (nm - 1, -1)
        return copy(e, t, xb.at[t, OFF + m, pl.ds(PAD, rows)], xb.at[t, OFF + to, pl.ds(PAD, rows)], {"gx": x_to[e if via is None else via]}, 1 - e)

    def y_copy(t, e):
        return copy(2 + e, t, ystage.at[e, t], yland.at[1 - e, t], {"gy": y_to[e]}, 3 - e)

    def z_copy(t, e):
        src, dst = (ml, hz) if e == 0 else (mh, lz)
        return copy(4 + e, t, src.at[t], dst.at[t], {"gz": z_to[e]}, 5 - e)

    def xy_copy(t, e, d, via=None):
        k, back = 6 + 2 * e + d, 6 + 2 * (1 - e) + 1 - d
        return copy(k, t, xystage.at[k - 6, t], xyland.at[back - 6, t], {"gx": x_to[e if via is None else via], "gy": y_to[d]}, back)

    def xz_copy(t, e, d, via=None):
        k, back = 10 + 2 * e + d, 10 + 2 * (1 - e) + 1 - d
        j = 0 if e == 0 else nm // 2 - 1
        return copy(k, t, (ml, mh)[d].at[t, j], dg.at[t, back - 10], {"gx": x_to[e if via is None else via], "gz": z_to[d]}, back)

    def yz_copy(t, e, d):
        k, back = 14 + 2 * e + d, 14 + 2 * (1 - e) + 1 - d
        return copy(k, t, cn.at[1, t, k - 14], cn.at[0, t, back - 14], {"gy": y_to[e], "gz": z_to[d]}, back)

    def sx_copy(e, via=None):
        return copy(18 + e, 0, sface.at[0, e], sface.at[1, 1 - e], {"gx": x_to[e if via is None else via]}, 19 - e)

    def sy_copy(e):
        return copy(20 + e, 0, ystage.at[e, SWEEPS], yland.at[1 - e, SWEEPS], {"gy": y_to[e]}, 21 - e)

    def sz_copy(e):
        return copy(22 + e, 0, sedge.at[0, e], sedge.at[1, 1 - e], {"gz": z_to[e]}, 23 - e)

    def face_copies(t):
        return [y_copy(t, e) for e in range(2)] + [z_copy(t, e) for e in range(2)] + [yz_copy(t, e, d) for e in range(2) for d in range(2)]

    def wall_copies(t, e):
        return [x_copy(t, e)] + [xy_copy(t, e, d) for d in range(2)] + [xz_copy(t, e, d) for d in range(2)]

    def messages(t, src):
        for j in range(nm // 2):
            even, odd = src(2 * j), src(2 * j + 1)
            mh[t, j] = jnp.where(off < 2, even, roll(odd, 2))
            ml[t, j] = jnp.where(off < 2, roll(even, -2), odd)

    def send_all(t, between=None):
        for e in range(2):
            r = 0 if e == 0 else 7
            for d in range(2):
                cn[1, t, 2 * e + d] = (ml, mh)[d][t, :, r, :]
        for e in range(2):
            for d in range(2):
                m = 0 if e == 0 else nm - 1
                r = PAD if d == 0 else PAD + rows - 1
                xystage[2 * e + d, t] = xb[t, OFF + m, pl.ds(r, 1), :]
        for e in range(2):
            for d in range(2):
                yz_copy(t, e, d).start()
        for e in range(2):
            @pl.when(has[e])
            def _():
                for d in range(2):
                    xz_copy(t, e, d).start()
                for d in range(2):
                    xy_copy(t, e, d).start()
        for e in range(2):
            z_copy(t, e).start()
        for e in range(2):
            r = PAD if e == 0 else PAD + rows - 2
            for m in range(nm):
                ystage[e, t, m] = xb[t, OFF + m, pl.ds(r, 2), :]
            y_copy(t, e).start()
        if between is not None:
            between()
        for e in range(2):
            @pl.when(has[e])
            def _():
                x_copy(t, e).start()

    def arrive_y(t):
        for e in range(2):
            y_copy(t, e).wait_recv()
        for e in range(2):
            r = PAD - 2 if e == 0 else PAD + rows
            for m in range(nm):
                xb[t, OFF + m, pl.ds(r, 2), :] = yland[e, t, m]

    def arrive_z(t):
        for e in range(2):
            z_copy(t, e).wait_recv()
        for j in range(nm // 2):
            low, high = lz[t, j], hz[t, j]
            l1, l3, lm = roll(low, 1), roll(low, 3), roll(low, -1)
            h1, h3, hm = roll(high, 1), roll(high, -3), roll(high, -1)
            g[1 + 2 * j] = jnp.where(off < 2, jnp.where(off == 0, hm, h1), jnp.where(off == 2, l1, l3))
            g[2 + 2 * j] = jnp.where(off < 2, jnp.where(off == 0, h3, hm), jnp.where(off == 2, lm, l1))

    def arrive_diagonals(t):
        for e in range(2):
            for d in range(2):
                yz_copy(t, e, d).wait_recv()
        for j in range(nm // 2):
            for p in range(2):
                a, b = (jnp.broadcast_to(cn[0, t, k, pl.ds(j, 1), :], (8, cols)) for k in (0, 1))
                cu[2 * j + p] = jnp.where(off == 2, roll(a, 5 - 2 * p), roll(b, 5 - 2 * p))
                a, b = (jnp.broadcast_to(cn[0, t, k, pl.ds(j, 1), :], (8, cols)) for k in (2, 3))
                cd[2 * j + p] = jnp.where(off == 2, roll(a, -3 - 2 * p), roll(b, -3 - 2 * p))
    def arrive_xz(t):
        for e in range(2):
            @pl.when(has[e])
            def _():
                for d in range(2):
                    xz_copy(t, 1 - e, d, e).wait_recv()
                k = -1 if e == 0 else 1
                g[0 if e == 0 else nm + 1] = jnp.where(off == 2, roll(dg[t, 2 * e], k), roll(dg[t, 2 * e + 1], k))

    def arrive_xy(t):
        for e in range(2):
            @pl.when(has[e])
            def _():
                for d in range(2):
                    xy_copy(t, 1 - e, d, e).wait_recv()
                i = OFF - 1 if e == 0 else OFF + nm
                for d in range(2):
                    r = PAD - 1 if d == 0 else PAD + rows
                    xb[t, i, pl.ds(r, 1), :] = xyland[2 * e + d, t]

    def arrive_x(t, late):
        for e in range(2):
            @pl.when(has[e] & (flip if (e == 0) == late else jnp.logical_not(flip)))
            def _():
                x_copy(t, 1 - e, e).wait_recv()

    def edge_red(t):
        for m in range(nm):
            v = g[1 + m]
            up = pltpu.roll(jnp.where(row8 == 7, jnp.where(lane < 4, cu[m], roll(v, 4)), v), 1, 0)
            down = pltpu.roll(jnp.where(row8 == 0, jnp.where(lane >= cols - 4, cd[m], roll(v, -4)), v), 7, 0)
            side = jnp.where(off == 1, roll(v, 1), roll(v, -1))
            beside = jnp.where(odd_edge, g[2 + m], g[m])
            rd[m] = (((sg[m] + v) + (beside + up)) + ((down + side) + fb[t, m])) * jnp.float32(THIRD)

    def relax(read, i, blk0, n, src, c, inner=False):
        rs = PAD + 8 * blk0
        here = three(read(i, rs, 8 * n))
        below_at, above_at = i - 1, i + 1
        if inner:
            below_at, above_at = below_at - (nm - (i - OFF)) // nm, above_at - (OFF + nm) * ((i - OFF) // (nm - 1))
        below, above = three(read(below_at, rs, 8 * n)), three(read(above_at, rs, 8 * n))
        odd = rep(odd8, n)
        beside = jnp.where(odd, above, below) if c == 0 else jnp.where(odd, below, above)
        total = (three(src) + here) + beside
        total = total + three(read(i, rs - 1, 8 * n))
        total = total + three(read(i, rs + 1, 8 * n))
        return beside_lanes(total, here) * jnp.float32(THIRD)

    def beside_lanes(total, here):
        n = here.shape[0]
        total = total + jnp.where(rep(first8, n), 0.0, roll(here, 1))
        return total + jnp.where(rep(last8, n), 0.0, roll(here, -1))

    def red_pair(t, m, inner=False, keep=None):
        i = m + OFF

        def read(i, r, n):
            return xb[t, i, pl.ds(r, n), :]

        for blk0 in range(0, blocks, GROUP):
            y = relax(read, i, blk0, GROUP, sr[i, pl.ds(PAD + 8 * blk0, 8 * GROUP), :], 0, inner)
            if keep is not None:
                y = jnp.where(keep, y, 0.0)
            rb[i, pl.ds(PAD + 8 * blk0, 8 * GROUP), :] = flat(y)

    def relax_block(x, src, lo, n, r, c):
        def read(i, r):
            return x[pl.ds(i, n), pl.ds(r, 8), :]

        odd = rep(odd8, n)
        here, below, above = read(lo, r), read(lo - 1, r), read(lo + 1, r)
        total = (src + here) + (jnp.where(odd, above, below) if c == 0 else jnp.where(odd, below, above))
        total = (total + read(lo, r - 1)) + read(lo, r + 1)
        return beside_lanes(total, here) * jnp.float32(THIRD)

    def red_rows(t):
        for r in (PAD - 8, PAD + rows):
            src = sr[pl.ds(OFF, nm), pl.ds(r, 8), :]
            rb[pl.ds(OFF, nm), pl.ds(r, 8), :] = relax_block(xb.at[t], src, OFF, nm, r, 0)

    def red_borders(t, i, n):
        for r, d, k in ((PAD, -1, 0), (PAD + rows - 8, 1, 7)):
            halo = xb[t, pl.ds(i, n), pl.ds(r + d, 8), :]
            own = pl.ds(i, n), pl.ds(r, 8), slice(None)
            rb[own] = rb[own] + jnp.where(jnp.broadcast_to((row8 == k)[None], (n, 8, cols)), halo, 0.0) * jnp.float32(THIRD)

    def red_side(t, q, h, low):
        near = parity8 == jnp.where(low, 0, 1)
        for blk0 in range(0, blocks, GROUP):
            rs = pl.ds(PAD + 8 * blk0, 8 * GROUP)
            halo = jnp.where(rep(near, GROUP), three(xb[t, h + OFF, rs, :]), 0.0)
            rb[q + OFF, rs, :] = rb[q + OFF, rs, :] + flat(halo * jnp.float32(THIRD))

    def lift(m, blk):
        return jnp.where(brim, roll(dz[m], -(4 * blk + 2)), 0.0)

    def black_borders(t):
        for blk in (0, blocks - 1):
            r = PAD + 8 * blk
            y = relax_block(rb, sb[:, pl.ds(8 * blk, 8), :], OFF, nm, r, 1)
            xb[t + 1, pl.ds(OFF, nm), pl.ds(r, 8), :] = y
            for m in range(nm):
                fb[t + 1, m] = jnp.where(quad == blk, roll(y[m], 4 * blk + 2), fb[t + 1, m])

    def lift_borders(t):
        for m in range(1, nm - 1):
            for blk in (0, blocks - 1):
                rs = pl.ds(PAD + 8 * blk, 8)
                xb[t, OFF + m, rs, :] = xb[t, OFF + m, rs, :] + lift(m, blk)
            fb[t, m] = fb[t, m] + dz[m]

    def edge_response(t):
        def middle(v):
            return jnp.where(mid, v, 0.0)

        for m in range(nm):
            v = middle(g[1 + m])
            up = pltpu.roll(jnp.where(row8 == 7, jnp.where(lane < 4, middle(cu[m]), roll(v, 4)), v), 1, 0)
            down = pltpu.roll(jnp.where(row8 == 0, jnp.where(lane >= cols - 4, middle(cd[m]), roll(v, -4)), v), 7, 0)
            beside = jnp.where(odd_edge, middle(g[2 + m]), middle(g[m]))
            near = (rd[m] + ((v + beside) + (up + down)) * jnp.float32(THIRD)) * jnp.float32(THIRD)
            far = jnp.where(off == 0, roll(v, -1), roll(v, 1)) * jnp.float32(THIRD * THIRD)
            dz[m] = jnp.where(mid, near, far)

    def lift_pair(t, m, first, last):
        v = dz[m]
        for blk0 in range(0, blocks, GROUP):
            lo, hi = max(blk0, first), min(blk0 + GROUP, last)
            rs = pl.ds(PAD + 8 * lo, 8 * (hi - lo))
            y = jnp.stack([roll(v, -(4 * blk + 2)) for blk in range(lo, hi)], axis=0)
            xb[t, OFF + m, rs, :] = xb[t, OFF + m, rs, :] + flat(jnp.where(rep(brim, hi - lo), y, 0.0))

    def lift_rest(t):
        def body(m, carry):
            lift_pair(t, m, 1, blocks - 1)
            return carry

        lax.fori_loop(1, nm - 1, body, 0)

    def black_pair(m, emit):
        i = m + OFF

        def read(i, r, n):
            return rb[i, pl.ds(r, n), :]

        for blk0 in range(0, blocks, GROUP):
            rs = pl.ds(8 * blk0, 8 * GROUP)
            emit(blk0, relax(read, i, blk0, GROUP, sb[m, rs, :], 1))

    zero = jnp.zeros((rows + 16, cols), jnp.float32)
    for e in range(2):
        @pl.when(jnp.logical_not(has[e]))
        def _():
            i = OFF - 1 if e == 0 else OFF + nm
            for t in range(SWEEPS):
                xb[t, i, pl.ds(PAD - 8, rows + 16), :] = zero
            rb[i, pl.ds(PAD - 8, rows + 16), :] = zero
            g[0 if e == 0 else nm + 1] = zeros8

    def pack_field(a, carry):
        for m in (a, nm - 1 - a):
            load(f_hbm, fv, fsem, m).wait()
            parts = [zeros8] * 4
            for blk0 in range(0, blocks, GROUP):
                rs = pl.ds(8 * blk0, 8 * GROUP)
                y = jnp.where(rep(odd8, GROUP), three(fv[2 * m, rs, :]), three(fv[2 * m + 1, rs, :]))
                xb[0, OFF + m, pl.ds(PAD + 8 * blk0, 8 * GROUP), :] = flat(y)
                parts = pick(parts, y, blk0)
            fb[0, m] = merge(parts)
        return carry

    def pack_source(a, carry):
        for m in (a, nm - 1 - a):
            load(s_hbm, sv, ssem, m).wait()
            parts = [zeros8] * 4
            for blk0 in range(0, blocks, GROUP):
                rs = pl.ds(8 * blk0, 8 * GROUP)
                low, high = three(sv[2 * m, rs, :]), three(sv[2 * m + 1, rs, :])
                y = jnp.where(rep(odd8, GROUP), high, low)
                sr[OFF + m, pl.ds(PAD + 8 * blk0, 8 * GROUP), :] = flat(y)
                sb[m, rs, :] = flat(jnp.where(rep(odd8, GROUP), low, high))
                parts = pick(parts, y, blk0)
            sg[m] = merge(parts)
        return carry

    lax.fori_loop(0, nm // 2, pack_field, 0)
    messages(0, lambda m: fb[0, m])
    lax.fori_loop(0, nm // 2, pack_source, 0)
    half = rows // 2
    odd_lane = lax.rem(lax.broadcasted_iota(jnp.int32, (half, cols), 1), 2) == 1
    for e in range(2):
        for j in range(nm // 4):
            parts = [roll(sg[4 * j + k], k - 2 + e) for k in range(4)]
            sedge[0, e, j] = jnp.where(off < 2, jnp.where(off == 0, parts[0], parts[1]), jnp.where(off == 2, parts[2], parts[3]))
        r = PAD if e == 0 else PAD + rows - 1
        for m in range(nm):
            ystage[e, SWEEPS, m, pl.ds(0, 1), :] = sr[OFF + m, pl.ds(r, 1), :]

    pl.semaphore_wait(barrier, 8 + 5 * (has_lo.astype(jnp.int32) + has_hi.astype(jnp.int32)))
    def send_source():
        for e in range(2):
            sz_copy(e).start()
            sy_copy(e).start()

    send_all(0, send_source)
    for e in range(2):
        @pl.when(has[e])
        def _():
            i = OFF if e == 0 else OFF + nm - 1
            even = sr[i, pl.ds(PAD, half, stride=2), :]
            odd = sr[i, pl.ds(PAD + 1, half, stride=2), :]
            sface[0, e] = jnp.where(odd_lane, odd, even) if e == 0 else jnp.where(odd_lane, even, odd)
            sx_copy(e).start()

    for t in range(SWEEPS):
        xb[t, 0, pl.ds(PAD, rows), :] = zero[:rows]
        for r in (PAD - 8, PAD + rows):
            xb[t, pl.ds(OFF - 1, nm + 2), pl.ds(r, 8), :] = jnp.zeros((nm + 2, 8, cols), jnp.float32)

    def take_source():
        for e in range(2):
            sz_copy(e).wait_recv()
            sy_copy(e).wait_recv()
        for e in range(2):
            r = PAD - 1 if e == 0 else PAD + rows
            for m in range(nm):
                sr[OFF + m, pl.ds(r, 1), :] = yland[e, SWEEPS, m, pl.ds(0, 1), :]
        for j in range(nm // 4):
            low, high = sedge[1, 0, j], sedge[1, 1, j]
            for k in range(4):
                sg[4 * j + k] = jnp.where(off == 1, roll(high, 1 - k), roll(low, 2 - k))

    def take_source_x(late):
        for e in range(2):
            @pl.when(has[e] & (flip if (e == 0) == late else jnp.logical_not(flip)))
            def _():
                sx_copy(1 - e, e).wait_recv()
                i = OFF - 1 if e == 0 else OFF + nm
                got = sface[1, e]
                sr[i, pl.ds(PAD, half, stride=2), :] = got
                sr[i, pl.ds(PAD + 1, half, stride=2), :] = got

    def at(p):
        return jnp.where(flip, nm - 1 - p, p)

    def on_first(t, do):
        pl.when(t == 0)(do)

    def drain(t):
        for c in face_copies(t):
            c.wait_send()
        for e in range(2):
            @pl.when(has[e])
            def _():
                for c in wall_copies(t, e):
                    c.wait_send()

    def drain_source():
        for e in range(2):
            sz_copy(e).wait_send()
            sy_copy(e).wait_send()

            @pl.when(has[e])
            def _():
                sx_copy(e).wait_send()

    def full(t, carry):
        def red_inner(m, carry):
            red_pair(t, m, inner=True)
            return carry

        def black_inner(m, carry):
            parts = [zeros8] * 4

            def emit(blk0, y):
                xb[t + 1, OFF + m, pl.ds(PAD + 8 * blk0, 8 * GROUP), :] = flat(y)
                pick(parts, y, blk0)

            black_pair(m, emit)
            fb[t + 1, m] = merge(parts)
            return carry

        lax.fori_loop(0, nm, red_inner, 0)
        lax.fori_loop(1, nm - 1, black_inner, 0)
        drain(t)
        pl.when(t == 1)(drain_source)

        def side_red(late):
            h = int(late)
            q = at(nm - 1 if late else 0)
            out = at(nm if late else -1)
            red_side(t, q, out, flip if late else jnp.logical_not(flip))
            red_pair(t, out, keep=jnp.where(flip, has[1 - h], has[h]))

        def side_black(late):
            q = at(nm - 1 if late else 0)
            parts = [zeros8] * 4

            def emit(blk0, y):
                if late:
                    y = y + jnp.stack([lift(q, blk0 + k) for k in range(GROUP)], axis=0)
                xb[t + 1, OFF + q, pl.ds(PAD + 8 * blk0, 8 * GROUP), :] = flat(y)
                pick(parts, y, blk0)

            black_pair(q, emit)
            fb[t + 1, q] = merge(parts)

        arrive_x(t, False)
        on_first(t, lambda: take_source_x(False))
        side_red(False)
        side_black(False)
        arrive_y(t)
        red_borders(t, OFF, nm)
        arrive_xy(t)
        red_borders(t, at(-1) + OFF, 1)
        on_first(t, take_source)
        red_rows(t)
        black_borders(t)
        arrive_xz(t)
        arrive_z(t)
        arrive_diagonals(t)
        edge_red(t)
        edge_response(t)
        lift_borders(t + 1)
        early = at(0)
        lift_pair(t + 1, early, 0, blocks)
        fb[t + 1, early] = fb[t + 1, early] + dz[early]
        arrive_x(t, True)
        on_first(t, lambda: take_source_x(True))
        side_red(True)
        side_black(True)

        @pl.when(t < SWEEPS - 1)
        def _():
            messages(t + 1, lambda m: fb[t + 1, m])
            send_all(t + 1)
            lift_rest(t + 1)

        return carry

    lax.fori_loop(0, SWEEPS, full, 0)
    for m in (0, nm - 1):
        dz[m] = zeros8

    def write(m, carry):
        lr = jnp.where(mid, g[1 + m], 0.0) * jnp.float32(THIRD)
        lb = dz[m]
        low, high = jnp.where(odd_edge, lr, lb), jnp.where(odd_edge, lb, lr)
        low_red, high_red = jnp.where(odd_edge, lr, 0.0), jnp.where(odd_edge, 0.0, lr)
        for blk0 in range(0, blocks, GROUP):
            rs, ps = pl.ds(8 * blk0, 8 * GROUP), pl.ds(PAD + 8 * blk0, 8 * GROUP)
            red, black = three(rb[OFF + m, ps, :]), three(xb[SWEEPS, OFF + m, ps, :])
            odd, edge = rep(odd8, GROUP), rep(brim, GROUP)

            def add(inside, outer):
                return jnp.stack([roll(outer if blk in (0, blocks - 1) else inside, -(4 * blk + 2)) for blk in range(blk0, blk0 + GROUP)], axis=0)

            ov[2 * m, rs, :] = flat(jnp.where(odd, black, red) + jnp.where(edge, add(low, low_red), 0.0))
            ov[2 * m + 1, rs, :] = flat(jnp.where(odd, red, black) + jnp.where(edge, add(high, high_red), 0.0))
        return carry

    lax.fori_loop(0, nm, write, 0, unroll=4)


def solution(mesh):
    sizes = tuple(mesh.shape[a] for a in ("gx", "gy", "gz"))

    def on_device(field, source):
        planes, rows, cols = field.shape
        nm = planes // 2
        assert planes % 4 == 0 and rows == 256 and cols == 128 and rows % (8 * GROUP) == 0
        f32 = jnp.float32
        wide = (nm + 2 * OFF, rows + 2 * PAD, cols)
        return pl.pallas_call(
            functools.partial(kernel, sizes),
            out_shape=jax.ShapeDtypeStruct(field.shape, f32),
            in_specs=[pl.BlockSpec(memory_space=pltpu.HBM)] * 2,
            out_specs=pl.BlockSpec(memory_space=pltpu.VMEM),
            scratch_shapes=[
                pltpu.VMEM(field.shape, f32),
                pltpu.VMEM(field.shape, f32),
                pltpu.VMEM((SWEEPS + 1, *wide), f32),
                pltpu.VMEM(wide, f32),
                pltpu.VMEM(wide, f32),
                pltpu.VMEM((nm, rows, cols), f32),
                pltpu.VMEM((SWEEPS + 1, nm, 8, cols), f32),
                *[pltpu.VMEM((SWEEPS, nm // 2, 8, cols), f32)] * 4,
                pltpu.VMEM((SWEEPS, 4, 8, cols), f32),
                pltpu.VMEM((2, SWEEPS, 4, nm // 2, cols), f32),
                pltpu.VMEM((nm + 2, 8, cols), f32),
                *[pltpu.VMEM((nm, 8, cols), f32)] * 5,
                *[pltpu.VMEM((2, SWEEPS + 1, nm, 2, cols), f32)] * 2,
                *[pltpu.VMEM((4, SWEEPS, 1, cols), f32)] * 2,
                pltpu.VMEM((2, 2, rows // 2, cols), f32),
                pltpu.VMEM((2, 2, nm // 4, 8, cols), f32),
                pltpu.SemaphoreType.DMA((24, SWEEPS)),
                pltpu.SemaphoreType.DMA((24, SWEEPS)),
                pltpu.SemaphoreType.DMA((nm,)),
                pltpu.SemaphoreType.DMA((nm,)),
            ],
            compiler_params=pltpu.CompilerParams(
                collective_id=0, has_side_effects=True, vmem_limit_bytes=60 * 1024 * 1024
            ),
        )(field, source)

    spec = P("gx", "gy", "gz")
    return jax.shard_map(on_device, mesh=mesh, in_specs=(spec, spec), out_specs=spec, check_vma=False)
```

```python
import functools

import jax
import jax.numpy as jnp
from jax import lax
from jax.experimental import pallas as pl
from jax.experimental.pallas import tpu as pltpu
from jax.sharding import PartitionSpec as P

SWEEPS = 3
MESH = pl.DeviceIdType.MESH
PAD = 16
OFF = 2
GROUP = 8
THIRD = 1.0 / 6.0


def kernel(sizes, f_hbm, s_hbm, ov, fv, sv, xb, rb, sr, sb, fb, mh, ml, lz, hz, dg, cn, g, rd, sg, cu, cd, dz, ystage, yland, xystage, xyland, sface, sedge,
           send, recv, fsem, ssem):
    ngx, ngy, ngz = sizes
    planes, rows, cols = f_hbm.shape
    nm = planes // 2
    blocks = rows // 8
    gx, gy, gz = (lax.axis_index(a) for a in ("gx", "gy", "gz"))
    has_lo, has_hi = gx > 0, gx < ngx - 1
    y_lo, y_hi = lax.rem(gy + ngy - 1, ngy), lax.rem(gy + 1, ngy)
    z_lo, z_hi = lax.rem(gz + ngz - 1, ngz), lax.rem(gz + 1, ngz)
    x_to = (gx - 1, gx + 1)
    y_to = (y_lo, y_hi)
    z_to = (z_lo, z_hi)
    has = (has_lo, has_hi)
    flip = gx >= ngx // 2
    order = [m for a in range(nm // 2) for m in (a, nm - 1 - a)]

    def load(ref, to, sem, m):
        return pltpu.make_async_copy(ref.at[pl.ds(2 * m, 2)], to.at[pl.ds(2 * m, 2)], sem.at[m])

    barrier = pltpu.get_barrier_semaphore()

    def greet(device):
        pl.semaphore_signal(barrier, inc=1, device_id=device, device_id_type=MESH)

    for e in range(2):
        for d in range(2):
            greet({"gy": y_to[e], "gz": z_to[d]})
    for e in range(2):
        greet({"gz": z_to[e]})
        greet({"gy": y_to[e]})

        @pl.when(has[e])
        def _():
            greet({"gx": x_to[e]})
            for d in range(2):
                greet({"gx": x_to[e], "gy": y_to[d]})
                greet({"gx": x_to[e], "gz": z_to[d]})

    for m in order:
        load(f_hbm, fv, fsem, m).start()
    for m in order:
        load(s_hbm, sv, ssem, m).start()

    row8 = lax.broadcasted_iota(jnp.int32, (8, cols), 0)
    lane = lax.broadcasted_iota(jnp.int32, (8, cols), 1)
    off = lax.rem(lane, 4)
    quad = lax.div(lane, 4)
    parity8 = lax.rem(row8 + lane, 2)
    odd8 = parity8 == 1
    odd_edge = lax.rem(row8 + off, 2) == 0
    mid = lax.rem(off + 1, 4) >= 2
    brim = lax.rem(lane + 2, cols) < 4
    first8, last8 = lane == 0, lane == cols - 1

    def rep(mask, n):
        return jnp.broadcast_to(mask[None], (n, 8, cols))

    def roll(v, k):
        k = k % cols
        return v if k == 0 else pltpu.roll(v, k, v.ndim - 1)

    def three(v):
        return v.reshape(v.shape[0] // 8, 8, cols)

    def flat(v):
        return v.reshape(v.shape[0] * 8, cols)

    def pick(parts, y, blk0):
        for k in range(y.shape[0]):
            blk = blk0 + k
            j = blk % len(parts)
            parts[j] = jnp.where(quad == blk, roll(y[k], 4 * blk + 2), parts[j])
        return parts

    def merge(parts):
        while len(parts) > 1:
            parts = [p + q for p, q in zip(parts[::2], parts[1::2])]
        return parts[0]

    zeros8 = jnp.zeros((8, cols), jnp.float32)

    def copy(k, t, src, dst, to, back):
        return pltpu.make_async_remote_copy(
            src_ref=src, dst_ref=dst, send_sem=send.at[k, t], recv_sem=recv.at[back, t], device_id=to, device_id_type=MESH
        )

    def x_copy(t, e, via=None):
        m, to = (0, nm) if e == 0 else (nm - 1, -1)
        return copy(e, t, xb.at[t, OFF + m, pl.ds(PAD, rows)], xb.at[t, OFF + to, pl.ds(PAD, rows)], {"gx": x_to[e if via is None else via]}, 1 - e)

    def y_copy(t, e):
        return copy(2 + e, t, ystage.at[e, t], yland.at[1 - e, t], {"gy": y_to[e]}, 3 - e)

    def z_copy(t, e):
        src, dst = (ml, hz) if e == 0 else (mh, lz)
        return copy(4 + e, t, src.at[t], dst.at[t], {"gz": z_to[e]}, 5 - e)

    def xy_copy(t, e, d, via=None):
        k, back = 6 + 2 * e + d, 6 + 2 * (1 - e) + 1 - d
        return copy(k, t, xystage.at[k - 6, t], xyland.at[back - 6, t], {"gx": x_to[e if via is None else via], "gy": y_to[d]}, back)

    def xz_copy(t, e, d, via=None):
        k, back = 10 + 2 * e + d, 10 + 2 * (1 - e) + 1 - d
        j = 0 if e == 0 else nm // 2 - 1
        return copy(k, t, (ml, mh)[d].at[t, j], dg.at[t, back - 10], {"gx": x_to[e if via is None else via], "gz": z_to[d]}, back)

    def yz_copy(t, e, d):
        k, back = 14 + 2 * e + d, 14 + 2 * (1 - e) + 1 - d
        return copy(k, t, cn.at[1, t, k - 14], cn.at[0, t, back - 14], {"gy": y_to[e], "gz": z_to[d]}, back)

    def sx_copy(e, via=None):
        return copy(18 + e, 0, sface.at[0, e], sface.at[1, 1 - e], {"gx": x_to[e if via is None else via]}, 19 - e)

    def sy_copy(e):
        return copy(20 + e, 0, ystage.at[e, SWEEPS], yland.at[1 - e, SWEEPS], {"gy": y_to[e]}, 21 - e)

    def sz_copy(e):
        return copy(22 + e, 0, sedge.at[0, e], sedge.at[1, 1 - e], {"gz": z_to[e]}, 23 - e)

    def face_copies(t):
        return [y_copy(t, e) for e in range(2)] + [z_copy(t, e) for e in range(2)] + [yz_copy(t, e, d) for e in range(2) for d in range(2)]

    def wall_copies(t, e):
        return [x_copy(t, e)] + [xy_copy(t, e, d) for d in range(2)] + [xz_copy(t, e, d) for d in range(2)]

    def messages(t, src):
        for j in range(nm // 2):
            even, odd = src(2 * j), src(2 * j + 1)
            mh[t, j] = jnp.where(off < 2, even, roll(odd, 2))
            ml[t, j] = jnp.where(off < 2, roll(even, -2), odd)

    def send_all(t, between=None):
        for e in range(2):
            r = 0 if e == 0 else 7
            for d in range(2):
                cn[1, t, 2 * e + d] = (ml, mh)[d][t, :, r, :]
        for e in range(2):
            for d in range(2):
                m = 0 if e == 0 else nm - 1
                r = PAD if d == 0 else PAD + rows - 1
                xystage[2 * e + d, t] = xb[t, OFF + m, pl.ds(r, 1), :]
        for e in range(2):
            for d in range(2):
                yz_copy(t, e, d).start()
        for e in range(2):
            @pl.when(has[e])
            def _():
                for d in range(2):
                    xz_copy(t, e, d).start()
                for d in range(2):
                    xy_copy(t, e, d).start()
        for e in range(2):
            z_copy(t, e).start()
        for e in range(2):
            r = PAD if e == 0 else PAD + rows - 2
            for m in range(nm):
                ystage[e, t, m] = xb[t, OFF + m, pl.ds(r, 2), :]
            y_copy(t, e).start()
        if between is not None:
            between()
        for e in range(2):
            @pl.when(has[e])
            def _():
                x_copy(t, e).start()

    def arrive_y(t):
        for e in range(2):
            y_copy(t, e).wait_recv()
        for e in range(2):
            r = PAD - 2 if e == 0 else PAD + rows
            for m in range(nm):
                xb[t, OFF + m, pl.ds(r, 2), :] = yland[e, t, m]

    def arrive_z(t):
        for e in range(2):
            z_copy(t, e).wait_recv()
        for j in range(nm // 2):
            low, high = lz[t, j], hz[t, j]
            l1, l3, lm = roll(low, 1), roll(low, 3), roll(low, -1)
            h1, h3, hm = roll(high, 1), roll(high, -3), roll(high, -1)
            g[1 + 2 * j] = jnp.where(off < 2, jnp.where(off == 0, hm, h1), jnp.where(off == 2, l1, l3))
            g[2 + 2 * j] = jnp.where(off < 2, jnp.where(off == 0, h3, hm), jnp.where(off == 2, lm, l1))

    def arrive_diagonals(t):
        for e in range(2):
            for d in range(2):
                yz_copy(t, e, d).wait_recv()
        for j in range(nm // 2):
            for p in range(2):
                a, b = (jnp.broadcast_to(cn[0, t, k, pl.ds(j, 1), :], (8, cols)) for k in (0, 1))
                cu[2 * j + p] = jnp.where(off == 2, roll(a, 5 - 2 * p), roll(b, 5 - 2 * p))
                a, b = (jnp.broadcast_to(cn[0, t, k, pl.ds(j, 1), :], (8, cols)) for k in (2, 3))
                cd[2 * j + p] = jnp.where(off == 2, roll(a, -3 - 2 * p), roll(b, -3 - 2 * p))
    def arrive_xz(t):
        for e in range(2):
            @pl.when(has[e])
            def _():
                for d in range(2):
                    xz_copy(t, 1 - e, d, e).wait_recv()
                k = -1 if e == 0 else 1
                g[0 if e == 0 else nm + 1] = jnp.where(off == 2, roll(dg[t, 2 * e], k), roll(dg[t, 2 * e + 1], k))

    def arrive_xy(t):
        for e in range(2):
            @pl.when(has[e])
            def _():
                for d in range(2):
                    xy_copy(t, 1 - e, d, e).wait_recv()
                i = OFF - 1 if e == 0 else OFF + nm
                for d in range(2):
                    r = PAD - 1 if d == 0 else PAD + rows
                    xb[t, i, pl.ds(r, 1), :] = xyland[2 * e + d, t]

    def arrive_x(t, late):
        for e in range(2):
            @pl.when(has[e] & (flip if (e == 0) == late else jnp.logical_not(flip)))
            def _():
                x_copy(t, 1 - e, e).wait_recv()

    def edge_red(t):
        for m in range(nm):
            v = g[1 + m]
            up = pltpu.roll(jnp.where(row8 == 7, jnp.where(lane < 4, cu[m], roll(v, 4)), v), 1, 0)
            down = pltpu.roll(jnp.where(row8 == 0, jnp.where(lane >= cols - 4, cd[m], roll(v, -4)), v), 7, 0)
            side = jnp.where(off == 1, roll(v, 1), roll(v, -1))
            beside = jnp.where(odd_edge, g[2 + m], g[m])
            rd[m] = (((sg[m] + v) + (beside + up)) + ((down + side) + fb[t, m])) * jnp.float32(THIRD)

    def relax(read, i, blk0, n, src, c, inner=False):
        rs = PAD + 8 * blk0
        here = three(read(i, rs, 8 * n))
        below_at, above_at = i - 1, i + 1
        if inner:
            below_at, above_at = below_at - (nm - (i - OFF)) // nm, above_at - (OFF + nm) * ((i - OFF) // (nm - 1))
        below, above = three(read(below_at, rs, 8 * n)), three(read(above_at, rs, 8 * n))
        odd = rep(odd8, n)
        beside = jnp.where(odd, above, below) if c == 0 else jnp.where(odd, below, above)
        total = (three(src) + here) + beside
        total = total + three(read(i, rs - 1, 8 * n))
        total = total + three(read(i, rs + 1, 8 * n))
        return beside_lanes(total, here) * jnp.float32(THIRD)

    def beside_lanes(total, here):
        n = here.shape[0]
        total = total + jnp.where(rep(first8, n), 0.0, roll(here, 1))
        return total + jnp.where(rep(last8, n), 0.0, roll(here, -1))

    def red_pair(t, m, inner=False, keep=None):
        i = m + OFF

        def read(i, r, n):
            return xb[t, i, pl.ds(r, n), :]

        for blk0 in range(0, blocks, GROUP):
            y = relax(read, i, blk0, GROUP, sr[i, pl.ds(PAD + 8 * blk0, 8 * GROUP), :], 0, inner)
            if keep is not None:
                y = jnp.where(keep, y, 0.0)
            rb[i, pl.ds(PAD + 8 * blk0, 8 * GROUP), :] = flat(y)

    def relax_block(x, src, lo, n, r, c):
        def read(i, r):
            return x[pl.ds(i, n), pl.ds(r, 8), :]

        odd = rep(odd8, n)
        here, below, above = read(lo, r), read(lo - 1, r), read(lo + 1, r)
        total = (src + here) + (jnp.where(odd, above, below) if c == 0 else jnp.where(odd, below, above))
        total = (total + read(lo, r - 1)) + read(lo, r + 1)
        return beside_lanes(total, here) * jnp.float32(THIRD)

    def red_rows(t):
        for r in (PAD - 8, PAD + rows):
            src = sr[pl.ds(OFF, nm), pl.ds(r, 8), :]
            rb[pl.ds(OFF, nm), pl.ds(r, 8), :] = relax_block(xb.at[t], src, OFF, nm, r, 0)

    def red_borders(t, i, n):
        for r, d, k in ((PAD, -1, 0), (PAD + rows - 8, 1, 7)):
            halo = xb[t, pl.ds(i, n), pl.ds(r + d, 8), :]
            own = pl.ds(i, n), pl.ds(r, 8), slice(None)
            rb[own] = rb[own] + jnp.where(jnp.broadcast_to((row8 == k)[None], (n, 8, cols)), halo, 0.0) * jnp.float32(THIRD)

    def red_side(t, q, h, low):
        near = parity8 == jnp.where(low, 0, 1)
        for blk0 in range(0, blocks, GROUP):
            rs = pl.ds(PAD + 8 * blk0, 8 * GROUP)
            halo = jnp.where(rep(near, GROUP), three(xb[t, h + OFF, rs, :]), 0.0)
            rb[q + OFF, rs, :] = rb[q + OFF, rs, :] + flat(halo * jnp.float32(THIRD))

    def lift(m, blk):
        return jnp.where(brim, roll(dz[m], -(4 * blk + 2)), 0.0)

    def black_borders(t):
        for blk in (0, blocks - 1):
            r = PAD + 8 * blk
            y = relax_block(rb, sb[:, pl.ds(8 * blk, 8), :], OFF, nm, r, 1)
            xb[t + 1, pl.ds(OFF, nm), pl.ds(r, 8), :] = y
            for m in range(nm):
                fb[t + 1, m] = jnp.where(quad == blk, roll(y[m], 4 * blk + 2), fb[t + 1, m])

    def lift_borders(t):
        for m in range(1, nm - 1):
            for blk in (0, blocks - 1):
                rs = pl.ds(PAD + 8 * blk, 8)
                xb[t, OFF + m, rs, :] = xb[t, OFF + m, rs, :] + lift(m, blk)
            fb[t, m] = fb[t, m] + dz[m]

    def edge_response(t):
        def middle(v):
            return jnp.where(mid, v, 0.0)

        for m in range(nm):
            v = middle(g[1 + m])
            up = pltpu.roll(jnp.where(row8 == 7, jnp.where(lane < 4, middle(cu[m]), roll(v, 4)), v), 1, 0)
            down = pltpu.roll(jnp.where(row8 == 0, jnp.where(lane >= cols - 4, middle(cd[m]), roll(v, -4)), v), 7, 0)
            beside = jnp.where(odd_edge, middle(g[2 + m]), middle(g[m]))
            near = (rd[m] + ((v + beside) + (up + down)) * jnp.float32(THIRD)) * jnp.float32(THIRD)
            far = jnp.where(off == 0, roll(v, -1), roll(v, 1)) * jnp.float32(THIRD * THIRD)
            dz[m] = jnp.where(mid, near, far)

    def lift_pair(t, m, first, last):
        v = dz[m]
        for blk0 in range(0, blocks, GROUP):
            lo, hi = max(blk0, first), min(blk0 + GROUP, last)
            rs = pl.ds(PAD + 8 * lo, 8 * (hi - lo))
            y = jnp.stack([roll(v, -(4 * blk + 2)) for blk in range(lo, hi)], axis=0)
            xb[t, OFF + m, rs, :] = xb[t, OFF + m, rs, :] + flat(jnp.where(rep(brim, hi - lo), y, 0.0))

    def lift_rest(t):
        def body(m, carry):
            lift_pair(t, m, 1, blocks - 1)
            return carry

        lax.fori_loop(1, nm - 1, body, 0)

    def black_pair(m, emit):
        i = m + OFF

        def read(i, r, n):
            return rb[i, pl.ds(r, n), :]

        for blk0 in range(0, blocks, GROUP):
            rs = pl.ds(8 * blk0, 8 * GROUP)
            emit(blk0, relax(read, i, blk0, GROUP, sb[m, rs, :], 1))

    zero = jnp.zeros((rows + 16, cols), jnp.float32)
    for e in range(2):
        @pl.when(jnp.logical_not(has[e]))
        def _():
            i = OFF - 1 if e == 0 else OFF + nm
            for t in range(SWEEPS):
                xb[t, i, pl.ds(PAD - 8, rows + 16), :] = zero
            rb[i, pl.ds(PAD - 8, rows + 16), :] = zero
            g[0 if e == 0 else nm + 1] = zeros8

    def pack_field(a, carry):
        for m in (a, nm - 1 - a):
            load(f_hbm, fv, fsem, m).wait()
            parts = [zeros8] * 4
            for blk0 in range(0, blocks, GROUP):
                rs = pl.ds(8 * blk0, 8 * GROUP)
                y = jnp.where(rep(odd8, GROUP), three(fv[2 * m, rs, :]), three(fv[2 * m + 1, rs, :]))
                xb[0, OFF + m, pl.ds(PAD + 8 * blk0, 8 * GROUP), :] = flat(y)
                parts = pick(parts, y, blk0)
            fb[0, m] = merge(parts)
        return carry

    def pack_source(a, carry):
        for m in (a, nm - 1 - a):
            load(s_hbm, sv, ssem, m).wait()
            parts = [zeros8] * 4
            for blk0 in range(0, blocks, GROUP):
                rs = pl.ds(8 * blk0, 8 * GROUP)
                low, high = three(sv[2 * m, rs, :]), three(sv[2 * m + 1, rs, :])
                y = jnp.where(rep(odd8, GROUP), high, low)
                sr[OFF + m, pl.ds(PAD + 8 * blk0, 8 * GROUP), :] = flat(y)
                sb[m, rs, :] = flat(jnp.where(rep(odd8, GROUP), low, high))
                parts = pick(parts, y, blk0)
            sg[m] = merge(parts)
        return carry

    lax.fori_loop(0, nm // 2, pack_field, 0)
    messages(0, lambda m: fb[0, m])
    lax.fori_loop(0, nm // 2, pack_source, 0)
    half = rows // 2
    odd_lane = lax.rem(lax.broadcasted_iota(jnp.int32, (half, cols), 1), 2) == 1
    for e in range(2):
        for j in range(nm // 4):
            parts = [roll(sg[4 * j + k], k - 2 + e) for k in range(4)]
            sedge[0, e, j] = jnp.where(off < 2, jnp.where(off == 0, parts[0], parts[1]), jnp.where(off == 2, parts[2], parts[3]))
        r = PAD if e == 0 else PAD + rows - 1
        for m in range(nm):
            ystage[e, SWEEPS, m, pl.ds(0, 1), :] = sr[OFF + m, pl.ds(r, 1), :]

    pl.semaphore_wait(barrier, 8 + 5 * (has_lo.astype(jnp.int32) + has_hi.astype(jnp.int32)))
    def send_source():
        for e in range(2):
            sz_copy(e).start()
            sy_copy(e).start()

    send_all(0, send_source)
    for e in range(2):
        @pl.when(has[e])
        def _():
            i = OFF if e == 0 else OFF + nm - 1
            even = sr[i, pl.ds(PAD, half, stride=2), :]
            odd = sr[i, pl.ds(PAD + 1, half, stride=2), :]
            sface[0, e] = jnp.where(odd_lane, odd, even) if e == 0 else jnp.where(odd_lane, even, odd)
            sx_copy(e).start()

    for t in range(SWEEPS):
        xb[t, 0, pl.ds(PAD, rows), :] = zero[:rows]
        for r in (PAD - 8, PAD + rows):
            xb[t, pl.ds(OFF - 1, nm + 2), pl.ds(r, 8), :] = jnp.zeros((nm + 2, 8, cols), jnp.float32)

    def take_source():
        for e in range(2):
            sz_copy(e).wait_recv()
            sy_copy(e).wait_recv()
        for e in range(2):
            r = PAD - 1 if e == 0 else PAD + rows
            for m in range(nm):
                sr[OFF + m, pl.ds(r, 1), :] = yland[e, SWEEPS, m, pl.ds(0, 1), :]
        for j in range(nm // 4):
            low, high = sedge[1, 0, j], sedge[1, 1, j]
            for k in range(4):
                sg[4 * j + k] = jnp.where(off == 1, roll(high, 1 - k), roll(low, 2 - k))

    def take_source_x(late):
        for e in range(2):
            @pl.when(has[e] & (flip if (e == 0) == late else jnp.logical_not(flip)))
            def _():
                sx_copy(1 - e, e).wait_recv()
                i = OFF - 1 if e == 0 else OFF + nm
                got = sface[1, e]
                sr[i, pl.ds(PAD, half, stride=2), :] = got
                sr[i, pl.ds(PAD + 1, half, stride=2), :] = got

    def at(p):
        return jnp.where(flip, nm - 1 - p, p)

    def on_first(t, do):
        pl.when(t == 0)(do)

    def drain(t):
        for c in face_copies(t):
            c.wait_send()
        for e in range(2):
            @pl.when(has[e])
            def _():
                for c in wall_copies(t, e):
                    c.wait_send()

    def drain_source():
        for e in range(2):
            sz_copy(e).wait_send()
            sy_copy(e).wait_send()

            @pl.when(has[e])
            def _():
                sx_copy(e).wait_send()

    def full(t, carry):
        def red_inner(m, carry):
            red_pair(t, m, inner=True)
            return carry

        def black_inner(m, carry):
            parts = [zeros8] * 4

            def emit(blk0, y):
                xb[t + 1, OFF + m, pl.ds(PAD + 8 * blk0, 8 * GROUP), :] = flat(y)
                pick(parts, y, blk0)

            black_pair(m, emit)
            fb[t + 1, m] = merge(parts)
            return carry

        lax.fori_loop(0, nm, red_inner, 0)
        lax.fori_loop(1, nm - 1, black_inner, 0)
        drain(t)
        pl.when(t == 1)(drain_source)

        def side_red(late):
            h = int(late)
            q = at(nm - 1 if late else 0)
            out = at(nm if late else -1)
            red_side(t, q, out, flip if late else jnp.logical_not(flip))
            red_pair(t, out, keep=jnp.where(flip, has[1 - h], has[h]))

        def side_black(late):
            q = at(nm - 1 if late else 0)
            parts = [zeros8] * 4

            def emit(blk0, y):
                if late:
                    y = y + jnp.stack([lift(q, blk0 + k) for k in range(GROUP)], axis=0)
                xb[t + 1, OFF + q, pl.ds(PAD + 8 * blk0, 8 * GROUP), :] = flat(y)
                pick(parts, y, blk0)

            black_pair(q, emit)
            fb[t + 1, q] = merge(parts)

        arrive_x(t, False)
        on_first(t, lambda: take_source_x(False))
        side_red(False)
        side_black(False)
        arrive_y(t)
        red_borders(t, OFF, nm)
        arrive_xy(t)
        red_borders(t, at(-1) + OFF, 1)
        on_first(t, take_source)
        red_rows(t)
        black_borders(t)
        arrive_xz(t)
        arrive_z(t)
        arrive_diagonals(t)
        edge_red(t)
        edge_response(t)
        lift_borders(t + 1)
        early = at(0)
        lift_pair(t + 1, early, 0, blocks)
        fb[t + 1, early] = fb[t + 1, early] + dz[early]
        arrive_x(t, True)
        on_first(t, lambda: take_source_x(True))
        side_red(True)
        side_black(True)

        @pl.when(t < SWEEPS - 1)
        def _():
            messages(t + 1, lambda m: fb[t + 1, m])
            send_all(t + 1)
            lift_rest(t + 1)

        return carry

    lax.fori_loop(0, SWEEPS, full, 0)
    for m in (0, nm - 1):
        dz[m] = zeros8

    def write(m, carry):
        lr = jnp.where(mid, g[1 + m], 0.0) * jnp.float32(THIRD)
        lb = dz[m]
        low, high = jnp.where(odd_edge, lr, lb), jnp.where(odd_edge, lb, lr)
        low_red, high_red = jnp.where(odd_edge, lr, 0.0), jnp.where(odd_edge, 0.0, lr)
        for blk0 in range(0, blocks, GROUP):
            rs, ps = pl.ds(8 * blk0, 8 * GROUP), pl.ds(PAD + 8 * blk0, 8 * GROUP)
            red, black = three(rb[OFF + m, ps, :]), three(xb[SWEEPS, OFF + m, ps, :])
            odd, edge = rep(odd8, GROUP), rep(brim, GROUP)

            def add(inside, outer):
                return jnp.stack([roll(outer if blk in (0, blocks - 1) else inside, -(4 * blk + 2)) for blk in range(blk0, blk0 + GROUP)], axis=0)

            ov[2 * m, rs, :] = flat(jnp.where(odd, black, red) + jnp.where(edge, add(low, low_red), 0.0))
            ov[2 * m + 1, rs, :] = flat(jnp.where(odd, red, black) + jnp.where(edge, add(high, high_red), 0.0))
        return carry

    lax.fori_loop(0, nm, write, 0, unroll=4)


def solution(mesh):
    sizes = tuple(mesh.shape[a] for a in ("gx", "gy", "gz"))

    def on_device(field, source):
        planes, rows, cols = field.shape
        nm = planes // 2
        assert planes % 4 == 0 and rows == 256 and cols == 128 and rows % (8 * GROUP) == 0
        f32 = jnp.float32
        wide = (nm + 2 * OFF, rows + 2 * PAD, cols)
        return pl.pallas_call(
            functools.partial(kernel, sizes),
            out_shape=jax.ShapeDtypeStruct(field.shape, f32),
            in_specs=[pl.BlockSpec(memory_space=pltpu.HBM)] * 2,
            out_specs=pl.BlockSpec(memory_space=pltpu.VMEM),
            scratch_shapes=[
                pltpu.VMEM(field.shape, f32),
                pltpu.VMEM(field.shape, f32),
                pltpu.VMEM((SWEEPS + 1, *wide), f32),
                pltpu.VMEM(wide, f32),
                pltpu.VMEM(wide, f32),
                pltpu.VMEM((nm, rows, cols), f32),
                pltpu.VMEM((SWEEPS + 1, nm, 8, cols), f32),
                *[pltpu.VMEM((SWEEPS, nm // 2, 8, cols), f32)] * 4,
                pltpu.VMEM((SWEEPS, 4, 8, cols), f32),
                pltpu.VMEM((2, SWEEPS, 4, nm // 2, cols), f32),
                pltpu.VMEM((nm + 2, 8, cols), f32),
                *[pltpu.VMEM((nm, 8, cols), f32)] * 5,
                *[pltpu.VMEM((2, SWEEPS + 1, nm, 2, cols), f32)] * 2,
                *[pltpu.VMEM((4, SWEEPS, 1, cols), f32)] * 2,
                pltpu.VMEM((2, 2, rows // 2, cols), f32),
                pltpu.VMEM((2, 2, nm // 4, 8, cols), f32),
                pltpu.SemaphoreType.DMA((24, SWEEPS)),
                pltpu.SemaphoreType.DMA((24, SWEEPS)),
                pltpu.SemaphoreType.DMA((nm,)),
                pltpu.SemaphoreType.DMA((nm,)),
            ],
            compiler_params=pltpu.CompilerParams(
                collective_id=0, has_side_effects=True, vmem_limit_bytes=60 * 1024 * 1024
            ),
        )(field, source)

    spec = P("gx", "gy", "gz")
    return jax.shard_map(on_device, mesh=mesh, in_specs=(spec, spec), out_specs=spec, check_vma=False)
```
